32 devices in a mesh: groups: 2 (over y), col: 4 (over x, core), row: 4 (over z).
Axes of the slice: x: 2, y: 2, z: 4, core: 2. Of those that a mesh axis runs over, the one named last changes fastest.
Arguments:
- features: bfloat16 [128, 128, 256], P(('groups', 'row'), 'col'), parts along dimension 0, may hold values from -6 to 6
- tissue: int32 [128, 128], P(('groups', 'row'), 'col'), parts along dimension 0, may hold values from 0 to 1, as said below
- conv_first: bfloat16 [3, 3, 256, 256], replicated, may hold values from -0.1875 to 0.1875
- bias_first: float32 [256], replicated, may hold values from -3 to 3
- conv_second: bfloat16 [3, 3, 256, 256], replicated, may hold values from -0.1875 to 0.1875
- bias_second: float32 [256], replicated, may hold values from -3 to 3
- key_weight: bfloat16 [256, 1280], replicated, may hold values from -0.375 to 0.375
- value_weight: bfloat16 [256, 1280], replicated, may hold values from -0.375 to 0.375
- latent_queries: bfloat16 [512, 1280], P(('col', 'row')), may hold values from -70 to 70
- out_weight: bfloat16 [1280, 1280], P(None, 'col'), may hold values from -0.15625 to 0.15625
Outputs:
- encoded: bfloat16 [1024, 1280], P(('groups', 'row'), 'col'), parts along dimension 0
The draws below stay inside these ranges and needn't reach their ends.
There are 2 independent parts, one for each index of `groups`. The reference program is written for one: setup_inputs(seed, part) draws one part's arguments, and reference() takes and returns one part's arrays. A program takes and returns all parts, laid end to end along the dimension named above; an argument that names none is the same for every part. Nothing has to cross between parts.
Inputs may be any that keep to these rules, and one draw needn't show every extreme that they name: Every region of 16 x 32 patches of one device holds at least one tissue patch; the share of tissue differs widely from region to region.
All inputs are finite; a program needn't handle non-finite values.
Results may differ from the reference program's by a relative error of at most 0.007.
The reference program's roundings to bfloat16 on the way (of `inputs`, `hidden`, `second`, `key_rows`, `normalized` and `attended`) count: a program that leaves them out, or rounds other values in their place, can miss the bound.
Values may be sent and summed in bfloat16 or wider, within the bound.
No kernel may reach another device: no remote copies, remote signals or barrier semaphores. Data moves between devices by JAX's collectives and lax.ppermute only.
A program may use at most 64 MiB of HBM per device.

```python
import math
import jax
import jax.numpy as jnp
from jax import lax

C = 256
E = 1280
Q = 512
PH = 16
PW = 32
GH = 64
GW = 128


def draw_tissue(key, part):
    first_key = jax.random.fold_in(key, 11)
    second_key = jax.random.fold_in(key, 12)
    levels = jax.random.randint(first_key, (GH // PH, GW // PW), 1, 9)
    levels = jnp.repeat(jnp.repeat(levels, PH, axis=0), PW, axis=1)
    cells = jax.random.randint(second_key, (GH, GW), 0, 8)
    chosen = (cells < levels).astype(jnp.int32)
    row_index = lax.broadcasted_iota(jnp.int32, (GH, GW), 0)
    col_index = lax.broadcasted_iota(jnp.int32, (GH, GW), 1)
    corner = jnp.logical_and(row_index % PH == 0, col_index % PW == 0)
    return jnp.where(corner, 1, chosen).astype(jnp.int32)


def draw_latent_queries(key, part):
    base_key = jax.random.fold_in(key, 21)
    values = jnp.clip(2.0 * jax.random.normal(base_key, (Q, E), jnp.float32), -12.0, 12.0)
    return values.astype(jnp.bfloat16)


def block_scale(own_key, dims, split, low, largest):
    level = 1.0
    for position, shards_of in split:
        draws = jax.random.uniform(jax.random.fold_in(jax.random.fold_in(own_key, 6), position), (shards_of,), jnp.float32, low / len(split), largest / len(split))
        level = level * jnp.repeat(jnp.exp(draws), dims[position] // shards_of).reshape((-1,) + (1,) * (len(dims) - 1 - position))
    return level


def centred(key, shape, deviation, reach, cuts=(), held_as=jnp.bfloat16):
    drawn = jax.random.normal(key, shape, jnp.float32) * deviation
    if len(cuts) > 0:
        drawn = block_scale(key, shape, cuts, -0.22, 0.18) * drawn
    return jnp.clip(drawn, min=-reach, max=reach).astype(held_as)


def setup_inputs(seed: int = 0, part: int = 0) -> dict:
    key_of = jax.random.split(jax.random.key(seed), 11)
    part_keys = jax.random.split(jax.random.fold_in(key_of[10], part), 11)
    return {
        "features": centred(part_keys[0], (GH, GW, C), 1.0, 6.0, ((0, 4), (1, 4))),
        "tissue": draw_tissue(jax.random.fold_in(jax.random.fold_in(key_of[10], part), 71), part),
        "conv_first": centred(key_of[2], (3, 3, C, C), (4 * C) ** -0.5, 0.1875),
        "bias_first": centred(key_of[3], (C,), 0.5, 3.0, (), jnp.float32),
        "conv_second": centred(key_of[4], (3, 3, C, C), (4 * C) ** -0.5, 0.1875),
        "bias_second": centred(key_of[5], (C,), 0.5, 3.0, (), jnp.float32),
        "key_weight": centred(key_of[6], (C, E), C ** -0.5, 0.375),
        "value_weight": centred(key_of[7], (C, E), C ** -0.5, 0.375),
        "latent_queries": draw_latent_queries(jax.random.fold_in(key_of[10], 71), part),
        "out_weight": centred(key_of[9], (E, E), E ** -0.5, 0.15625, ((1, 4),)),
    }


def convolve(field_in, weight):
    height, breadth, channels = field_in.shape
    padded = jnp.pad(field_in, ((1, 1), (1, 1), (0, 0)))
    summed = jnp.zeros((height * breadth, weight.shape[3]), jnp.float32)
    for offset_row in range(3):
        for offset_col in range(3):
            window = padded[offset_row:offset_row + height, offset_col:offset_col + breadth]
            summed = summed + jnp.dot(window.reshape(height * breadth, channels), weight[offset_row, offset_col], preferred_element_type=jnp.float32)
    return summed.reshape(height, breadth, weight.shape[3])

def reference(features, tissue, conv_first, bias_first, conv_second, bias_second, key_weight, value_weight, latent_queries, out_weight):
    keep_half = tissue.astype(jnp.bfloat16)
    keep_float = tissue.astype(jnp.float32)[:, :, None]
    inputs = features * keep_half[:, :, None]
    hidden = (jax.nn.gelu(convolve(inputs, conv_first) + bias_first, approximate=False) * keep_float).astype(jnp.bfloat16)
    second = (jax.nn.gelu(convolve(hidden, conv_second) + bias_second, approximate=False) * keep_float).astype(jnp.bfloat16)
    flattened = second.reshape(-1, second.shape[2])
    key_rows = jnp.dot(flattened, key_weight, preferred_element_type=jnp.float32).astype(jnp.bfloat16)
    scale = 1.0 / math.sqrt(latent_queries.shape[1])
    scores = lax.dot_general(latent_queries, key_rows, (((1,), (1,)), ((), ())), preferred_element_type=jnp.float32) * scale
    living = tissue.reshape(-1) > 0
    scores = jnp.where(living[None, :], scores, -1e+30)
    top_score = lax.optimization_barrier(jnp.max(scores, axis=1, keepdims=True))
    weights = jnp.exp(scores - top_score)
    denominator = lax.optimization_barrier(jnp.sum(weights, axis=1, keepdims=True))
    pooled = jnp.dot(weights.astype(jnp.bfloat16), flattened, preferred_element_type=jnp.float32)
    normalized = (pooled / denominator).astype(jnp.bfloat16)
    attended = jnp.dot(normalized, value_weight, preferred_element_type=jnp.float32).astype(jnp.bfloat16)
    return jnp.dot(attended, out_weight, preferred_element_type=jnp.float32).astype(jnp.bfloat16)
```

```python
import math

import jax
import jax.numpy as jnp
from jax import lax
from jax.sharding import PartitionSpec as P

HALO = 2
FAR = float("inf")


def shifted(array, axis, step):
    count = lax.axis_size(axis)
    return lax.ppermute(array, axis, [(i, (i + step) % count) for i in range(count)])


def flipped(array, axis, bit):
    count = lax.axis_size(axis)
    return lax.ppermute(array, axis, [(i, i ^ bit) for i in range(count)])


def with_halo(cells, axis, dim):
    size = cells.shape[dim]
    index, last = lax.axis_index(axis), lax.axis_size(axis) - 1
    before = shifted(lax.slice_in_dim(cells, size - HALO, size, axis=dim), axis, 1)
    after = shifted(lax.slice_in_dim(cells, 0, HALO, axis=dim), axis, -1)
    far = jnp.asarray(FAR, cells.dtype)
    return jnp.concatenate(
        [jnp.where(index == 0, far, before), cells, jnp.where(index == last, far, after)], axis=dim
    )


def convolve_valid(padded, weight):
    height, breadth = padded.shape[0] - 2, padded.shape[1] - 2
    channels = padded.shape[2]
    summed = jnp.zeros((height * breadth, weight.shape[3]), jnp.float32)
    for offset_row in range(3):
        for offset_col in range(3):
            window = padded[offset_row : offset_row + height, offset_col : offset_col + breadth]
            summed = summed + jnp.dot(
                window.reshape(height * breadth, channels),
                weight[offset_row, offset_col],
                preferred_element_type=jnp.float32,
            )
    return summed.reshape(height, breadth, weight.shape[3])


def rotated(parts, offset, step):
    count = len(parts)
    size = parts[0].shape[0]
    ordered = [parts[(step * k) % count] for k in range(count)]
    twice = jnp.concatenate(ordered + ordered[:-1], axis=0)
    return lax.dynamic_slice_in_dim(twice, ((count - offset) % count) * size, count * size, axis=0)


def gathered_queries(latent_queries):
    rows, cols = lax.axis_size("row"), lax.axis_size("col")
    parts = [latent_queries] + [shifted(latent_queries, "row", k) for k in range(1, rows)]
    queries = rotated(parts, lax.axis_index("row"), -1)
    own = lax.axis_index("col")
    bit = cols // 2
    groups = [queries]
    order = [0]
    while bit > 0:
        groups = groups + list(flipped(jnp.concatenate(groups, axis=0), "col", bit).reshape(len(groups), -1, queries.shape[1]))
        order = order + [place ^ bit for place in order]
        bit //= 2
    stacked = jnp.stack(groups)
    place = jnp.asarray([order.index(k) for k in range(cols)], jnp.int32)
    return stacked[place[own ^ jnp.arange(cols)]].reshape(-1, queries.shape[1])


def in_parts(values, count):
    parts = []
    for _ in range(count):
        part = lax.reduce_precision(values, exponent_bits=8, mantissa_bits=7)
        parts.append(part.astype(jnp.bfloat16))
        values = values - part
    return parts


def packed(pooled, top, total):
    rest = jnp.zeros((11, pooled.shape[1]), jnp.bfloat16)
    return jnp.concatenate(
        [pooled.astype(jnp.bfloat16)] + in_parts(top, 3) + in_parts(total, 2) + [rest], axis=0
    )


def unpacked(block, channels):
    wide = block.astype(jnp.float32)
    row = lambda k: wide[channels + k : channels + k + 1]
    return wide[:channels], row(0) + row(1) + row(2), row(3) + row(4)


def merged(partials):
    top = partials[0][1]
    for _, other, _ in partials[1:]:
        top = jnp.maximum(top, other)
    pooled = total = 0.0
    for part, shift, count in partials:
        factor = jnp.exp(shift - top)
        pooled = pooled + part * factor
        total = total + count * factor
    return pooled, top, total


def shards(
    features,
    tissue,
    conv_first,
    bias_first,
    conv_second,
    bias_second,
    key_weight,
    value_weight,
    latent_queries,
    out_weight,
):
    height, breadth, channels = features.shape
    rows = lax.axis_size("row")
    marked = jnp.where(tissue[:, :, None] > 0, features, jnp.asarray(FAR, features.dtype))
    marked = with_halo(with_halo(marked, "row", 0), "col", 1)
    queries = gathered_queries(latent_queries)
    alive = marked < FAR
    inputs = jnp.where(alive, marked, jnp.zeros_like(marked))
    hidden = jax.nn.gelu(convolve_valid(inputs, conv_first) + bias_first, approximate=False)
    hidden = jnp.where(alive[1:-1, 1:-1], hidden, 0.0).astype(jnp.bfloat16)
    second = jax.nn.gelu(convolve_valid(hidden, conv_second) + bias_second, approximate=False)
    second = jnp.where(alive[HALO:-HALO, HALO:-HALO], second, 0.0).astype(jnp.bfloat16)
    flattened = second.reshape(height * breadth, channels)
    key_rows = jnp.dot(flattened, key_weight, preferred_element_type=jnp.float32).astype(
        jnp.bfloat16
    )
    scale = 1.0 / math.sqrt(latent_queries.shape[1])
    scores = (
        lax.dot_general(
            key_rows, queries, (((1,), (1,)), ((), ())), preferred_element_type=jnp.float32
        )
        * scale
    )
    scores = jnp.where(tissue.reshape(-1, 1) > 0, scores, -1e30)
    shift = jnp.max(scores, axis=0, keepdims=True)
    weights = jnp.exp(scores - shift)
    total = jnp.sum(weights, axis=0, keepdims=True)
    pooled = lax.dot_general(
        flattened,
        weights.astype(jnp.bfloat16),
        (((0,), (0,)), ((), ())),
        preferred_element_type=jnp.float32,
    )

    own_row = lax.axis_index("row")
    size = pooled.shape[1] // rows

    def block_of(step):
        start = ((own_row + step) % rows) * size
        cut = lambda array: lax.dynamic_slice_in_dim(array, start, size, axis=1)
        return cut(pooled), cut(shift), cut(total)

    arrived = [shifted(packed(*block_of(k)), "row", k) for k in range(1, rows)]
    partial = merged([block_of(0)] + [unpacked(block, channels) for block in arrived])
    bit = lax.axis_size("col") // 2
    while bit > 0:
        other = flipped(packed(*partial), "col", bit)
        partial = merged([partial, unpacked(other, channels)])
        bit //= 2
    normalized = (partial[0] / partial[2]).astype(jnp.bfloat16)
    attended = lax.dot_general(
        normalized, value_weight, (((0,), (0,)), ((), ())), preferred_element_type=jnp.float32
    ).astype(jnp.bfloat16)
    return jnp.dot(attended, out_weight, preferred_element_type=jnp.float32).astype(jnp.bfloat16)


def solution(mesh):
    placed = (
        P(("groups", "row"), "col", None),
        P(("groups", "row"), "col"),
        P(),
        P(),
        P(),
        P(),
        P(),
        P(),
        P(("col", "row"), None),
        P(None, "col"),
    )
    return jax.shard_map(
        shards, mesh=mesh, in_specs=placed, out_specs=P(("groups", "row"), "col"), check_vma=False
    )
```

```python
import functools
import math

import jax
import jax.numpy as jnp
from jax import lax
from jax.experimental import pallas as pl
from jax.experimental.pallas import tpu as pltpu
from jax.sharding import PartitionSpec as P

HALO = 2
FAR = float("inf")
EDGE = 8
LEAD = 16


def shifted(array, axis, step):
    count = lax.axis_size(axis)
    return lax.ppermute(array, axis, [(i, (i + step) % count) for i in range(count)])


def flipped(array, axis, bit):
    count = lax.axis_size(axis)
    return lax.ppermute(array, axis, [(i, i ^ bit) for i in range(count)])


def with_halo(cells, axis, dim):
    size = cells.shape[dim]
    index, last = lax.axis_index(axis), lax.axis_size(axis) - 1
    before = shifted(lax.slice_in_dim(cells, size - HALO, size, axis=dim), axis, 1)
    after = shifted(lax.slice_in_dim(cells, 0, HALO, axis=dim), axis, -1)
    far = jnp.asarray(FAR, cells.dtype)
    return jnp.concatenate(
        [jnp.where(index == 0, far, before), cells, jnp.where(index == last, far, after)], axis=dim
    )


def convolve_valid(padded, weight):
    height, breadth = padded.shape[0] - 2, padded.shape[1] - 2
    channels = padded.shape[2]
    summed = jnp.zeros((height * breadth, weight.shape[3]), jnp.float32)
    for offset_row in range(3):
        for offset_col in range(3):
            window = padded[offset_row : offset_row + height, offset_col : offset_col + breadth]
            summed = summed + jnp.dot(
                window.reshape(height * breadth, channels),
                weight[offset_row, offset_col],
                preferred_element_type=jnp.float32,
            )
    return summed.reshape(height, breadth, weight.shape[3])


def rotated(parts, offset, step):
    count = len(parts)
    size = parts[0].shape[0]
    ordered = [parts[(step * k) % count] for k in range(count)]
    twice = jnp.concatenate(ordered + ordered[:-1], axis=0)
    return lax.dynamic_slice_in_dim(twice, ((count - offset) % count) * size, count * size, axis=0)


def gathered_queries(latent_queries):
    rows, cols = lax.axis_size("row"), lax.axis_size("col")
    parts = [latent_queries] + [shifted(latent_queries, "row", k) for k in range(1, rows)]
    queries = rotated(parts, lax.axis_index("row"), -1)
    own = lax.axis_index("col")
    bit = cols // 2
    groups = [queries]
    order = [0]
    while bit > 0:
        groups = groups + list(flipped(jnp.concatenate(groups, axis=0), "col", bit).reshape(len(groups), -1, queries.shape[1]))
        order = order + [place ^ bit for place in order]
        bit //= 2
    stacked = jnp.stack(groups)
    place = jnp.asarray([order.index(k) for k in range(cols)], jnp.int32)
    return stacked[place[own ^ jnp.arange(cols)]].reshape(-1, queries.shape[1])


def in_parts(values, count):
    parts = []
    for _ in range(count):
        part = lax.reduce_precision(values, exponent_bits=8, mantissa_bits=7)
        parts.append(part.astype(jnp.bfloat16))
        values = values - part
    return parts


def packed(pooled, top, total):
    rest = jnp.zeros((11, pooled.shape[1]), jnp.bfloat16)
    return jnp.concatenate(
        [pooled.astype(jnp.bfloat16)] + in_parts(top, 3) + in_parts(total, 2) + [rest], axis=0
    )


def unpacked(block, channels):
    wide = block.astype(jnp.float32)
    row = lambda k: wide[channels + k : channels + k + 1]
    return wide[:channels], row(0) + row(1) + row(2), row(3) + row(4)


def merged(partials):
    top = partials[0][1]
    for _, other, _ in partials[1:]:
        top = jnp.maximum(top, other)
    pooled = total = 0.0
    for part, shift, count in partials:
        factor = jnp.exp(shift - top)
        pooled = pooled + part * factor
        total = total + count * factor
    return pooled, top, total


def plain_attend(features, tissue, marked, latent_queries, weights):
    conv_first, bias_first, conv_second, bias_second, key_weight = weights
    height, breadth, channels = features.shape
    rows = lax.axis_size("row")
    queries = gathered_queries(latent_queries)
    alive = marked < FAR
    inputs = jnp.where(alive, marked, jnp.zeros_like(marked))
    hidden = jax.nn.gelu(convolve_valid(inputs, conv_first) + bias_first, approximate=False)
    hidden = jnp.where(alive[1:-1, 1:-1], hidden, 0.0).astype(jnp.bfloat16)
    second = jax.nn.gelu(convolve_valid(hidden, conv_second) + bias_second, approximate=False)
    second = jnp.where(alive[HALO:-HALO, HALO:-HALO], second, 0.0).astype(jnp.bfloat16)
    flattened = second.reshape(height * breadth, channels)
    key_rows = jnp.dot(flattened, key_weight, preferred_element_type=jnp.float32).astype(
        jnp.bfloat16
    )
    scale = 1.0 / math.sqrt(latent_queries.shape[1])
    scores = (
        lax.dot_general(
            key_rows, queries, (((1,), (1,)), ((), ())), preferred_element_type=jnp.float32
        )
        * scale
    )
    scores = jnp.where(tissue.reshape(-1, 1) > 0, scores, -1e30)
    shift = jnp.max(scores, axis=0, keepdims=True)
    chosen = jnp.exp(scores - shift)
    total = jnp.sum(chosen, axis=0, keepdims=True)
    pooled = lax.dot_general(
        flattened,
        chosen.astype(jnp.bfloat16),
        (((0,), (0,)), ((), ())),
        preferred_element_type=jnp.float32,
    )

    own_row = lax.axis_index("row")
    size = pooled.shape[1] // rows

    def block_of(step):
        start = ((own_row + step) % rows) * size
        cut = lambda array: lax.dynamic_slice_in_dim(array, start, size, axis=1)
        return cut(pooled), cut(shift), cut(total)

    arrived = [shifted(packed(*block_of(k)), "row", k) for k in range(1, rows)]
    partial = merged([block_of(0)] + [unpacked(block, channels) for block in arrived])
    bit = lax.axis_size("col") // 2
    while bit > 0:
        other = flipped(packed(*partial), "col", bit)
        partial = merged([partial, unpacked(other, channels)])
        bit //= 2
    normalized = (partial[0] / partial[2]).astype(jnp.bfloat16)
    return normalized


def gelu(value):
    return 0.5 * value * (1.0 + lax.erf(value * math.sqrt(0.5)))


def conv_kernel(
    marked, top, bottom, left, right, first, bias_first, second, bias_second, key_weight,
    out, keys, cells, mid, taps,
):
    height, breadth, channels = marked.shape
    slot = (cells.shape[0] - 2 * EDGE - LEAD) // (height + 2 * HALO)
    flat = cells.shape[0] - 2 * EDGE
    row, col = lax.axis_index("row"), lax.axis_index("col")
    first_row, last_row = row == 0, row == lax.axis_size("row") - 1
    first_col, last_col = col == 0, col == lax.axis_size("col") - 1

    def put(line, place, values, outside):
        start = EDGE + LEAD + line * slot + place
        values = values.astype(jnp.float32)
        if outside is not None:
            values = jnp.where(outside, FAR, values)
        cells[start : start + values.shape[0], :] = values

    cells[...] = jnp.full(cells.shape, FAR, jnp.float32)
    for line in range(height):
        put(line + HALO, 0, marked[line], None)
    for line in range(HALO):
        put(line, 0, top[line], first_row)
        put(height + HALO + line, 0, bottom[line], last_row)
    for line in range(height + 2 * HALO):
        beyond_left, beyond_right = first_col, last_col
        if line < HALO:
            beyond_left, beyond_right = first_col | first_row, last_col | first_row
        if line >= height + HALO:
            beyond_left, beyond_right = first_col | last_row, last_col | last_row
        put(line, -HALO, left[line], beyond_left)
        put(line, breadth, right[line], beyond_right)

    for shift in range(3):
        values = cells[EDGE - 1 + shift : EDGE - 1 + shift + flat, :]
        taps[:, shift * channels : (shift + 1) * channels] = jnp.where(
            values < FAR, values, 0.0
        ).astype(jnp.bfloat16)

    count = flat - 2 * slot
    summed = jnp.dot(taps[0:count, :], first[0], preferred_element_type=jnp.float32)
    for line in range(1, 3):
        summed = summed + jnp.dot(
            taps[line * slot : line * slot + count, :], first[line],
            preferred_element_type=jnp.float32,
        )
    alive = cells[EDGE + slot : EDGE + slot + count, :] < FAR
    edge = jnp.zeros((EDGE, channels), jnp.float32)
    mid[0:EDGE, :] = edge
    mid[EDGE + count : 2 * EDGE + count, :] = edge
    mid[EDGE : EDGE + count, :] = jnp.where(alive, gelu(summed + bias_first[...]), 0.0)

    for shift in range(3):
        taps[0:count, shift * channels : (shift + 1) * channels] = mid[
            EDGE - 1 + shift : EDGE - 1 + shift + count, :
        ].astype(jnp.bfloat16)
    inner = height * slot
    summed = jnp.dot(taps[LEAD : LEAD + inner, :], second[0], preferred_element_type=jnp.float32)
    for line in range(1, 3):
        summed = summed + jnp.dot(
            taps[LEAD + line * slot : LEAD + line * slot + inner, :], second[line],
            preferred_element_type=jnp.float32,
        )
    summed = summed.reshape(height, slot, channels)[:, :breadth].reshape(height * breadth, channels)
    alive = marked[...].reshape(height * breadth, channels) < FAR
    out[...] = jnp.where(alive, gelu(summed + bias_second[...]), 0.0).astype(jnp.bfloat16)
    keys[...] = jnp.dot(out[...], key_weight[...], preferred_element_type=jnp.float32).astype(
        jnp.bfloat16
    )


def write_parts(block, values, top, total):
    channels = values.shape[0]
    parts = []
    for source, count in ((top, 3), (total, 2)):
        rest = source
        for _ in range(count):
            part = rest.astype(jnp.bfloat16).astype(jnp.float32)
            parts.append(part)
            rest = rest - part
    parts.append(jnp.zeros((block.shape[0] - channels - 5, values.shape[1]), jnp.float32))
    block[0:channels, :] = values.astype(jnp.bfloat16)
    block[channels:, :] = jnp.concatenate(parts, axis=0).astype(jnp.bfloat16)


def read_parts(block):
    channels = block.shape[0] - 16
    tail = block[channels:, :].astype(jnp.float32)
    row = lambda k: tail[k : k + 1]
    return (
        block[0:channels, :].astype(jnp.float32),
        row(0) + row(1) + row(2),
        row(3) + row(4),
    )


def read_whole(block):
    channels = block.shape[0] - 8
    tail = block[channels:, :]
    return block[0:channels, :], tail[0:1], tail[1:2]


def write_whole(block, values, top, total):
    channels = values.shape[0]
    block[0:channels, :] = values
    block[channels:, :] = jnp.concatenate(
        [top, total, jnp.zeros((6, values.shape[1]), jnp.float32)], axis=0
    )


def score_blocks(cells, keys, marked, queries, scale):
    scores = lax.dot_general(
        keys[...], queries, (((1,), (1,)), ((), ())), preferred_element_type=jnp.float32
    )
    alive = marked[...] < FAR
    if alive.shape != scores.shape:
        alive = jnp.broadcast_to(alive[:, :1], scores.shape)
    scores = jnp.where(alive, scores * scale, -1e30)
    top = jnp.max(scores, axis=0, keepdims=True)
    chosen = jnp.exp(scores - top)
    total = jnp.sum(chosen, axis=0, keepdims=True)
    pooled = lax.dot_general(
        cells[...], chosen.astype(jnp.bfloat16), (((0,), (0,)), ((), ())),
        preferred_element_type=jnp.float32,
    )
    return pooled, top, total


def score_kernel(cells, keys, marked, *refs):
    *queries, out, held = refs
    size = queries[0].shape[0]
    for place, part in enumerate(queries):
        held[place * size : (place + 1) * size, :] = part[...]
    pooled, top, total = score_blocks(
        cells, keys, marked, held[...], 1.0 / math.sqrt(held.shape[1])
    )
    for place in range(len(queries)):
        cut = slice(place * size, (place + 1) * size)
        write_whole(out.at[place], pooled[:, cut], top[:, cut], total[:, cut])


def spread_kernel(count, size, *refs):
    held, own, sends, all_blocks = refs[:-count - 1], refs[-count - 1], refs[-count : -1], refs[-1]
    done = 0
    for part in held:
        all_blocks[done : done + part.shape[0]] = part[...]
        done += part.shape[0]
    row, col = lax.axis_index("row"), lax.axis_index("col")
    for step in range(count):
        block = all_blocks[lax.rem(row + step, count) ^ col]
        block = pltpu.roll(block, lax.rem(row + 1, count) * size, 1)
        channels = block.shape[0] - 8
        if step == 0:
            own[...] = block
        else:
            write_parts(
                sends[step - 1],
                block[:channels],
                block[channels : channels + 1],
                block[channels + 1 : channels + 2],
            )


def merge_kernel(own, *refs):
    *arrived, whole, packed_out = refs
    values, top, total = merged([read_whole(own)] + [read_parts(block) for block in arrived])
    write_whole(whole, values, top, total)
    write_parts(packed_out, values, top, total)


def finish_kernel(own, arrived, value_weight, out_weight, out):
    values, _, total = merged([read_whole(own), read_parts(arrived)])
    normalized = (values / total).astype(jnp.bfloat16)
    attended = lax.dot_general(
        normalized, value_weight[...], (((0,), (0,)), ((), ())),
        preferred_element_type=jnp.float32,
    ).astype(jnp.bfloat16)
    out[...] = jnp.dot(
        attended, out_weight[...], preferred_element_type=jnp.float32
    ).astype(out.dtype)


def shape_of(*dims, dtype=jnp.bfloat16):
    return jax.ShapeDtypeStruct(dims, dtype)


def kernel_path(
    features, tissue, conv_first, bias_first, conv_second, bias_second, key_weight,
    value_weight, latent_queries, out_weight,
):
    height, breadth, channels = features.shape
    rows, cols = lax.axis_size("row"), lax.axis_size("col")
    width = latent_queries.shape[1]
    cells = height * breadth
    slot = -(-(breadth + 2 * HALO) // 16) * 16
    flat = LEAD + (height + 2 * HALO) * slot

    with jax.named_scope("query_rows"):
        turned = [shifted(latent_queries, "row", k) for k in range(1, rows)]
    marked = jnp.where(tissue[:, :, None] > 0, features, jnp.asarray(FAR, features.dtype))
    with jax.named_scope("halo_rows"):
        top = shifted(marked[height - HALO :], "row", 1)
        bottom = shifted(marked[:HALO], "row", -1)
    edge = lambda cut: jnp.concatenate([top[:, cut], marked[:, cut], bottom[:, cut]], axis=0)
    with jax.named_scope("halo_cols"):
        left = shifted(edge(slice(breadth - HALO, breadth)), "col", 1)
        right = shifted(edge(slice(0, HALO)), "col", -1)

    own_column = jnp.concatenate(turned[::-1] + [latent_queries], axis=0)
    block = own_column.shape[0]
    blocks = [own_column]
    bit = cols // 2
    pairs = []
    with jax.named_scope("query_cols"):
        across = flipped(own_column, "col", 2)
        beside = flipped(own_column, "col", 1)
        diagonal = flipped(across, "col", 1)

    second, keys = pl.pallas_call(
        conv_kernel,
        out_shape=(shape_of(cells, channels), shape_of(cells, width)),
        scratch_shapes=[
            pltpu.VMEM((flat + 2 * EDGE, channels), jnp.float32),
            pltpu.VMEM((flat - 2 * slot + 2 * EDGE, channels), jnp.float32),
            pltpu.VMEM((flat, 3 * channels), jnp.bfloat16),
        ],
        name="convolve",
    )(
        marked, top, bottom, left, right,
        conv_first.reshape(3, 3 * channels, channels), bias_first.reshape(1, channels),
        conv_second.reshape(3, 3 * channels, channels), bias_second.reshape(1, channels),
        key_weight,
    )
    alive = marked.reshape(cells, channels)
    score = lambda *queries: pl.pallas_call(
        score_kernel,
        out_shape=shape_of(len(queries), channels + 8, block, dtype=jnp.float32),
        scratch_shapes=[pltpu.VMEM((len(queries) * block, width), jnp.bfloat16)],
        name="score",
    )(second, keys, alive, *queries)
    near, far = score(own_column, beside), score(across, diagonal)
    own, *sends = pl.pallas_call(
        functools.partial(spread_kernel, cols, latent_queries.shape[0]),
        out_shape=[shape_of(channels + 8, block, dtype=jnp.float32)]
        + [shape_of(channels + 16, block)] * (rows - 1),
        scratch_shapes=[pltpu.VMEM((cols, channels + 8, block), jnp.float32)],
        name="spread",
    )(near, far)
    with jax.named_scope("pool_rows"):
        arrived = [shifted(part, "row", k + 1) for k, part in enumerate(sends)]
    merge = lambda *parts: pl.pallas_call(
        merge_kernel,
        out_shape=[shape_of(channels + 8, block, dtype=jnp.float32), shape_of(channels + 16, block)],
        name="merge",
    )(*parts)
    own, packed_own = merge(own, *arrived)
    with jax.named_scope("pool_across"):
        arrived = flipped(packed_own, "col", 2)
    own, packed_own = merge(own, arrived)
    with jax.named_scope("pool_beside"):
        arrived = flipped(packed_own, "col", 1)
    return pl.pallas_call(
        finish_kernel,
        out_shape=shape_of(block, out_weight.shape[1]),
        name="finish",
    )(own, arrived, value_weight, out_weight)


def shards(
    features, tissue, conv_first, bias_first, conv_second, bias_second, key_weight,
    value_weight, latent_queries, out_weight,
):
    rows, cols = lax.axis_size("row"), lax.axis_size("col")
    if rows == cols == 4 and (rows * latent_queries.shape[0]) % 128 == 0:
        return kernel_path(
            features, tissue, conv_first, bias_first, conv_second, bias_second, key_weight,
            value_weight, latent_queries, out_weight,
        )
    marked = jnp.where(tissue[:, :, None] > 0, features, jnp.asarray(FAR, features.dtype))
    marked = with_halo(with_halo(marked, "row", 0), "col", 1)
    normalized = plain_attend(
        features, tissue, marked, latent_queries,
        (conv_first, bias_first, conv_second, bias_second, key_weight),
    )
    attended = lax.dot_general(
        normalized, value_weight, (((0,), (0,)), ((), ())), preferred_element_type=jnp.float32
    ).astype(jnp.bfloat16)
    return jnp.dot(attended, out_weight, preferred_element_type=jnp.float32).astype(jnp.bfloat16)


def solution(mesh):
    placed = (
        P(("groups", "row"), "col", None),
        P(("groups", "row"), "col"),
        P(),
        P(),
        P(),
        P(),
        P(),
        P(),
        P(("col", "row"), None),
        P(None, "col"),
    )
    return jax.shard_map(
        shards, mesh=mesh, in_specs=placed, out_specs=P(("groups", "row"), "col"), check_vma=False
    )
```

```python
import math

import jax
import jax.numpy as jnp
from jax import lax
from jax.experimental import pallas as pl
from jax.experimental.pallas import tpu as pltpu
from jax.sharding import PartitionSpec as P


HALO = 2
FAR = float("inf")
EDGE = 8
LEAD = 16


def shifted(array, axis, step):
    count = lax.axis_size(axis)
    return lax.ppermute(array, axis, [(i, (i + step) % count) for i in range(count)])


def flipped(array, axis, bit):
    count = lax.axis_size(axis)
    return lax.ppermute(array, axis, [(i, i ^ bit) for i in range(count)])


def with_halo(cells, axis, dim):
    size = cells.shape[dim]
    index, last = lax.axis_index(axis), lax.axis_size(axis) - 1
    before = shifted(lax.slice_in_dim(cells, size - HALO, size, axis=dim), axis, 1)
    after = shifted(lax.slice_in_dim(cells, 0, HALO, axis=dim), axis, -1)
    far = jnp.asarray(FAR, cells.dtype)
    return jnp.concatenate(
        [jnp.where(index == 0, far, before), cells, jnp.where(index == last, far, after)], axis=dim
    )


def convolve_valid(padded, weight):
    height, breadth = padded.shape[0] - 2, padded.shape[1] - 2
    channels = padded.shape[2]
    summed = jnp.zeros((height * breadth, weight.shape[3]), jnp.float32)
    for offset_row in range(3):
        for offset_col in range(3):
            window = padded[offset_row : offset_row + height, offset_col : offset_col + breadth]
            summed = summed + jnp.dot(
                window.reshape(height * breadth, channels),
                weight[offset_row, offset_col],
                preferred_element_type=jnp.float32,
            )
    return summed.reshape(height, breadth, weight.shape[3])


def rotated(parts, offset, step):
    count = len(parts)
    size = parts[0].shape[0]
    ordered = [parts[(step * k) % count] for k in range(count)]
    twice = jnp.concatenate(ordered + ordered[:-1], axis=0)
    return lax.dynamic_slice_in_dim(twice, ((count - offset) % count) * size, count * size, axis=0)


def gathered_queries(latent_queries):
    rows, cols = lax.axis_size("row"), lax.axis_size("col")
    parts = [latent_queries] + [shifted(latent_queries, "row", k) for k in range(1, rows)]
    queries = rotated(parts, lax.axis_index("row"), -1)
    own = lax.axis_index("col")
    bit = cols // 2
    groups = [queries]
    order = [0]
    while bit > 0:
        groups = groups + list(flipped(jnp.concatenate(groups, axis=0), "col", bit).reshape(len(groups), -1, queries.shape[1]))
        order = order + [place ^ bit for place in order]
        bit //= 2
    stacked = jnp.stack(groups)
    place = jnp.asarray([order.index(k) for k in range(cols)], jnp.int32)
    return stacked[place[own ^ jnp.arange(cols)]].reshape(-1, queries.shape[1])


def in_parts(values, count):
    parts = []
    for _ in range(count):
        part = lax.reduce_precision(values, exponent_bits=8, mantissa_bits=7)
        parts.append(part.astype(jnp.bfloat16))
        values = values - part
    return parts


def packed(pooled, top, total):
    rest = jnp.zeros((11, pooled.shape[1]), jnp.bfloat16)
    return jnp.concatenate(
        [pooled.astype(jnp.bfloat16)] + in_parts(top, 3) + in_parts(total, 2) + [rest], axis=0
    )


def unpacked(block, channels):
    wide = block.astype(jnp.float32)
    row = lambda k: wide[channels + k : channels + k + 1]
    return wide[:channels], row(0) + row(1) + row(2), row(3) + row(4)


def merged(partials):
    top = partials[0][1]
    for _, other, _ in partials[1:]:
        top = jnp.maximum(top, other)
    pooled = total = 0.0
    for part, shift, count in partials:
        factor = jnp.exp(shift - top)
        pooled = pooled + part * factor
        total = total + count * factor
    return pooled, top, total


def plain_attend(features, tissue, marked, latent_queries, weights):
    conv_first, bias_first, conv_second, bias_second, key_weight = weights
    height, breadth, channels = features.shape
    rows = lax.axis_size("row")
    queries = gathered_queries(latent_queries)
    alive = marked < FAR
    inputs = jnp.where(alive, marked, jnp.zeros_like(marked))
    hidden = jax.nn.gelu(convolve_valid(inputs, conv_first) + bias_first, approximate=False)
    hidden = jnp.where(alive[1:-1, 1:-1], hidden, 0.0).astype(jnp.bfloat16)
    second = jax.nn.gelu(convolve_valid(hidden, conv_second) + bias_second, approximate=False)
    second = jnp.where(alive[HALO:-HALO, HALO:-HALO], second, 0.0).astype(jnp.bfloat16)
    flattened = second.reshape(height * breadth, channels)
    key_rows = jnp.dot(flattened, key_weight, preferred_element_type=jnp.float32).astype(
        jnp.bfloat16
    )
    scale = 1.0 / math.sqrt(latent_queries.shape[1])
    scores = (
        lax.dot_general(
            key_rows, queries, (((1,), (1,)), ((), ())), preferred_element_type=jnp.float32
        )
        * scale
    )
    scores = jnp.where(tissue.reshape(-1, 1) > 0, scores, -1e30)
    shift = jnp.max(scores, axis=0, keepdims=True)
    chosen = jnp.exp(scores - shift)
    total = jnp.sum(chosen, axis=0, keepdims=True)
    pooled = lax.dot_general(
        flattened,
        chosen.astype(jnp.bfloat16),
        (((0,), (0,)), ((), ())),
        preferred_element_type=jnp.float32,
    )

    own_row = lax.axis_index("row")
    size = pooled.shape[1] // rows

    def block_of(step):
        start = ((own_row + step) % rows) * size
        cut = lambda array: lax.dynamic_slice_in_dim(array, start, size, axis=1)
        return cut(pooled), cut(shift), cut(total)

    arrived = [shifted(packed(*block_of(k)), "row", k) for k in range(1, rows)]
    partial = merged([block_of(0)] + [unpacked(block, channels) for block in arrived])
    bit = lax.axis_size("col") // 2
    while bit > 0:
        other = flipped(packed(*partial), "col", bit)
        partial = merged([partial, unpacked(other, channels)])
        bit //= 2
    normalized = (partial[0] / partial[2]).astype(jnp.bfloat16)
    return normalized


def gelu(value):
    return 0.5 * value * (1.0 + lax.erf(value * math.sqrt(0.5)))


def conv_kernel(
    marked, top, bottom, left, right, first, bias_first, second, bias_second, key_weight,
    out, keys, cells, mid, taps, second_held, key_held, done,
):
    later = [
        pltpu.make_async_copy(second, second_held, done.at[0]),
        pltpu.make_async_copy(key_weight, key_held, done.at[1]),
    ]
    for copy in later:
        copy.start()
    height, breadth, channels = marked.shape
    slot = (cells.shape[0] - 2 * EDGE - LEAD) // (height + 2 * HALO)
    flat = cells.shape[0] - 2 * EDGE
    row, col = lax.axis_index("row"), lax.axis_index("col")
    first_row, last_row = row == 0, row == lax.axis_size("row") - 1
    first_col, last_col = col == 0, col == lax.axis_size("col") - 1

    def put(line, place, values, outside):
        start = EDGE + LEAD + line * slot + place
        values = values.astype(jnp.float32)
        if outside is not None:
            values = jnp.where(outside, FAR, values)
        cells[start : start + values.shape[0], :] = values

    cells[...] = jnp.full(cells.shape, FAR, jnp.float32)
    for line in range(height):
        put(line + HALO, 0, marked[line], None)
    for line in range(HALO):
        put(line, 0, top[line], first_row)
        put(height + HALO + line, 0, bottom[line], last_row)
    for line in range(height + 2 * HALO):
        beyond_left, beyond_right = first_col, last_col
        if line < HALO:
            beyond_left, beyond_right = first_col | first_row, last_col | first_row
        if line >= height + HALO:
            beyond_left, beyond_right = first_col | last_row, last_col | last_row
        put(line, -HALO, left[line], beyond_left)
        put(line, breadth, right[line], beyond_right)

    for shift in range(3):
        values = cells[EDGE - 1 + shift : EDGE - 1 + shift + flat, :]
        taps[:, shift * channels : (shift + 1) * channels] = jnp.where(
            values < FAR, values, 0.0
        ).astype(jnp.bfloat16)

    count = flat - 2 * slot
    summed = jnp.dot(taps[0:count, :], first[0], preferred_element_type=jnp.float32)
    for line in range(1, 3):
        summed = summed + jnp.dot(
            taps[line * slot : line * slot + count, :], first[line],
            preferred_element_type=jnp.float32,
        )
    alive = cells[EDGE + slot : EDGE + slot + count, :] < FAR
    edge = jnp.zeros((EDGE, channels), jnp.float32)
    mid[0:EDGE, :] = edge
    mid[EDGE + count : 2 * EDGE + count, :] = edge
    mid[EDGE : EDGE + count, :] = jnp.where(alive, gelu(summed + bias_first[...]), 0.0)

    for shift in range(3):
        taps[0:count, shift * channels : (shift + 1) * channels] = mid[
            EDGE - 1 + shift : EDGE - 1 + shift + count, :
        ].astype(jnp.bfloat16)
    inner = height * slot
    later[0].wait()
    summed = jnp.dot(
        taps[LEAD : LEAD + inner, :], second_held[0], preferred_element_type=jnp.float32
    )
    for line in range(1, 3):
        summed = summed + jnp.dot(
            taps[LEAD + line * slot : LEAD + line * slot + inner, :], second_held[line],
            preferred_element_type=jnp.float32,
        )
    summed = summed.reshape(height, slot, channels)[:, :breadth].reshape(height * breadth, channels)
    alive = marked[...].reshape(height * breadth, channels) < FAR
    out[...] = jnp.where(alive, gelu(summed + bias_second[...]), 0.0).astype(jnp.bfloat16)
    later[1].wait()
    keys[...] = jnp.dot(out[...], key_held[...], preferred_element_type=jnp.float32).astype(
        jnp.bfloat16
    )


def write_parts(block, values, top, total):
    channels = values.shape[0]
    parts = []
    for source, count in ((top, 3), (total, 2)):
        rest = source
        for _ in range(count):
            part = rest.astype(jnp.bfloat16).astype(jnp.float32)
            parts.append(part)
            rest = rest - part
    parts.append(jnp.zeros((block.shape[0] - channels - 5, values.shape[1]), jnp.float32))
    block[0:channels, :] = values.astype(jnp.bfloat16)
    block[channels:, :] = jnp.concatenate(parts, axis=0).astype(jnp.bfloat16)


def read_parts(block):
    channels = block.shape[0] - 16
    tail = block[channels:, :].astype(jnp.float32)
    row = lambda k: tail[k : k + 1]
    return (
        block[0:channels, :].astype(jnp.float32),
        row(0) + row(1) + row(2),
        row(3) + row(4),
    )


def read_whole(block):
    channels = block.shape[0] - 8
    tail = block[channels:, :]
    return block[0:channels, :], tail[0:1], tail[1:2]


def write_whole(block, values, top, total):
    channels = values.shape[0]
    block[0:channels, :] = values
    block[channels:, :] = jnp.concatenate(
        [top, total, jnp.zeros((6, values.shape[1]), jnp.float32)], axis=0
    )


def score_blocks(cells, keys, marked, queries, scale):
    scores = lax.dot_general(
        keys[...], queries, (((1,), (1,)), ((), ())), preferred_element_type=jnp.float32
    )
    alive = marked[...] < FAR
    if alive.shape != scores.shape:
        alive = jnp.broadcast_to(alive[:, :1], scores.shape)
    scores = jnp.where(alive, scores * scale, -1e30)
    top = jnp.max(scores, axis=0, keepdims=True)
    chosen = jnp.exp(scores - top)
    total = jnp.sum(chosen, axis=0, keepdims=True)
    pooled = lax.dot_general(
        cells[...], chosen.astype(jnp.bfloat16), (((0,), (0,)), ((), ())),
        preferred_element_type=jnp.float32,
    )
    return pooled, top, total


def score_kernel(cells, keys, marked, *refs):
    *queries, out, held = refs
    size = queries[0].shape[0]
    for place, part in enumerate(queries):
        held[place * size : (place + 1) * size, :] = part[...]
    pooled, top, total = score_blocks(
        cells, keys, marked, held[...], 1.0 / math.sqrt(held.shape[1])
    )
    for place in range(len(queries)):
        cut = slice(place * size, (place + 1) * size)
        write_whole(out.at[place], pooled[:, cut], top[:, cut], total[:, cut])


def last_score_kernel(rows, size, held, cells, keys, marked, queries, *refs):
    own, *sends, blocks = refs
    done = 0
    for part in held:
        blocks[done : done + part.shape[0]] = part[...]
        done += part.shape[0]
    pooled, top, total = score_blocks(
        cells, keys, marked, queries[...], 1.0 / math.sqrt(queries.shape[1])
    )
    write_whole(blocks.at[done], pooled, top, total)
    row, col = lax.axis_index("row"), lax.axis_index("col")
    for step in range(rows):
        block = blocks[lax.rem(row + step, rows) ^ col]
        block = pltpu.roll(block, lax.rem(row + 1, rows) * size, 1)
        channels = block.shape[0] - 8
        if step == 0:
            own[...] = block
        else:
            write_parts(
                sends[step - 1],
                block[:channels],
                block[channels : channels + 1],
                block[channels + 1 : channels + 2],
            )


def merge_kernel(own, *refs):
    *arrived, whole, packed_out = refs
    values, top, total = merged([read_whole(own)] + [read_parts(block) for block in arrived])
    write_whole(whole, values, top, total)
    write_parts(packed_out, values, top, total)


def finish_kernel(own, arrived, value_weight, out_weight, out):
    values, _, total = merged([read_whole(own), read_parts(arrived)])
    normalized = (values / total).astype(jnp.bfloat16)
    attended = lax.dot_general(
        normalized, value_weight[...], (((0,), (0,)), ((), ())),
        preferred_element_type=jnp.float32,
    ).astype(jnp.bfloat16)
    out[...] = lax.dot_general(
        out_weight[...], attended, (((1,), (1,)), ((), ())), preferred_element_type=jnp.float32
    ).astype(out.dtype)


MIB = 1 << 20


def call(kernel, outs, args, scratch=(), limit=4, flops=0, far=()):
    held = pl.BlockSpec(memory_space=pltpu.VMEM)
    outside = pl.BlockSpec(memory_space=pltpu.HBM)
    return pl.pallas_call(
        kernel,
        out_shape=[pltpu.VMEM(shape, dtype) for shape, dtype in outs],
        in_specs=[outside if k in far else held for k in range(len(args))],
        out_specs=[held] * len(outs),
        scratch_shapes=[
            pltpu.VMEM(*kind) if isinstance(kind, tuple) else kind for kind in scratch
        ],
        compiler_params=pltpu.CompilerParams(vmem_limit_bytes=limit * MIB),
        cost_estimate=pl.CostEstimate(flops=flops, bytes_accessed=0, transcendentals=0),
    )(
        *[
            pltpu.with_memory_space_constraint(arg, pltpu.HBM if k in far else pltpu.VMEM)
            for k, arg in enumerate(args)
        ]
    )


def kernel_path(
    features, tissue, conv_first, bias_first, conv_second, bias_second, key_weight,
    value_weight, latent_queries, out_weight,
):
    height, breadth, channels = features.shape
    rows, cols = lax.axis_size("row"), lax.axis_size("col")
    width = latent_queries.shape[1]
    cells = height * breadth
    slot = -(-(breadth + 2 * HALO) // 16) * 16
    flat = LEAD + (height + 2 * HALO) * slot
    wide, half = jnp.float32, jnp.bfloat16
    block = rows * latent_queries.shape[0]
    whole_block, sent_block = (channels + 8, block), (channels + 16, block)

    turned = [shifted(latent_queries, "row", k) for k in range(1, rows)]
    marked = jnp.where(tissue[:, :, None] > 0, features, jnp.asarray(FAR, features.dtype))
    top = shifted(marked[height - HALO :], "row", 1)
    bottom = shifted(marked[:HALO], "row", -1)
    edge = lambda cut: jnp.concatenate([top[:, cut], marked[:, cut], bottom[:, cut]], axis=0)
    left = shifted(edge(slice(breadth - HALO, breadth)), "col", 1)
    right = shifted(edge(slice(0, HALO)), "col", -1)

    own_column = jnp.concatenate(turned[::-1] + [latent_queries], axis=0)
    across = flipped(own_column, "col", 2)
    beside = flipped(own_column, "col", 1)
    diagonal = flipped(across, "col", 1)

    second, keys = call(
        conv_kernel, [((cells, channels), half), ((cells, width), half)],
        [
            marked, top, bottom, left, right,
            conv_first.reshape(3, 3 * channels, channels), bias_first.reshape(1, channels),
            conv_second.reshape(3, 3 * channels, channels), bias_second.reshape(1, channels),
            key_weight,
        ],
        [
            ((flat + 2 * EDGE, channels), wide),
            ((flat - 2 * slot + 2 * EDGE, channels), wide),
            ((flat, 3 * channels), half),
            ((3, 3 * channels, channels), half),
            ((channels, width), half),
            pltpu.SemaphoreType.DMA((2,)),
        ],
        limit=16, far=(7, 9), flops=2 * cells * channels * (21 * channels + width),
    )
    marked = marked.reshape(cells, channels)

    def score(*queries):
        return call(
            score_kernel, [((len(queries),) + whole_block, wide)],
            [second, keys, marked, *queries],
            [((len(queries) * block, width), half)],
            limit=8, flops=2 * cells * block * len(queries) * (width + channels),
        )[0]

    near = score(own_column, beside)
    far = score(across)

    def last(near, far, *rest):
        last_score_kernel(rows, latent_queries.shape[0], (near, far), *rest)

    own, *sends = call(
        last, [(whole_block, wide)] + [(sent_block, half)] * (rows - 1),
        [near, far, second, keys, marked, diagonal],
        [((cols,) + whole_block, wide)],
        limit=8, flops=2 * cells * block * (width + channels),
    )
    arrived = [shifted(part, "row", k + 1) for k, part in enumerate(sends)]
    merge = lambda *parts: call(merge_kernel, [(whole_block, wide), (sent_block, half)], parts)
    own, sent = merge(own, *arrived)
    arrived = flipped(sent, "col", 2)
    own, sent = merge(own, arrived)
    arrived = flipped(sent, "col", 1)
    held = pl.BlockSpec(memory_space=pltpu.VMEM)
    keep = lambda array: pltpu.with_memory_space_constraint(array, pltpu.VMEM)
    return pl.pallas_call(
        finish_kernel,
        out_shape=jax.ShapeDtypeStruct((out_weight.shape[1], block), half),
        in_specs=[held] * 4,
        out_specs=held,
        compiler_params=pltpu.CompilerParams(vmem_limit_bytes=6 * MIB),
        name="finish",
    )(keep(own), keep(arrived), keep(value_weight), keep(out_weight.T)).T


def shards(
    features, tissue, conv_first, bias_first, conv_second, bias_second, key_weight,
    value_weight, latent_queries, out_weight,
):
    rows, cols = lax.axis_size("row"), lax.axis_size("col")
    if rows == cols == 4 and (rows * latent_queries.shape[0]) % 128 == 0:
        return kernel_path(
            features, tissue, conv_first, bias_first, conv_second, bias_second, key_weight,
            value_weight, latent_queries, out_weight,
        )
    marked = jnp.where(tissue[:, :, None] > 0, features, jnp.asarray(FAR, features.dtype))
    marked = with_halo(with_halo(marked, "row", 0), "col", 1)
    normalized = plain_attend(
        features, tissue, marked, latent_queries,
        (conv_first, bias_first, conv_second, bias_second, key_weight),
    )
    attended = lax.dot_general(
        normalized, value_weight, (((0,), (0,)), ((), ())), preferred_element_type=jnp.float32
    ).astype(jnp.bfloat16)
    return jnp.dot(attended, out_weight, preferred_element_type=jnp.float32).astype(jnp.bfloat16)


def solution(mesh):
    placed = (
        P(("groups", "row"), "col", None),
        P(("groups", "row"), "col"),
        P(),
        P(),
        P(),
        P(),
        P(),
        P(),
        P(("col", "row"), None),
        P(None, "col"),
    )
    return jax.shard_map(
        shards, mesh=mesh, in_specs=placed, out_specs=P(("groups", "row"), "col"), check_vma=False
    )
```

```python
import math

import jax
import jax.numpy as jnp
from jax import lax
from jax.experimental import pallas as pl
from jax.experimental.pallas import tpu as pltpu
from jax.sharding import PartitionSpec as P


HALO = 2
FAR = float("inf")
EDGE = 8
LEAD = 16


def shifted(array, axis, step):
    count = lax.axis_size(axis)
    return lax.ppermute(array, axis, [(i, (i + step) % count) for i in range(count)])


def flipped(array, axis, bit):
    count = lax.axis_size(axis)
    return lax.ppermute(array, axis, [(i, i ^ bit) for i in range(count)])


def with_halo(cells, axis, dim):
    size = cells.shape[dim]
    index, last = lax.axis_index(axis), lax.axis_size(axis) - 1
    before = shifted(lax.slice_in_dim(cells, size - HALO, size, axis=dim), axis, 1)
    after = shifted(lax.slice_in_dim(cells, 0, HALO, axis=dim), axis, -1)
    far = jnp.asarray(FAR, cells.dtype)
    return jnp.concatenate(
        [jnp.where(index == 0, far, before), cells, jnp.where(index == last, far, after)], axis=dim
    )


def convolve_valid(padded, weight):
    height, breadth = padded.shape[0] - 2, padded.shape[1] - 2
    channels = padded.shape[2]
    summed = jnp.zeros((height * breadth, weight.shape[3]), jnp.float32)
    for offset_row in range(3):
        for offset_col in range(3):
            window = padded[offset_row : offset_row + height, offset_col : offset_col + breadth]
            summed = summed + jnp.dot(
                window.reshape(height * breadth, channels),
                weight[offset_row, offset_col],
                preferred_element_type=jnp.float32,
            )
    return summed.reshape(height, breadth, weight.shape[3])


def rotated(parts, offset, step):
    count = len(parts)
    size = parts[0].shape[0]
    ordered = [parts[(step * k) % count] for k in range(count)]
    twice = jnp.concatenate(ordered + ordered[:-1], axis=0)
    return lax.dynamic_slice_in_dim(twice, ((count - offset) % count) * size, count * size, axis=0)


def gathered_queries(latent_queries):
    rows, cols = lax.axis_size("row"), lax.axis_size("col")
    parts = [latent_queries] + [shifted(latent_queries, "row", k) for k in range(1, rows)]
    queries = rotated(parts, lax.axis_index("row"), -1)
    own = lax.axis_index("col")
    bit = cols // 2
    groups = [queries]
    order = [0]
    while bit > 0:
        groups = groups + list(flipped(jnp.concatenate(groups, axis=0), "col", bit).reshape(len(groups), -1, queries.shape[1]))
        order = order + [place ^ bit for place in order]
        bit //= 2
    stacked = jnp.stack(groups)
    place = jnp.asarray([order.index(k) for k in range(cols)], jnp.int32)
    return stacked[place[own ^ jnp.arange(cols)]].reshape(-1, queries.shape[1])


def in_parts(values, count):
    parts = []
    for _ in range(count):
        part = lax.reduce_precision(values, exponent_bits=8, mantissa_bits=7)
        parts.append(part.astype(jnp.bfloat16))
        values = values - part
    return parts


def packed(pooled, top, total):
    rest = jnp.zeros((11, pooled.shape[1]), jnp.bfloat16)
    return jnp.concatenate(
        [pooled.astype(jnp.bfloat16)] + in_parts(top, 3) + in_parts(total, 2) + [rest], axis=0
    )


def unpacked(block, channels):
    wide = block.astype(jnp.float32)
    row = lambda k: wide[channels + k : channels + k + 1]
    return wide[:channels], row(0) + row(1) + row(2), row(3) + row(4)


def merged(partials):
    top = partials[0][1]
    for _, other, _ in partials[1:]:
        top = jnp.maximum(top, other)
    pooled = total = 0.0
    for part, shift, count in partials:
        factor = jnp.exp(shift - top)
        pooled = pooled + part * factor
        total = total + count * factor
    return pooled, top, total


def plain_attend(features, tissue, marked, latent_queries, weights):
    conv_first, bias_first, conv_second, bias_second, key_weight = weights
    height, breadth, channels = features.shape
    rows = lax.axis_size("row")
    queries = gathered_queries(latent_queries)
    alive = marked < FAR
    inputs = jnp.where(alive, marked, jnp.zeros_like(marked))
    hidden = jax.nn.gelu(convolve_valid(inputs, conv_first) + bias_first, approximate=False)
    hidden = jnp.where(alive[1:-1, 1:-1], hidden, 0.0).astype(jnp.bfloat16)
    second = jax.nn.gelu(convolve_valid(hidden, conv_second) + bias_second, approximate=False)
    second = jnp.where(alive[HALO:-HALO, HALO:-HALO], second, 0.0).astype(jnp.bfloat16)
    flattened = second.reshape(height * breadth, channels)
    key_rows = jnp.dot(flattened, key_weight, preferred_element_type=jnp.float32).astype(
        jnp.bfloat16
    )
    scale = 1.0 / math.sqrt(latent_queries.shape[1])
    scores = (
        lax.dot_general(
            key_rows, queries, (((1,), (1,)), ((), ())), preferred_element_type=jnp.float32
        )
        * scale
    )
    scores = jnp.where(tissue.reshape(-1, 1) > 0, scores, -1e30)
    shift = jnp.max(scores, axis=0, keepdims=True)
    chosen = jnp.exp(scores - shift)
    total = jnp.sum(chosen, axis=0, keepdims=True)
    pooled = lax.dot_general(
        flattened,
        chosen.astype(jnp.bfloat16),
        (((0,), (0,)), ((), ())),
        preferred_element_type=jnp.float32,
    )

    own_row = lax.axis_index("row")
    size = pooled.shape[1] // rows

    def block_of(step):
        start = ((own_row + step) % rows) * size
        cut = lambda array: lax.dynamic_slice_in_dim(array, start, size, axis=1)
        return cut(pooled), cut(shift), cut(total)

    arrived = [shifted(packed(*block_of(k)), "row", k) for k in range(1, rows)]
    partial = merged([block_of(0)] + [unpacked(block, channels) for block in arrived])
    bit = lax.axis_size("col") // 2
    while bit > 0:
        other = flipped(packed(*partial), "col", bit)
        partial = merged([partial, unpacked(other, channels)])
        bit //= 2
    normalized = (partial[0] / partial[2]).astype(jnp.bfloat16)
    return normalized


def gelu(value):
    return 0.5 * value * (1.0 + lax.erf(value * math.sqrt(0.5)))


def mark_kernel(features, tissue, queries, out, queries_out, features_held, tissue_held, done):
    copies = [
        pltpu.make_async_copy(tissue, tissue_held, done.at[0]),
        pltpu.make_async_copy(features, features_held, done.at[1]),
        pltpu.make_async_copy(queries, queries_out, done.at[2]),
    ]
    for copy in copies:
        copy.start()
    height, breadth, channels = features.shape
    copies[0].wait()
    line = lax.broadcasted_iota(jnp.int32, (breadth, breadth), 0)
    place = lax.broadcasted_iota(jnp.int32, (breadth, breadth), 1)
    flags = tissue_held[...].astype(jnp.float32)
    spread = [
        jnp.where(line == place, jnp.broadcast_to(flags[k : k + 1], line.shape), 0.0)
        for k in range(height)
    ]
    keep = jnp.dot(
        jnp.concatenate(spread, axis=0).astype(jnp.bfloat16),
        jnp.ones((breadth, channels), jnp.bfloat16),
        preferred_element_type=jnp.float32,
    )
    copies[1].wait()
    for k in range(height):
        out[k] = jnp.where(
            keep[k * breadth : (k + 1) * breadth] > 0.0, features_held[k].astype(jnp.float32), FAR
        ).astype(jnp.bfloat16)
    copies[2].wait()


def halve_kernel(own, other, out):
    half = own.shape[0] // 2
    core = lax.rem(lax.axis_index("col"), 2)
    start = pl.multiple_of(core * half, half)
    out[pl.ds(start, half), :] = own[pl.ds(start, half), :]
    out[pl.ds(pl.multiple_of((1 - core) * half, half), half), :] = other[pl.ds(start, half), :]


def conv_kernel(
    marked, top, bottom, paired, crossed, first, bias_first, second, bias_second,
    out, sent, cells, mid, taps, second_held, done,
):
    later = pltpu.make_async_copy(second, second_held, done)
    later.start()
    height, breadth, channels = marked.shape
    slot = (cells.shape[0] - 2 * EDGE - LEAD) // (height + 2 * HALO)
    flat = cells.shape[0] - 2 * EDGE
    row, col = lax.axis_index("row"), lax.axis_index("col")
    first_row, last_row = row == 0, row == lax.axis_size("row") - 1
    first_col, last_col = col == 0, col == lax.axis_size("col") - 1
    even = lax.rem(col, 2) == 0

    def put(line, place, values, outside):
        start = EDGE + LEAD + line * slot + place
        values = values.astype(jnp.float32)
        if outside is not None:
            values = jnp.where(outside, FAR, values)
        cells[start : start + values.shape[0], :] = values

    cells[...] = jnp.full(cells.shape, FAR, jnp.float32)
    for line in range(height):
        put(line + HALO, 0, marked[line], None)
    for line in range(HALO):
        put(line, 0, top[line], first_row)
        put(height + HALO + line, 0, bottom[line], last_row)
    for line in range(height + 2 * HALO):
        beyond_left, beyond_right = first_col, last_col
        if line < HALO:
            beyond_left, beyond_right = first_col | first_row, last_col | first_row
        if line >= height + HALO:
            beyond_left, beyond_right = first_col | last_row, last_col | last_row
        one, two = paired[line].astype(jnp.float32), crossed[line].astype(jnp.float32)
        put(line, -HALO, jnp.where(even, two, one), beyond_left)
        put(line, breadth, jnp.where(even, one, two), beyond_right)

    for shift in range(3):
        values = cells[EDGE - 1 + shift : EDGE - 1 + shift + flat, :]
        taps[:, shift * channels : (shift + 1) * channels] = jnp.where(
            values < FAR, values, 0.0
        ).astype(jnp.bfloat16)

    count = flat - 2 * slot
    summed = jnp.dot(taps[0:count, :], first[0], preferred_element_type=jnp.float32)
    for line in range(1, 3):
        summed = summed + jnp.dot(
            taps[line * slot : line * slot + count, :], first[line],
            preferred_element_type=jnp.float32,
        )
    alive = cells[EDGE + slot : EDGE + slot + count, :] < FAR
    edge = jnp.zeros((EDGE, channels), jnp.float32)
    mid[0:EDGE, :] = edge
    mid[EDGE + count : 2 * EDGE + count, :] = edge
    mid[EDGE : EDGE + count, :] = jnp.where(alive, gelu(summed + bias_first[...]), 0.0)

    for shift in range(3):
        taps[0:count, shift * channels : (shift + 1) * channels] = mid[
            EDGE - 1 + shift : EDGE - 1 + shift + count, :
        ].astype(jnp.bfloat16)
    inner = height * slot
    later.wait()
    summed = jnp.dot(
        taps[LEAD : LEAD + inner, :], second_held[0], preferred_element_type=jnp.float32
    )
    for line in range(1, 3):
        summed = summed + jnp.dot(
            taps[LEAD + line * slot : LEAD + line * slot + inner, :], second_held[line],
            preferred_element_type=jnp.float32,
        )
    summed = summed.reshape(height, slot, channels)[:, :breadth].reshape(height * breadth, channels)
    alive = marked[...].reshape(height * breadth, channels) < FAR
    value = gelu(summed + bias_second[...])
    out[...] = jnp.where(alive, value, 0.0).astype(jnp.bfloat16)
    sent[...] = jnp.where(alive, value, FAR).astype(jnp.bfloat16)


def key_kernel(cells, weight, keys):
    keys[...] = jnp.dot(cells[...], weight[...], preferred_element_type=jnp.float32).astype(
        jnp.bfloat16
    )


def write_parts(block, values, top, total):
    channels = values.shape[0]
    parts = []
    for source, count in ((top, 3), (total, 2)):
        rest = source
        for _ in range(count):
            part = rest.astype(jnp.bfloat16).astype(jnp.float32)
            parts.append(part)
            rest = rest - part
    parts.append(jnp.zeros((block.shape[0] - channels - 5, values.shape[1]), jnp.float32))
    block[0:channels, :] = values.astype(jnp.bfloat16)
    block[channels:, :] = jnp.concatenate(parts, axis=0).astype(jnp.bfloat16)


def read_parts(block):
    channels = block.shape[0] - 16
    tail = block[channels:, :].astype(jnp.float32)
    row = lambda k: tail[k : k + 1]
    return (
        block[0:channels, :].astype(jnp.float32),
        row(0) + row(1) + row(2),
        row(3) + row(4),
    )


def read_whole(block):
    channels = block.shape[0] - 8
    tail = block[channels:, :]
    return block[0:channels, :], tail[0:1], tail[1:2]


def write_whole(block, values, top, total):
    channels = values.shape[0]
    block[0:channels, :] = values
    block[channels:, :] = jnp.concatenate(
        [top, total, jnp.zeros((6, values.shape[1]), jnp.float32)], axis=0
    )


def score_blocks(held, queries, sides):
    half = queries.shape[0] // 8
    row = lax.axis_index("row")
    for place in range(4):
        for parity in range(2):
            source = (2 * place + parity) * half
            target = pl.multiple_of(parity * 4 * half + (row ^ place) * half, half)
            held[pl.ds(target, half), :] = queries[source : source + half, :]
    scale = 1.0 / math.sqrt(held.shape[1])
    scores = []
    for _, marked, keys in sides:
        raw = lax.dot_general(
            keys[...], held[...], (((1,), (1,)), ((), ())), preferred_element_type=jnp.float32
        )
        alive = marked[:, : raw.shape[1]] < FAR
        scores.append(jnp.where(alive, raw * scale, -1e30))
    top = jnp.maximum(*[jnp.max(part, axis=0, keepdims=True) for part in scores])
    pooled = total = 0.0
    for part, (cells, _, _) in zip(scores, sides):
        chosen = jnp.exp(part - top)
        total = total + jnp.sum(chosen, axis=0, keepdims=True)
        pooled = pooled + lax.dot_general(
            cells[...], chosen.astype(jnp.bfloat16), (((0,), (0,)), ((), ())),
            preferred_element_type=jnp.float32,
        )
    channels, lanes = pooled.shape[0] // 2, pooled.shape[1]
    turn = lambda array: pltpu.roll(array, lanes // 2, 1)
    lower = lambda rows: lax.broadcasted_iota(jnp.int32, (rows, lanes), 1) < lanes // 2
    tall, flat = lower(channels), lower(1)
    turned, turned_top, turned_total = turn(pooled), turn(top), turn(total)
    return (
        (
            jnp.where(tall, pooled[:channels], turned[channels:]),
            jnp.where(flat, top, turned_top),
            jnp.where(flat, total, turned_total),
        ),
        (
            jnp.where(tall, turned[:channels], pooled[channels:]),
            jnp.where(flat, turned_top, top),
            jnp.where(flat, turned_total, total),
        ),
    )


def near_kernel(own, own_sent, own_keys, other_sent, weight, queries, out, other, keys, held):
    values = other_sent[...].astype(jnp.float32)
    other[...] = jnp.where(values < FAR, values, 0.0).astype(jnp.bfloat16)
    key_kernel(other, weight, keys)
    sides = ((own, own_sent, own_keys), (other, other_sent, keys))
    for parity, block in enumerate(score_blocks(held, queries, sides)):
        write_whole(out.at[parity], *block)


def far_kernel(
    near, own, own_sent, own_keys, other, other_sent, other_keys, queries,
    kept, send_1, send_2, send_3, held, blocks,
):
    row, across = lax.axis_index("row"), lax.axis_index("col") // 2
    sides = ((own, own_sent, own_keys), (other, other_sent, other_keys))
    for parity in range(2):
        blocks[2 * across + parity] = near[parity]
    for parity, block in enumerate(score_blocks(held, queries, sides)):
        write_whole(blocks.at[2 * (1 - across) + parity], *block)
    kept[...] = blocks[row]
    for step, send in ((1, send_1), (2, send_2), (3, send_3)):
        write_parts(send, *read_whole(blocks.at[row ^ step]))


def merge_kernel(own, *refs):
    *arrived, whole, packed_out = refs
    values, top, total = merged([read_whole(own)] + [read_parts(block) for block in arrived])
    write_whole(whole, values, top, total)
    write_parts(packed_out, values, top, total)


def normalize_kernel(own, arrived, out):
    values, _, total = merged([read_whole(own), read_parts(arrived)])
    out[...] = (values / total).astype(jnp.bfloat16)


def finish_kernel(own, arrived, value_weight, out_weight, out, attended):
    lanes = own.shape[1]
    half = lanes // 2
    first_core = lax.rem(lax.axis_index("col"), 2) == 0
    mine, other = own[...].astype(jnp.float32), arrived[...].astype(jnp.float32)
    even, odd = jnp.where(first_core, mine, other), jnp.where(first_core, other, mine)
    lower = lax.broadcasted_iota(jnp.int32, mine.shape, 1) < half
    normalized = jnp.concatenate(
        [
            jnp.where(lower, even, pltpu.roll(odd, half, 1)),
            jnp.where(lower, pltpu.roll(even, half, 1), odd),
        ],
        axis=0,
    ).astype(jnp.bfloat16)
    product = lax.dot_general(
        normalized, value_weight[...], (((0,), (0,)), ((), ())),
        preferred_element_type=jnp.float32,
    ).astype(jnp.bfloat16)
    piece = half // 4
    for core in range(2):
        for place in range(4):
            source, target = core * half + place * piece, (2 * place + core) * piece
            attended[target : target + piece, :] = product[source : source + piece]
    out[...] = lax.dot_general(
        out_weight[...], attended[...], (((1,), (1,)), ((), ())),
        preferred_element_type=jnp.float32,
    ).astype(out.dtype)


MIB = 1 << 20


def call(kernel, outs, args, scratch=(), limit=4, flops=0, far=()):
    held = pl.BlockSpec(memory_space=pltpu.VMEM)
    outside = pl.BlockSpec(memory_space=pltpu.HBM)
    return pl.pallas_call(
        kernel,
        out_shape=[pltpu.VMEM(shape, dtype) for shape, dtype in outs],
        in_specs=[outside if k in far else held for k in range(len(args))],
        out_specs=[held] * len(outs),
        scratch_shapes=[
            pltpu.VMEM(*kind) if isinstance(kind, tuple) else kind for kind in scratch
        ],
        compiler_params=pltpu.CompilerParams(vmem_limit_bytes=limit * MIB),
        cost_estimate=pl.CostEstimate(flops=flops, bytes_accessed=0, transcendentals=0),
    )(
        *[
            pltpu.with_memory_space_constraint(arg, pltpu.HBM if k in far else pltpu.VMEM)
            for k, arg in enumerate(args)
        ]
    )


def kernel_path(
    features, tissue, conv_first, bias_first, conv_second, bias_second, key_weight,
    value_weight, latent_queries, out_weight,
):
    height, breadth, channels = features.shape
    col, cols = lax.axis_index("col"), lax.axis_size("col")
    size, width = latent_queries.shape
    cells = height * breadth
    slot = -(-(breadth + 2 * HALO) // 16) * 16
    flat = LEAD + (height + 2 * HALO) * slot
    wide, half = jnp.float32, jnp.bfloat16
    block = 4 * size
    whole_block, sent_block = (channels // 2 + 8, block), (channels // 2 + 16, block)
    score_flops = 4 * cells * block * (width + channels)

    beside = flipped(latent_queries, "col", 1)
    marked, queries = call(
        mark_kernel, [(features.shape, half), ((size, width), half)],
        [features, tissue, latent_queries],
        [(features.shape, half), (tissue.shape, jnp.int32), pltpu.SemaphoreType.DMA((3,))],
        far=(0, 1, 2), flops=1 << 20,
    )
    (queries,) = call(halve_kernel, [((size, width), half)], [queries, beside])
    turned = [flipped(queries, "row", k) for k in range(1, 4)]
    top = shifted(marked[height - HALO :], "row", 1)
    bottom = shifted(marked[:HALO], "row", -1)
    edge = lambda cut: jnp.concatenate([top[:, cut], marked[:, cut], bottom[:, cut]], axis=0)
    even = lax.rem(col, 2) == 0
    ends = edge(slice(breadth - HALO, breadth)), edge(slice(0, HALO))
    paired = flipped(jnp.where(even, *ends), "col", 1)
    rounds = [(k, (k + 1 if k % 2 else k - 1) % cols) for k in range(cols)]
    crossed = lax.ppermute(jnp.where(even, *ends[::-1]), "col", rounds)

    near_queries = jnp.concatenate([queries] + turned, axis=0)
    far_queries = flipped(near_queries, "col", 2)

    own, own_sent = call(
        conv_kernel, [((cells, channels), half)] * 2,
        [
            marked, top, bottom, paired, crossed,
            conv_first.reshape(3, 3 * channels, channels), bias_first.reshape(1, channels),
            conv_second.reshape(3, 3 * channels, channels), bias_second.reshape(1, channels),
        ],
        [
            ((flat + 2 * EDGE, channels), wide),
            ((flat - 2 * slot + 2 * EDGE, channels), wide),
            ((flat, 3 * channels), half),
            ((3, 3 * channels, channels), half),
            pltpu.SemaphoreType.DMA,
        ],
        limit=16, far=(7,), flops=42 * cells * channels * channels,
    )
    other_sent = flipped(own_sent, "col", 1)
    (own_keys,) = call(
        key_kernel, [((cells, width), half)], [own, key_weight],
        limit=6, flops=2 * cells * channels * width,
    )
    near, other, other_keys = call(
        near_kernel,
        [((2,) + whole_block, wide), ((cells, channels), half), ((cells, width), half)],
        [own, own_sent, own_keys, other_sent, key_weight, near_queries],
        [((block, width), half)],
        limit=8, flops=score_flops + 2 * cells * channels * width,
    )
    kept, *sends = call(
        far_kernel, [(whole_block, wide)] + [(sent_block, half)] * 3,
        [near, own, own_sent, own_keys, other, other_sent, other_keys, far_queries],
        [((block, width), half), ((4,) + whole_block, wide)],
        limit=8, flops=score_flops,
    )
    arrived = [flipped(part, "row", k + 1) for k, part in enumerate(sends)]
    kept, sent = call(merge_kernel, [(whole_block, wide), (sent_block, half)], [kept, *arrived])
    arrived = flipped(sent, "col", 2)
    (normalized,) = call(normalize_kernel, [((channels // 2, block), half)], [kept, arrived])
    arrived = flipped(normalized, "col", 1)
    held = pl.BlockSpec(memory_space=pltpu.VMEM)
    keep = lambda array: pltpu.with_memory_space_constraint(array, pltpu.VMEM)
    return pl.pallas_call(
        finish_kernel,
        out_shape=jax.ShapeDtypeStruct((out_weight.shape[1], block), half),
        in_specs=[held] * 4,
        out_specs=held,
        scratch_shapes=[pltpu.VMEM((block, width), half)],
        compiler_params=pltpu.CompilerParams(vmem_limit_bytes=6 * MIB),
        name="finish",
    )(keep(normalized), keep(arrived), keep(value_weight), keep(out_weight.T)).T


def shards(
    features, tissue, conv_first, bias_first, conv_second, bias_second, key_weight,
    value_weight, latent_queries, out_weight,
):
    rows, cols = lax.axis_size("row"), lax.axis_size("col")
    if rows == cols == 4 and rows * latent_queries.shape[0] == 128:
        return kernel_path(
            features, tissue, conv_first, bias_first, conv_second, bias_second, key_weight,
            value_weight, latent_queries, out_weight,
        )
    marked = jnp.where(tissue[:, :, None] > 0, features, jnp.asarray(FAR, features.dtype))
    marked = with_halo(with_halo(marked, "row", 0), "col", 1)
    normalized = plain_attend(
        features, tissue, marked, latent_queries,
        (conv_first, bias_first, conv_second, bias_second, key_weight),
    )
    attended = lax.dot_general(
        normalized, value_weight, (((0,), (0,)), ((), ())), preferred_element_type=jnp.float32
    ).astype(jnp.bfloat16)
    return jnp.dot(attended, out_weight, preferred_element_type=jnp.float32).astype(jnp.bfloat16)


def solution(mesh):
    placed = (
        P(("groups", "row"), "col", None),
        P(("groups", "row"), "col"),
        P(),
        P(),
        P(),
        P(),
        P(),
        P(),
        P(("col", "row"), None),
        P(None, "col"),
    )
    return jax.shard_map(
        shards, mesh=mesh, in_specs=placed, out_specs=P(("groups", "row"), "col"), check_vma=False
    )
```

```python
import math

import jax
import jax.numpy as jnp
from jax import lax
from jax.experimental import pallas as pl
from jax.experimental.pallas import tpu as pltpu
from jax.sharding import PartitionSpec as P


HALO = 2
FAR = float("inf")
EDGE = 8
LEAD = 16


def shifted(array, axis, step):
    count = lax.axis_size(axis)
    return lax.ppermute(array, axis, [(i, (i + step) % count) for i in range(count)])


def flipped(array, axis, bit):
    count = lax.axis_size(axis)
    return lax.ppermute(array, axis, [(i, i ^ bit) for i in range(count)])


def with_halo(cells, axis, dim):
    size = cells.shape[dim]
    index, last = lax.axis_index(axis), lax.axis_size(axis) - 1
    before = shifted(lax.slice_in_dim(cells, size - HALO, size, axis=dim), axis, 1)
    after = shifted(lax.slice_in_dim(cells, 0, HALO, axis=dim), axis, -1)
    far = jnp.asarray(FAR, cells.dtype)
    return jnp.concatenate(
        [jnp.where(index == 0, far, before), cells, jnp.where(index == last, far, after)], axis=dim
    )


def convolve_valid(padded, weight):
    height, breadth = padded.shape[0] - 2, padded.shape[1] - 2
    channels = padded.shape[2]
    summed = jnp.zeros((height * breadth, weight.shape[3]), jnp.float32)
    for offset_row in range(3):
        for offset_col in range(3):
            window = padded[offset_row : offset_row + height, offset_col : offset_col + breadth]
            summed = summed + jnp.dot(
                window.reshape(height * breadth, channels),
                weight[offset_row, offset_col],
                preferred_element_type=jnp.float32,
            )
    return summed.reshape(height, breadth, weight.shape[3])


def rotated(parts, offset, step):
    count = len(parts)
    size = parts[0].shape[0]
    ordered = [parts[(step * k) % count] for k in range(count)]
    twice = jnp.concatenate(ordered + ordered[:-1], axis=0)
    return lax.dynamic_slice_in_dim(twice, ((count - offset) % count) * size, count * size, axis=0)


def gathered_queries(latent_queries):
    rows, cols = lax.axis_size("row"), lax.axis_size("col")
    parts = [latent_queries] + [shifted(latent_queries, "row", k) for k in range(1, rows)]
    queries = rotated(parts, lax.axis_index("row"), -1)
    own = lax.axis_index("col")
    bit = cols // 2
    groups = [queries]
    order = [0]
    while bit > 0:
        groups = groups + list(flipped(jnp.concatenate(groups, axis=0), "col", bit).reshape(len(groups), -1, queries.shape[1]))
        order = order + [place ^ bit for place in order]
        bit //= 2
    stacked = jnp.stack(groups)
    place = jnp.asarray([order.index(k) for k in range(cols)], jnp.int32)
    return stacked[place[own ^ jnp.arange(cols)]].reshape(-1, queries.shape[1])


def in_parts(values, count):
    parts = []
    for _ in range(count):
        part = lax.reduce_precision(values, exponent_bits=8, mantissa_bits=7)
        parts.append(part.astype(jnp.bfloat16))
        values = values - part
    return parts


def packed(pooled, top, total):
    rest = jnp.zeros((11, pooled.shape[1]), jnp.bfloat16)
    return jnp.concatenate(
        [pooled.astype(jnp.bfloat16)] + in_parts(top, 3) + in_parts(total, 2) + [rest], axis=0
    )


def unpacked(block, channels):
    wide = block.astype(jnp.float32)
    row = lambda k: wide[channels + k : channels + k + 1]
    return wide[:channels], row(0) + row(1) + row(2), row(3) + row(4)


def merged(partials):
    top = partials[0][1]
    for _, other, _ in partials[1:]:
        top = jnp.maximum(top, other)
    pooled = total = 0.0
    for part, shift, count in partials:
        factor = jnp.exp(shift - top)
        pooled = pooled + part * factor
        total = total + count * factor
    return pooled, top, total


def plain_attend(features, tissue, marked, latent_queries, weights):
    conv_first, bias_first, conv_second, bias_second, key_weight = weights
    height, breadth, channels = features.shape
    rows = lax.axis_size("row")
    queries = gathered_queries(latent_queries)
    alive = marked < FAR
    inputs = jnp.where(alive, marked, jnp.zeros_like(marked))
    hidden = jax.nn.gelu(convolve_valid(inputs, conv_first) + bias_first, approximate=False)
    hidden = jnp.where(alive[1:-1, 1:-1], hidden, 0.0).astype(jnp.bfloat16)
    second = jax.nn.gelu(convolve_valid(hidden, conv_second) + bias_second, approximate=False)
    second = jnp.where(alive[HALO:-HALO, HALO:-HALO], second, 0.0).astype(jnp.bfloat16)
    flattened = second.reshape(height * breadth, channels)
    key_rows = jnp.dot(flattened, key_weight, preferred_element_type=jnp.float32).astype(
        jnp.bfloat16
    )
    scale = 1.0 / math.sqrt(latent_queries.shape[1])
    scores = (
        lax.dot_general(
            key_rows, queries, (((1,), (1,)), ((), ())), preferred_element_type=jnp.float32
        )
        * scale
    )
    scores = jnp.where(tissue.reshape(-1, 1) > 0, scores, -1e30)
    shift = jnp.max(scores, axis=0, keepdims=True)
    chosen = jnp.exp(scores - shift)
    total = jnp.sum(chosen, axis=0, keepdims=True)
    pooled = lax.dot_general(
        flattened,
        chosen.astype(jnp.bfloat16),
        (((0,), (0,)), ((), ())),
        preferred_element_type=jnp.float32,
    )

    own_row = lax.axis_index("row")
    size = pooled.shape[1] // rows

    def block_of(step):
        start = ((own_row + step) % rows) * size
        cut = lambda array: lax.dynamic_slice_in_dim(array, start, size, axis=1)
        return cut(pooled), cut(shift), cut(total)

    arrived = [shifted(packed(*block_of(k)), "row", k) for k in range(1, rows)]
    partial = merged([block_of(0)] + [unpacked(block, channels) for block in arrived])
    bit = lax.axis_size("col") // 2
    while bit > 0:
        other = flipped(packed(*partial), "col", bit)
        partial = merged([partial, unpacked(other, channels)])
        bit //= 2
    normalized = (partial[0] / partial[2]).astype(jnp.bfloat16)
    return normalized


def gelu(value):
    return 0.5 * value * (1.0 + lax.erf(value * math.sqrt(0.5)))


def mark_kernel(features, tissue, queries, out, queries_out, features_held, tissue_held, done):
    copies = [
        pltpu.make_async_copy(tissue, tissue_held, done.at[0]),
        pltpu.make_async_copy(features, features_held, done.at[1]),
        pltpu.make_async_copy(queries, queries_out, done.at[2]),
    ]
    for copy in copies:
        copy.start()
    height, breadth, channels = features.shape
    copies[0].wait()
    line = lax.broadcasted_iota(jnp.int32, (breadth, breadth), 0)
    place = lax.broadcasted_iota(jnp.int32, (breadth, breadth), 1)
    flags = tissue_held[...].astype(jnp.float32)
    spread = [
        jnp.where(line == place, jnp.broadcast_to(flags[k : k + 1], line.shape), 0.0)
        for k in range(height)
    ]
    keep = jnp.dot(
        jnp.concatenate(spread, axis=0).astype(jnp.bfloat16),
        jnp.ones((breadth, channels), jnp.bfloat16),
        preferred_element_type=jnp.float32,
    )
    copies[1].wait()
    for k in range(height):
        out[k] = jnp.where(
            keep[k * breadth : (k + 1) * breadth] > 0.0, features_held[k].astype(jnp.float32), FAR
        ).astype(jnp.bfloat16)
    copies[2].wait()


def halve_kernel(own, other, out):
    half = own.shape[0] // 2
    core = lax.rem(lax.axis_index("col"), 2)
    start = pl.multiple_of(core * half, half)
    out[pl.ds(start, half), :] = own[pl.ds(start, half), :]
    out[pl.ds(pl.multiple_of((1 - core) * half, half), half), :] = other[pl.ds(start, half), :]


def conv_kernel(
    marked, top, bottom, paired, crossed, first, bias_first, second,
    mid, second_held, cells, taps, done,
):
    later = pltpu.make_async_copy(second, second_held, done)
    later.start()
    height, breadth, channels = marked.shape
    slot = (cells.shape[0] - 2 * EDGE - LEAD) // (height + 2 * HALO)
    flat = cells.shape[0] - 2 * EDGE
    row, col = lax.axis_index("row"), lax.axis_index("col")
    first_row, last_row = row == 0, row == lax.axis_size("row") - 1
    first_col, last_col = col == 0, col == lax.axis_size("col") - 1
    even = lax.rem(col, 2) == 0

    def put(line, place, values, outside):
        start = EDGE + LEAD + line * slot + place
        values = values.astype(jnp.float32)
        if outside is not None:
            values = jnp.where(outside, FAR, values)
        cells[start : start + values.shape[0], :] = values

    cells[...] = jnp.full(cells.shape, FAR, jnp.float32)
    for line in range(height):
        put(line + HALO, 0, marked[line], None)
    for line in range(HALO):
        put(line, 0, top[line], first_row)
        put(height + HALO + line, 0, bottom[line], last_row)
    for line in range(height + 2 * HALO):
        beyond_left, beyond_right = first_col, last_col
        if line < HALO:
            beyond_left, beyond_right = first_col | first_row, last_col | first_row
        if line >= height + HALO:
            beyond_left, beyond_right = first_col | last_row, last_col | last_row
        one, two = paired[line].astype(jnp.float32), crossed[line].astype(jnp.float32)
        put(line, -HALO, jnp.where(even, two, one), beyond_left)
        put(line, breadth, jnp.where(even, one, two), beyond_right)

    for shift in range(3):
        values = cells[EDGE - 1 + shift : EDGE - 1 + shift + flat, :]
        taps[:, shift * channels : (shift + 1) * channels] = jnp.where(
            values < FAR, values, 0.0
        ).astype(jnp.bfloat16)

    count = flat - 2 * slot
    summed = jnp.dot(taps[0:count, :], first[0], preferred_element_type=jnp.float32)
    for line in range(1, 3):
        summed = summed + jnp.dot(
            taps[line * slot : line * slot + count, :], first[line],
            preferred_element_type=jnp.float32,
        )
    alive = cells[EDGE + slot : EDGE + slot + count, :] < FAR
    edge = jnp.zeros((EDGE, channels), jnp.float32)
    mid[0:EDGE, :] = edge
    mid[EDGE + count : 2 * EDGE + count, :] = edge
    mid[EDGE : EDGE + count, :] = jnp.where(alive, gelu(summed + bias_first[...]), 0.0)
    later.wait()


def second_conv_kernel(marked, mid, second, bias_second, out, sent, taps):
    height, breadth, channels = marked.shape
    count = mid.shape[0] - 2 * EDGE
    slot = (count - LEAD) // (height + 2)
    for shift in range(3):
        taps[0:count, shift * channels : (shift + 1) * channels] = mid[
            EDGE - 1 + shift : EDGE - 1 + shift + count, :
        ].astype(jnp.bfloat16)
    inner = height * slot
    summed = jnp.dot(taps[LEAD : LEAD + inner, :], second[0], preferred_element_type=jnp.float32)
    for line in range(1, 3):
        summed = summed + jnp.dot(
            taps[LEAD + line * slot : LEAD + line * slot + inner, :], second[line],
            preferred_element_type=jnp.float32,
        )
    summed = summed.reshape(height, slot, channels)[:, :breadth].reshape(height * breadth, channels)
    alive = marked[...].reshape(height * breadth, channels) < FAR
    value = gelu(summed + bias_second[...])
    out[...] = jnp.where(alive, value, 0.0).astype(jnp.bfloat16)
    sent[...] = jnp.where(alive, value, FAR).astype(jnp.bfloat16)


def key_kernel(cells, weight, keys):
    keys[...] = jnp.dot(cells[...], weight[...], preferred_element_type=jnp.float32).astype(
        jnp.bfloat16
    )


def write_parts(block, values, top, total):
    channels = values.shape[0]
    parts = []
    for source, count in ((top, 3), (total, 2)):
        rest = source
        for _ in range(count):
            part = rest.astype(jnp.bfloat16).astype(jnp.float32)
            parts.append(part)
            rest = rest - part
    parts.append(jnp.zeros((block.shape[0] - channels - 5, values.shape[1]), jnp.float32))
    block[0:channels, :] = values.astype(jnp.bfloat16)
    block[channels:, :] = jnp.concatenate(parts, axis=0).astype(jnp.bfloat16)


def read_parts(block):
    channels = block.shape[0] - 16
    tail = block[channels:, :].astype(jnp.float32)
    row = lambda k: tail[k : k + 1]
    return (
        block[0:channels, :].astype(jnp.float32),
        row(0) + row(1) + row(2),
        row(3) + row(4),
    )


def read_whole(block):
    channels = block.shape[0] - 8
    tail = block[channels:, :]
    return block[0:channels, :], tail[0:1], tail[1:2]


def write_whole(block, values, top, total):
    channels = values.shape[0]
    block[0:channels, :] = values
    block[channels:, :] = jnp.concatenate(
        [top, total, jnp.zeros((6, values.shape[1]), jnp.float32)], axis=0
    )


PLACES = (0, 2, 1, 3)


def hold_queries(held, parts):
    half = held.shape[0] // 8
    row = lax.axis_index("row")
    for number, place in enumerate(PLACES):
        part = parts[number // 2]
        for parity in range(2):
            source = (2 * (number % 2) + parity) * half
            target = pl.multiple_of(parity * 4 * half + (row ^ place) * half, half)
            held[pl.ds(target, half), :] = part[source : source + half, :]


def masked_scores(queries, marked, keys):
    scale = 1.0 / math.sqrt(queries.shape[1])
    raw = lax.dot_general(
        keys[...], queries[...], (((1,), (1,)), ((), ())), preferred_element_type=jnp.float32
    )
    return jnp.where(marked[:, : raw.shape[1]] < FAR, raw * scale, -1e30)


def score_blocks(scores, sides):
    top = jnp.maximum(*[jnp.max(part, axis=0, keepdims=True) for part in scores])
    pooled = total = 0.0
    for part, cells in zip(scores, sides):
        chosen = jnp.exp(part - top)
        total = total + jnp.sum(chosen, axis=0, keepdims=True)
        pooled = pooled + lax.dot_general(
            cells[...], chosen.astype(jnp.bfloat16), (((0,), (0,)), ((), ())),
            preferred_element_type=jnp.float32,
        )
    channels, lanes = pooled.shape[0] // 2, pooled.shape[1]
    turn = lambda array: pltpu.roll(array, lanes // 2, 1)
    lower = lambda rows: lax.broadcasted_iota(jnp.int32, (rows, lanes), 1) < lanes // 2
    tall, flat = lower(channels), lower(1)
    turned, turned_top, turned_total = turn(pooled), turn(top), turn(total)
    return (
        (
            jnp.where(tall, pooled[:channels], turned[channels:]),
            jnp.where(flat, top, turned_top),
            jnp.where(flat, total, turned_total),
        ),
        (
            jnp.where(tall, turned[:channels], pooled[channels:]),
            jnp.where(flat, turned_top, top),
            jnp.where(flat, turned_total, total),
        ),
    )


def own_kernel(own, own_sent, weight, first_queries, last_queries, keys, scores, held):
    key_kernel(own, weight, keys)
    hold_queries(held, (first_queries, last_queries))
    scores[...] = masked_scores(held, own_sent, keys)


def near_kernel(own, own_scores, other_sent, weight, held, out, other, keys):
    values = other_sent[...].astype(jnp.float32)
    other[...] = jnp.where(values < FAR, values, 0.0).astype(jnp.bfloat16)
    key_kernel(other, weight, keys)
    scores = (own_scores[...], masked_scores(held, other_sent, keys))
    for parity, block in enumerate(score_blocks(scores, (own, other))):
        write_whole(out.at[parity], *block)


def far_kernel(
    near, own, own_sent, own_keys, other, other_sent, other_keys, first_queries, last_queries,
    kept, send_1, send_2, send_3, held, blocks,
):
    row, across = lax.axis_index("row"), lax.axis_index("col") // 2
    for parity in range(2):
        blocks[2 * across + parity] = near[parity]
    hold_queries(held, (first_queries, last_queries))
    scores = (
        masked_scores(held, own_sent, own_keys), masked_scores(held, other_sent, other_keys)
    )
    for parity, block in enumerate(score_blocks(scores, (own, other))):
        write_whole(blocks.at[2 * (1 - across) + parity], *block)
    kept[...] = blocks[row]
    for step, send in ((1, send_1), (2, send_2), (3, send_3)):
        write_parts(send, *read_whole(blocks.at[row ^ step]))


def merge_kernel(own, *refs):
    *arrived, whole, packed_out = refs
    values, top, total = merged([read_whole(own)] + [read_parts(block) for block in arrived])
    write_whole(whole, values, top, total)
    write_parts(packed_out, values, top, total)


def normalize_kernel(own, arrived, out):
    values, _, total = merged([read_whole(own), read_parts(arrived)])
    out[...] = (values / total).astype(jnp.bfloat16)


def attend_kernel(normalized, value_weight, attended):
    lanes = normalized.shape[1] // 2
    values = normalized[...].astype(jnp.float32)
    tall = jnp.concatenate([values, pltpu.roll(values, lanes, 1)], axis=0).astype(jnp.bfloat16)
    attended[...] = lax.dot_general(
        tall, value_weight[...], (((0,), (0,)), ((), ())), preferred_element_type=jnp.float32
    )[:lanes].astype(jnp.bfloat16)


def finish_kernel(mine, arrived, value_weight, out_weight, out, other, attended):
    attend_kernel(arrived, value_weight, other)
    core = lax.rem(lax.axis_index("col"), 2)
    piece = mine.shape[0] // 4
    for place in range(4):
        source = slice(place * piece, (place + 1) * piece)
        first = pl.multiple_of((2 * place + core) * piece, piece)
        last = pl.multiple_of((2 * place + 1 - core) * piece, piece)
        attended[pl.ds(first, piece), :] = mine[source]
        attended[pl.ds(last, piece), :] = other[source]
    out[...] = lax.dot_general(
        out_weight[...], attended[...], (((1,), (1,)), ((), ())),
        preferred_element_type=jnp.float32,
    ).astype(out.dtype)


MIB = 1 << 20


def call(kernel, outs, args, scratch=(), limit=4, flops=0, far=()):
    held = pl.BlockSpec(memory_space=pltpu.VMEM)
    outside = pl.BlockSpec(memory_space=pltpu.HBM)
    return pl.pallas_call(
        kernel,
        out_shape=[pltpu.VMEM(shape, dtype) for shape, dtype in outs],
        in_specs=[outside if k in far else held for k in range(len(args))],
        out_specs=[held] * len(outs),
        scratch_shapes=[
            pltpu.VMEM(*kind) if isinstance(kind, tuple) else kind for kind in scratch
        ],
        compiler_params=pltpu.CompilerParams(vmem_limit_bytes=limit * MIB),
        cost_estimate=pl.CostEstimate(flops=flops, bytes_accessed=0, transcendentals=0),
    )(
        *[
            pltpu.with_memory_space_constraint(arg, pltpu.HBM if k in far else pltpu.VMEM)
            for k, arg in enumerate(args)
        ]
    )


def kernel_path(
    features, tissue, conv_first, bias_first, conv_second, bias_second, key_weight,
    value_weight, latent_queries, out_weight,
):
    height, breadth, channels = features.shape
    col, cols = lax.axis_index("col"), lax.axis_size("col")
    size, width = latent_queries.shape
    cells = height * breadth
    slot = -(-(breadth + 2 * HALO) // 16) * 16
    flat = LEAD + (height + 2 * HALO) * slot
    wide, half = jnp.float32, jnp.bfloat16
    block = 4 * size
    whole_block, sent_block = (channels // 2 + 8, block), (channels // 2 + 16, block)
    score_flops = 4 * cells * block * (width + channels)

    beside = flipped(latent_queries, "col", 1)
    marked, queries = call(
        mark_kernel, [(features.shape, half), ((size, width), half)],
        [features, tissue, latent_queries],
        [(features.shape, half), (tissue.shape, jnp.int32), pltpu.SemaphoreType.DMA((3,))],
        far=(0, 1, 2), flops=1 << 20,
    )
    (queries,) = call(halve_kernel, [((size, width), half)], [queries, beside])
    two = flipped(queries, "row", 2)
    top = shifted(marked[height - HALO :], "row", 1)
    bottom = shifted(marked[:HALO], "row", -1)
    edge = lambda cut: jnp.concatenate([top[:, cut], marked[:, cut], bottom[:, cut]], axis=0)
    even = lax.rem(col, 2) == 0
    ends = edge(slice(breadth - HALO, breadth)), edge(slice(0, HALO))
    paired = flipped(jnp.where(even, *ends), "col", 1)
    rounds = [(k, (k + 1 if k % 2 else k - 1) % cols) for k in range(cols)]
    crossed = lax.ppermute(jnp.where(even, *ends[::-1]), "col", rounds)

    pair = jnp.concatenate([queries, two], axis=0)
    far_pair = flipped(pair, "col", 2)
    next_pair = flipped(pair, "row", 1)
    last_pair = flipped(next_pair, "col", 2)

    count = flat - 2 * slot
    mid, weight = call(
        conv_kernel,
        [((count + 2 * EDGE, channels), wide), ((3, 3 * channels, channels), half)],
        [
            marked, top, bottom, paired, crossed,
            conv_first.reshape(3, 3 * channels, channels), bias_first.reshape(1, channels),
            conv_second.reshape(3, 3 * channels, channels),
        ],
        [
            ((flat + 2 * EDGE, channels), wide),
            ((flat, 3 * channels), half),
            pltpu.SemaphoreType.DMA,
        ],
        limit=12, far=(7,), flops=21 * cells * channels * channels,
    )
    own, own_sent = call(
        second_conv_kernel, [((cells, channels), half)] * 2,
        [marked, mid, weight, bias_second.reshape(1, channels)],
        [((count, 3 * channels), half)],
        limit=10, flops=18 * cells * channels * channels,
    )
    other_sent = flipped(own_sent, "col", 1)
    own_keys, own_scores, held_queries = call(
        own_kernel,
        [((cells, width), half), ((cells, block), wide), ((block, width), half)],
        [own, own_sent, key_weight, pair, next_pair],
        limit=6, flops=2 * cells * width * (channels + block),
    )
    near, other, other_keys = call(
        near_kernel,
        [((2,) + whole_block, wide), ((cells, channels), half), ((cells, width), half)],
        [own, own_scores, other_sent, key_weight, held_queries],
        limit=8, flops=score_flops,
    )
    kept, *sends = call(
        far_kernel, [(whole_block, wide)] + [(sent_block, half)] * 3,
        [
            near, own, own_sent, own_keys, other, other_sent, other_keys,
            far_pair, last_pair,
        ],
        [((block, width), half), ((4,) + whole_block, wide)],
        limit=8, flops=score_flops,
    )
    arrived = [flipped(part, "row", k + 1) for k, part in enumerate(sends)]
    kept, sent = call(merge_kernel, [(whole_block, wide), (sent_block, half)], [kept, *arrived])
    arrived = flipped(sent, "col", 2)
    (normalized,) = call(normalize_kernel, [((channels // 2, block), half)], [kept, arrived])
    arrived = flipped(normalized, "col", 1)
    (attended,) = call(
        attend_kernel, [((2 * size, width), half)], [normalized, value_weight],
        flops=8 * size * channels * width,
    )
    held = pl.BlockSpec(memory_space=pltpu.VMEM)
    keep = lambda array: pltpu.with_memory_space_constraint(array, pltpu.VMEM)
    return pl.pallas_call(
        finish_kernel,
        out_shape=jax.ShapeDtypeStruct((out_weight.shape[1], block), half),
        in_specs=[held] * 4,
        out_specs=held,
        scratch_shapes=[pltpu.VMEM((2 * size, width), half), pltpu.VMEM((block, width), half)],
        compiler_params=pltpu.CompilerParams(vmem_limit_bytes=6 * MIB),
        name="finish",
    )(keep(attended), keep(arrived), keep(value_weight), keep(out_weight.T)).T


def shards(
    features, tissue, conv_first, bias_first, conv_second, bias_second, key_weight,
    value_weight, latent_queries, out_weight,
):
    rows, cols = lax.axis_size("row"), lax.axis_size("col")
    if rows == cols == 4 and rows * latent_queries.shape[0] == 128:
        return kernel_path(
            features, tissue, conv_first, bias_first, conv_second, bias_second, key_weight,
            value_weight, latent_queries, out_weight,
        )
    marked = jnp.where(tissue[:, :, None] > 0, features, jnp.asarray(FAR, features.dtype))
    marked = with_halo(with_halo(marked, "row", 0), "col", 1)
    normalized = plain_attend(
        features, tissue, marked, latent_queries,
        (conv_first, bias_first, conv_second, bias_second, key_weight),
    )
    attended = lax.dot_general(
        normalized, value_weight, (((0,), (0,)), ((), ())), preferred_element_type=jnp.float32
    ).astype(jnp.bfloat16)
    return jnp.dot(attended, out_weight, preferred_element_type=jnp.float32).astype(jnp.bfloat16)


def solution(mesh):
    placed = (
        P(("groups", "row"), "col", None),
        P(("groups", "row"), "col"),
        P(),
        P(),
        P(),
        P(),
        P(),
        P(),
        P(("col", "row"), None),
        P(None, "col"),
    )
    return jax.shard_map(
        shards, mesh=mesh, in_specs=placed, out_specs=P(("groups", "row"), "col"), check_vma=False
    )
```

```python
import math

import jax
import jax.numpy as jnp
from jax import lax
from jax.experimental import pallas as pl
from jax.experimental.pallas import tpu as pltpu
from jax.sharding import PartitionSpec as P


HALO = 2
FAR = float("inf")
EDGE = 8
LEAD = 16


def shifted(array, axis, step):
    count = lax.axis_size(axis)
    return lax.ppermute(array, axis, [(i, (i + step) % count) for i in range(count)])


def flipped(array, axis, bit):
    count = lax.axis_size(axis)
    return lax.ppermute(array, axis, [(i, i ^ bit) for i in range(count)])


def with_halo(cells, axis, dim):
    size = cells.shape[dim]
    index, last = lax.axis_index(axis), lax.axis_size(axis) - 1
    before = shifted(lax.slice_in_dim(cells, size - HALO, size, axis=dim), axis, 1)
    after = shifted(lax.slice_in_dim(cells, 0, HALO, axis=dim), axis, -1)
    far = jnp.asarray(FAR, cells.dtype)
    return jnp.concatenate(
        [jnp.where(index == 0, far, before), cells, jnp.where(index == last, far, after)], axis=dim
    )


def convolve_valid(padded, weight):
    height, breadth = padded.shape[0] - 2, padded.shape[1] - 2
    channels = padded.shape[2]
    summed = jnp.zeros((height * breadth, weight.shape[3]), jnp.float32)
    for offset_row in range(3):
        for offset_col in range(3):
            window = padded[offset_row : offset_row + height, offset_col : offset_col + breadth]
            summed = summed + jnp.dot(
                window.reshape(height * breadth, channels),
                weight[offset_row, offset_col],
                preferred_element_type=jnp.float32,
            )
    return summed.reshape(height, breadth, weight.shape[3])


def rotated(parts, offset, step):
    count = len(parts)
    size = parts[0].shape[0]
    ordered = [parts[(step * k) % count] for k in range(count)]
    twice = jnp.concatenate(ordered + ordered[:-1], axis=0)
    return lax.dynamic_slice_in_dim(twice, ((count - offset) % count) * size, count * size, axis=0)


def gathered_queries(latent_queries):
    rows, cols = lax.axis_size("row"), lax.axis_size("col")
    parts = [latent_queries] + [shifted(latent_queries, "row", k) for k in range(1, rows)]
    queries = rotated(parts, lax.axis_index("row"), -1)
    own = lax.axis_index("col")
    bit = cols // 2
    groups = [queries]
    order = [0]
    while bit > 0:
        groups = groups + list(flipped(jnp.concatenate(groups, axis=0), "col", bit).reshape(len(groups), -1, queries.shape[1]))
        order = order + [place ^ bit for place in order]
        bit //= 2
    stacked = jnp.stack(groups)
    place = jnp.asarray([order.index(k) for k in range(cols)], jnp.int32)
    return stacked[place[own ^ jnp.arange(cols)]].reshape(-1, queries.shape[1])


def in_parts(values, count):
    parts = []
    for _ in range(count):
        part = lax.reduce_precision(values, exponent_bits=8, mantissa_bits=7)
        parts.append(part.astype(jnp.bfloat16))
        values = values - part
    return parts


def packed(pooled, top, total):
    rest = jnp.zeros((11, pooled.shape[1]), jnp.bfloat16)
    return jnp.concatenate(
        [pooled.astype(jnp.bfloat16)] + in_parts(top, 3) + in_parts(total, 2) + [rest], axis=0
    )


def unpacked(block, channels):
    wide = block.astype(jnp.float32)
    row = lambda k: wide[channels + k : channels + k + 1]
    return wide[:channels], row(0) + row(1) + row(2), row(3) + row(4)


def merged(partials):
    top = partials[0][1]
    for _, other, _ in partials[1:]:
        top = jnp.maximum(top, other)
    pooled = total = 0.0
    for part, shift, count in partials:
        factor = jnp.exp(shift - top)
        pooled = pooled + part * factor
        total = total + count * factor
    return pooled, top, total


def plain_attend(features, tissue, marked, latent_queries, weights):
    conv_first, bias_first, conv_second, bias_second, key_weight = weights
    height, breadth, channels = features.shape
    rows = lax.axis_size("row")
    queries = gathered_queries(latent_queries)
    alive = marked < FAR
    inputs = jnp.where(alive, marked, jnp.zeros_like(marked))
    hidden = jax.nn.gelu(convolve_valid(inputs, conv_first) + bias_first, approximate=False)
    hidden = jnp.where(alive[1:-1, 1:-1], hidden, 0.0).astype(jnp.bfloat16)
    second = jax.nn.gelu(convolve_valid(hidden, conv_second) + bias_second, approximate=False)
    second = jnp.where(alive[HALO:-HALO, HALO:-HALO], second, 0.0).astype(jnp.bfloat16)
    flattened = second.reshape(height * breadth, channels)
    key_rows = jnp.dot(flattened, key_weight, preferred_element_type=jnp.float32).astype(
        jnp.bfloat16
    )
    scale = 1.0 / math.sqrt(latent_queries.shape[1])
    scores = (
        lax.dot_general(
            key_rows, queries, (((1,), (1,)), ((), ())), preferred_element_type=jnp.float32
        )
        * scale
    )
    scores = jnp.where(tissue.reshape(-1, 1) > 0, scores, -1e30)
    shift = jnp.max(scores, axis=0, keepdims=True)
    chosen = jnp.exp(scores - shift)
    total = jnp.sum(chosen, axis=0, keepdims=True)
    pooled = lax.dot_general(
        flattened,
        chosen.astype(jnp.bfloat16),
        (((0,), (0,)), ((), ())),
        preferred_element_type=jnp.float32,
    )

    own_row = lax.axis_index("row")
    size = pooled.shape[1] // rows

    def block_of(step):
        start = ((own_row + step) % rows) * size
        cut = lambda array: lax.dynamic_slice_in_dim(array, start, size, axis=1)
        return cut(pooled), cut(shift), cut(total)

    arrived = [shifted(packed(*block_of(k)), "row", k) for k in range(1, rows)]
    partial = merged([block_of(0)] + [unpacked(block, channels) for block in arrived])
    bit = lax.axis_size("col") // 2
    while bit > 0:
        other = flipped(packed(*partial), "col", bit)
        partial = merged([partial, unpacked(other, channels)])
        bit //= 2
    normalized = (partial[0] / partial[2]).astype(jnp.bfloat16)
    return normalized


def gelu(value):
    return 0.5 * value * (1.0 + lax.erf(value * math.sqrt(0.5)))


def mark_kernel(features, tissue, queries, out, queries_out, features_held, tissue_held, done):
    copies = [
        pltpu.make_async_copy(tissue, tissue_held, done.at[0]),
        pltpu.make_async_copy(features, features_held, done.at[1]),
        pltpu.make_async_copy(queries, queries_out, done.at[2]),
    ]
    for copy in copies:
        copy.start()
    height, breadth, channels = features.shape
    copies[0].wait()
    line = lax.broadcasted_iota(jnp.int32, (breadth, breadth), 0)
    place = lax.broadcasted_iota(jnp.int32, (breadth, breadth), 1)
    flags = tissue_held[...].astype(jnp.float32)
    spread = [
        jnp.where(line == place, jnp.broadcast_to(flags[k : k + 1], line.shape), 0.0)
        for k in range(height)
    ]
    keep = jnp.dot(
        jnp.concatenate(spread, axis=0).astype(jnp.bfloat16),
        jnp.ones((breadth, channels), jnp.bfloat16),
        preferred_element_type=jnp.float32,
    )
    copies[1].wait()
    for k in range(height):
        out[k] = jnp.where(
            keep[k * breadth : (k + 1) * breadth] > 0.0, features_held[k].astype(jnp.float32), FAR
        ).astype(jnp.bfloat16)
    copies[2].wait()


def halve_kernel(own, other, out):
    half = own.shape[0] // 2
    core = lax.rem(lax.axis_index("col"), 2)
    start = pl.multiple_of(core * half, half)
    out[pl.ds(start, half), :] = own[pl.ds(start, half), :]
    out[pl.ds(pl.multiple_of((1 - core) * half, half), half), :] = other[pl.ds(start, half), :]


def conv_kernel(
    marked, top, bottom, paired, crossed, first, bias_first, second,
    mid, second_held, cells, taps, done,
):
    later = pltpu.make_async_copy(second, second_held, done)
    later.start()
    height, breadth, channels = marked.shape
    slot = (cells.shape[0] - 2 * EDGE - LEAD) // (height + 2 * HALO)
    flat = cells.shape[0] - 2 * EDGE
    row, col = lax.axis_index("row"), lax.axis_index("col")
    first_row, last_row = row == 0, row == lax.axis_size("row") - 1
    first_col, last_col = col == 0, col == lax.axis_size("col") - 1
    even = lax.rem(col, 2) == 0

    def put(line, place, values, outside):
        start = EDGE + LEAD + line * slot + place
        values = values.astype(jnp.float32)
        if outside is not None:
            values = jnp.where(outside, FAR, values)
        cells[start : start + values.shape[0], :] = values

    cells[...] = jnp.full(cells.shape, FAR, jnp.float32)
    for line in range(height):
        put(line + HALO, 0, marked[line], None)
    for line in range(HALO):
        put(line, 0, top[line], first_row)
        put(height + HALO + line, 0, bottom[line], last_row)
    for line in range(height + 2 * HALO):
        beyond_left, beyond_right = first_col, last_col
        if line < HALO:
            beyond_left, beyond_right = first_col | first_row, last_col | first_row
        if line >= height + HALO:
            beyond_left, beyond_right = first_col | last_row, last_col | last_row
        one, two = paired[line].astype(jnp.float32), crossed[line].astype(jnp.float32)
        put(line, -HALO, jnp.where(even, two, one), beyond_left)
        put(line, breadth, jnp.where(even, one, two), beyond_right)

    for shift in range(3):
        values = cells[EDGE - 1 + shift : EDGE - 1 + shift + flat, :]
        taps[:, shift * channels : (shift + 1) * channels] = jnp.where(
            values < FAR, values, 0.0
        ).astype(jnp.bfloat16)

    count = flat - 2 * slot
    summed = jnp.dot(taps[0:count, :], first[0], preferred_element_type=jnp.float32)
    for line in range(1, 3):
        summed = summed + jnp.dot(
            taps[line * slot : line * slot + count, :], first[line],
            preferred_element_type=jnp.float32,
        )
    alive = cells[EDGE + slot : EDGE + slot + count, :] < FAR
    edge = jnp.zeros((EDGE, channels), jnp.float32)
    mid[0:EDGE, :] = edge
    mid[EDGE + count : 2 * EDGE + count, :] = edge
    mid[EDGE : EDGE + count, :] = jnp.where(alive, gelu(summed + bias_first[...]), 0.0)
    later.wait()


def second_conv_kernel(marked, mid, second, bias_second, out, sent, taps):
    height, breadth, channels = marked.shape
    count = mid.shape[0] - 2 * EDGE
    slot = (count - LEAD) // (height + 2)
    for shift in range(3):
        taps[0:count, shift * channels : (shift + 1) * channels] = mid[
            EDGE - 1 + shift : EDGE - 1 + shift + count, :
        ].astype(jnp.bfloat16)
    inner = height * slot
    summed = jnp.dot(taps[LEAD : LEAD + inner, :], second[0], preferred_element_type=jnp.float32)
    for line in range(1, 3):
        summed = summed + jnp.dot(
            taps[LEAD + line * slot : LEAD + line * slot + inner, :], second[line],
            preferred_element_type=jnp.float32,
        )
    summed = summed.reshape(height, slot, channels)[:, :breadth].reshape(height * breadth, channels)
    alive = marked[...].reshape(height * breadth, channels) < FAR
    value = gelu(summed + bias_second[...])
    out[...] = jnp.where(alive, value, 0.0).astype(jnp.bfloat16)
    sent[...] = jnp.where(alive, value, FAR).astype(jnp.bfloat16)


def key_kernel(cells, weight, keys):
    keys[...] = jnp.dot(cells[...], weight[...], preferred_element_type=jnp.float32).astype(
        jnp.bfloat16
    )


def write_parts(block, values, top, total):
    channels = values.shape[0]
    parts = []
    for source, count in ((top, 3), (total, 2)):
        rest = source
        for _ in range(count):
            part = rest.astype(jnp.bfloat16).astype(jnp.float32)
            parts.append(part)
            rest = rest - part
    parts.append(jnp.zeros((block.shape[0] - channels - 5, values.shape[1]), jnp.float32))
    block[0:channels, :] = values.astype(jnp.bfloat16)
    block[channels:, :] = jnp.concatenate(parts, axis=0).astype(jnp.bfloat16)


def read_parts(block):
    channels = block.shape[0] - 16
    tail = block[channels:, :].astype(jnp.float32)
    row = lambda k: tail[k : k + 1]
    return (
        block[0:channels, :].astype(jnp.float32),
        row(0) + row(1) + row(2),
        row(3) + row(4),
    )


def read_whole(block):
    channels = block.shape[0] - 8
    tail = block[channels:, :]
    return block[0:channels, :], tail[0:1], tail[1:2]


def write_whole(block, values, top, total):
    channels = values.shape[0]
    block[0:channels, :] = values
    block[channels:, :] = jnp.concatenate(
        [top, total, jnp.zeros((6, values.shape[1]), jnp.float32)], axis=0
    )


PLACES = (0, 2, 1, 3)


def hold_queries(held, parts):
    half = held.shape[0] // 8
    row = lax.axis_index("row")
    blocks = [(part, 2 * k * half) for part in parts for k in range(part.shape[0] // (2 * half))]
    for (part, start), place in zip(blocks, PLACES):
        for parity in range(2):
            source = start + parity * half
            target = pl.multiple_of(parity * 4 * half + (row ^ place) * half, half)
            held[pl.ds(target, half), :] = part[source : source + half, :]


def masked_scores(queries, marked, keys):
    scale = 1.0 / math.sqrt(queries.shape[1])
    raw = lax.dot_general(
        keys[...], queries[...], (((1,), (1,)), ((), ())), preferred_element_type=jnp.float32
    )
    return jnp.where(marked[:, : raw.shape[1]] < FAR, raw * scale, -1e30)


def score_blocks(scores, sides):
    top = jnp.maximum(*[jnp.max(part, axis=0, keepdims=True) for part in scores])
    pooled = total = 0.0
    for part, cells in zip(scores, sides):
        chosen = jnp.exp(part - top)
        total = total + jnp.sum(chosen, axis=0, keepdims=True)
        pooled = pooled + lax.dot_general(
            cells[...], chosen.astype(jnp.bfloat16), (((0,), (0,)), ((), ())),
            preferred_element_type=jnp.float32,
        )
    channels, lanes = pooled.shape[0] // 2, pooled.shape[1]
    turn = lambda array: pltpu.roll(array, lanes // 2, 1)
    lower = lambda rows: lax.broadcasted_iota(jnp.int32, (rows, lanes), 1) < lanes // 2
    tall, flat = lower(channels), lower(1)
    turned, turned_top, turned_total = turn(pooled), turn(top), turn(total)
    return (
        (
            jnp.where(tall, pooled[:channels], turned[channels:]),
            jnp.where(flat, top, turned_top),
            jnp.where(flat, total, turned_total),
        ),
        (
            jnp.where(tall, turned[:channels], pooled[channels:]),
            jnp.where(flat, turned_top, top),
            jnp.where(flat, turned_total, total),
        ),
    )


def own_kernel(own, own_sent, weight, first_queries, last_queries, keys, scores, held):
    key_kernel(own, weight, keys)
    hold_queries(held, (first_queries, last_queries))
    scores[...] = masked_scores(held, own_sent, keys)


def near_kernel(own, own_scores, other_sent, weight, held, out, other, keys):
    values = other_sent[...].astype(jnp.float32)
    other[...] = jnp.where(values < FAR, values, 0.0).astype(jnp.bfloat16)
    key_kernel(other, weight, keys)
    scores = (own_scores[...], masked_scores(held, other_sent, keys))
    for parity, block in enumerate(score_blocks(scores, (own, other))):
        write_whole(out.at[parity], *block)


def far_kernel(
    near, own, own_sent, own_keys, other, other_sent, other_keys, first_queries, last_queries,
    kept, send_1, send_2, send_3, held, blocks,
):
    row, across = lax.axis_index("row"), lax.axis_index("col") // 2
    for parity in range(2):
        blocks[2 * across + parity] = near[parity]
    hold_queries(held, (first_queries, last_queries))
    scores = (
        masked_scores(held, own_sent, own_keys), masked_scores(held, other_sent, other_keys)
    )
    for parity, block in enumerate(score_blocks(scores, (own, other))):
        write_whole(blocks.at[2 * (1 - across) + parity], *block)
    kept[...] = blocks[row]
    for step, send in ((1, send_1), (2, send_2), (3, send_3)):
        write_parts(send, *read_whole(blocks.at[row ^ step]))


def merge_kernel(own, *refs):
    *arrived, whole, packed_out = refs
    values, top, total = merged([read_whole(own)] + [read_parts(block) for block in arrived])
    write_whole(whole, values, top, total)
    write_parts(packed_out, values, top, total)


def normalize_kernel(own, arrived, out):
    values, _, total = merged([read_whole(own), read_parts(arrived)])
    out[...] = (values / total).astype(jnp.bfloat16)


def attend_kernel(normalized, value_weight, attended):
    lanes = normalized.shape[1] // 2
    values = normalized[...].astype(jnp.float32)
    tall = jnp.concatenate([values, pltpu.roll(values, lanes, 1)], axis=0).astype(jnp.bfloat16)
    attended[...] = lax.dot_general(
        tall, value_weight[...], (((0,), (0,)), ((), ())), preferred_element_type=jnp.float32
    )[:lanes].astype(jnp.bfloat16)


def finish_kernel(mine, arrived, value_weight, out_weight, out, other, attended):
    attend_kernel(arrived, value_weight, other)
    core = lax.rem(lax.axis_index("col"), 2)
    piece = mine.shape[0] // 4
    for place in range(4):
        source = slice(place * piece, (place + 1) * piece)
        first = pl.multiple_of((2 * place + core) * piece, piece)
        last = pl.multiple_of((2 * place + 1 - core) * piece, piece)
        attended[pl.ds(first, piece), :] = mine[source]
        attended[pl.ds(last, piece), :] = other[source]
    out[...] = lax.dot_general(
        out_weight[...], attended[...], (((1,), (1,)), ((), ())),
        preferred_element_type=jnp.float32,
    ).astype(out.dtype)


MIB = 1 << 20


def call(kernel, outs, args, scratch=(), limit=4, flops=0, far=()):
    held = pl.BlockSpec(memory_space=pltpu.VMEM)
    outside = pl.BlockSpec(memory_space=pltpu.HBM)
    return pl.pallas_call(
        kernel,
        out_shape=[pltpu.VMEM(shape, dtype) for shape, dtype in outs],
        in_specs=[outside if k in far else held for k in range(len(args))],
        out_specs=[held] * len(outs),
        scratch_shapes=[
            pltpu.VMEM(*kind) if isinstance(kind, tuple) else kind for kind in scratch
        ],
        compiler_params=pltpu.CompilerParams(vmem_limit_bytes=limit * MIB),
        cost_estimate=pl.CostEstimate(flops=flops, bytes_accessed=0, transcendentals=0),
    )(
        *[
            pltpu.with_memory_space_constraint(arg, pltpu.HBM if k in far else pltpu.VMEM)
            for k, arg in enumerate(args)
        ]
    )


def kernel_path(
    features, tissue, conv_first, bias_first, conv_second, bias_second, key_weight,
    value_weight, latent_queries, out_weight,
):
    height, breadth, channels = features.shape
    col, cols = lax.axis_index("col"), lax.axis_size("col")
    size, width = latent_queries.shape
    cells = height * breadth
    slot = -(-(breadth + 2 * HALO) // 16) * 16
    flat = LEAD + (height + 2 * HALO) * slot
    wide, half = jnp.float32, jnp.bfloat16
    block = 4 * size
    whole_block, sent_block = (channels // 2 + 8, block), (channels // 2 + 16, block)
    score_flops = 4 * cells * block * (width + channels)

    beside = flipped(latent_queries, "col", 1)
    marked, queries = call(
        mark_kernel, [(features.shape, half), ((size, width), half)],
        [features, tissue, latent_queries],
        [(features.shape, half), (tissue.shape, jnp.int32), pltpu.SemaphoreType.DMA((3,))],
        far=(0, 1, 2), flops=1 << 20,
    )
    (queries,) = call(halve_kernel, [((size, width), half)], [queries, beside])
    two = flipped(queries, "row", 2)
    one = flipped(queries, "row", 1)
    top = shifted(marked[height - HALO :], "row", 1)
    bottom = shifted(marked[:HALO], "row", -1)
    edge = lambda cut: jnp.concatenate([top[:, cut], marked[:, cut], bottom[:, cut]], axis=0)
    even = lax.rem(col, 2) == 0
    ends = edge(slice(breadth - HALO, breadth)), edge(slice(0, HALO))
    paired = flipped(jnp.where(even, *ends), "col", 1)
    rounds = [(k, (k + 1 if k % 2 else k - 1) % cols) for k in range(cols)]
    crossed = lax.ppermute(jnp.where(even, *ends[::-1]), "col", rounds)

    trio = jnp.concatenate([queries, two, one], axis=0)
    far_trio = flipped(trio, "col", 2)
    three = flipped(two, "row", 1)
    far_three = flipped(three, "col", 2)

    count = flat - 2 * slot
    mid, weight = call(
        conv_kernel,
        [((count + 2 * EDGE, channels), wide), ((3, 3 * channels, channels), half)],
        [
            marked, top, bottom, paired, crossed,
            conv_first.reshape(3, 3 * channels, channels), bias_first.reshape(1, channels),
            conv_second.reshape(3, 3 * channels, channels),
        ],
        [
            ((flat + 2 * EDGE, channels), wide),
            ((flat, 3 * channels), half),
            pltpu.SemaphoreType.DMA,
        ],
        limit=12, far=(7,), flops=21 * cells * channels * channels,
    )
    own, own_sent = call(
        second_conv_kernel, [((cells, channels), half)] * 2,
        [marked, mid, weight, bias_second.reshape(1, channels)],
        [((count, 3 * channels), half)],
        limit=10, flops=18 * cells * channels * channels,
    )
    other_sent = flipped(own_sent, "col", 1)
    own_keys, own_scores, held_queries = call(
        own_kernel,
        [((cells, width), half), ((cells, block), wide), ((block, width), half)],
        [own, own_sent, key_weight, trio, three],
        limit=6, flops=2 * cells * width * (channels + block),
    )
    near, other, other_keys = call(
        near_kernel,
        [((2,) + whole_block, wide), ((cells, channels), half), ((cells, width), half)],
        [own, own_scores, other_sent, key_weight, held_queries],
        limit=8, flops=score_flops,
    )
    kept, *sends = call(
        far_kernel, [(whole_block, wide)] + [(sent_block, half)] * 3,
        [
            near, own, own_sent, own_keys, other, other_sent, other_keys,
            far_trio, far_three,
        ],
        [((block, width), half), ((4,) + whole_block, wide)],
        limit=8, flops=score_flops,
    )
    arrived = [flipped(part, "row", k + 1) for k, part in enumerate(sends)]
    kept, sent = call(merge_kernel, [(whole_block, wide), (sent_block, half)], [kept, *arrived])
    arrived = flipped(sent, "col", 2)
    (normalized,) = call(normalize_kernel, [((channels // 2, block), half)], [kept, arrived])
    arrived = flipped(normalized, "col", 1)
    (attended,) = call(
        attend_kernel, [((2 * size, width), half)], [normalized, value_weight],
        flops=8 * size * channels * width,
    )
    held = pl.BlockSpec(memory_space=pltpu.VMEM)
    keep = lambda array: pltpu.with_memory_space_constraint(array, pltpu.VMEM)
    return pl.pallas_call(
        finish_kernel,
        out_shape=jax.ShapeDtypeStruct((out_weight.shape[1], block), half),
        in_specs=[held] * 4,
        out_specs=held,
        scratch_shapes=[pltpu.VMEM((2 * size, width), half), pltpu.VMEM((block, width), half)],
        compiler_params=pltpu.CompilerParams(vmem_limit_bytes=6 * MIB),
        name="finish",
    )(keep(attended), keep(arrived), keep(value_weight), keep(out_weight.T)).T


def shards(
    features, tissue, conv_first, bias_first, conv_second, bias_second, key_weight,
    value_weight, latent_queries, out_weight,
):
    rows, cols = lax.axis_size("row"), lax.axis_size("col")
    if rows == cols == 4 and rows * latent_queries.shape[0] == 128:
        return kernel_path(
            features, tissue, conv_first, bias_first, conv_second, bias_second, key_weight,
            value_weight, latent_queries, out_weight,
        )
    marked = jnp.where(tissue[:, :, None] > 0, features, jnp.asarray(FAR, features.dtype))
    marked = with_halo(with_halo(marked, "row", 0), "col", 1)
    normalized = plain_attend(
        features, tissue, marked, latent_queries,
        (conv_first, bias_first, conv_second, bias_second, key_weight),
    )
    attended = lax.dot_general(
        normalized, value_weight, (((0,), (0,)), ((), ())), preferred_element_type=jnp.float32
    ).astype(jnp.bfloat16)
    return jnp.dot(attended, out_weight, preferred_element_type=jnp.float32).astype(jnp.bfloat16)


def solution(mesh):
    placed = (
        P(("groups", "row"), "col", None),
        P(("groups", "row"), "col"),
        P(),
        P(),
        P(),
        P(),
        P(),
        P(),
        P(("col", "row"), None),
        P(None, "col"),
    )
    return jax.shard_map(
        shards, mesh=mesh, in_specs=placed, out_specs=P(("groups", "row"), "col"), check_vma=False
    )
```

```python
import math

import jax
import jax.numpy as jnp
from jax import lax
from jax.experimental import pallas as pl
from jax.experimental.pallas import tpu as pltpu
from jax.sharding import PartitionSpec as P


HALO = 2
FAR = float("inf")
EDGE = 8
LEAD = 16


def shifted(array, axis, step):
    count = lax.axis_size(axis)
    return lax.ppermute(array, axis, [(i, (i + step) % count) for i in range(count)])


def flipped(array, axis, bit):
    count = lax.axis_size(axis)
    return lax.ppermute(array, axis, [(i, i ^ bit) for i in range(count)])


def with_halo(cells, axis, dim):
    size = cells.shape[dim]
    index, last = lax.axis_index(axis), lax.axis_size(axis) - 1
    before = shifted(lax.slice_in_dim(cells, size - HALO, size, axis=dim), axis, 1)
    after = shifted(lax.slice_in_dim(cells, 0, HALO, axis=dim), axis, -1)
    far = jnp.asarray(FAR, cells.dtype)
    return jnp.concatenate(
        [jnp.where(index == 0, far, before), cells, jnp.where(index == last, far, after)], axis=dim
    )


def convolve_valid(padded, weight):
    height, breadth = padded.shape[0] - 2, padded.shape[1] - 2
    channels = padded.shape[2]
    summed = jnp.zeros((height * breadth, weight.shape[3]), jnp.float32)
    for offset_row in range(3):
        for offset_col in range(3):
            window = padded[offset_row : offset_row + height, offset_col : offset_col + breadth]
            summed = summed + jnp.dot(
                window.reshape(height * breadth, channels),
                weight[offset_row, offset_col],
                preferred_element_type=jnp.float32,
            )
    return summed.reshape(height, breadth, weight.shape[3])


def rotated(parts, offset, step):
    count = len(parts)
    size = parts[0].shape[0]
    ordered = [parts[(step * k) % count] for k in range(count)]
    twice = jnp.concatenate(ordered + ordered[:-1], axis=0)
    return lax.dynamic_slice_in_dim(twice, ((count - offset) % count) * size, count * size, axis=0)


def gathered_queries(latent_queries):
    rows, cols = lax.axis_size("row"), lax.axis_size("col")
    parts = [latent_queries] + [shifted(latent_queries, "row", k) for k in range(1, rows)]
    queries = rotated(parts, lax.axis_index("row"), -1)
    own = lax.axis_index("col")
    bit = cols // 2
    groups = [queries]
    order = [0]
    while bit > 0:
        groups = groups + list(flipped(jnp.concatenate(groups, axis=0), "col", bit).reshape(len(groups), -1, queries.shape[1]))
        order = order + [place ^ bit for place in order]
        bit //= 2
    stacked = jnp.stack(groups)
    place = jnp.asarray([order.index(k) for k in range(cols)], jnp.int32)
    return stacked[place[own ^ jnp.arange(cols)]].reshape(-1, queries.shape[1])


def in_parts(values, count):
    parts = []
    for _ in range(count):
        part = lax.reduce_precision(values, exponent_bits=8, mantissa_bits=7)
        parts.append(part.astype(jnp.bfloat16))
        values = values - part
    return parts


def packed(pooled, top, total):
    rest = jnp.zeros((11, pooled.shape[1]), jnp.bfloat16)
    return jnp.concatenate(
        [pooled.astype(jnp.bfloat16)] + in_parts(top, 3) + in_parts(total, 2) + [rest], axis=0
    )


def unpacked(block, channels):
    wide = block.astype(jnp.float32)
    row = lambda k: wide[channels + k : channels + k + 1]
    return wide[:channels], row(0) + row(1) + row(2), row(3) + row(4)


def merged(partials):
    top = partials[0][1]
    for _, other, _ in partials[1:]:
        top = jnp.maximum(top, other)
    pooled = total = 0.0
    for part, shift, count in partials:
        factor = jnp.exp(shift - top)
        pooled = pooled + part * factor
        total = total + count * factor
    return pooled, top, total


def plain_attend(features, tissue, marked, latent_queries, weights):
    conv_first, bias_first, conv_second, bias_second, key_weight = weights
    height, breadth, channels = features.shape
    rows = lax.axis_size("row")
    queries = gathered_queries(latent_queries)
    alive = marked < FAR
    inputs = jnp.where(alive, marked, jnp.zeros_like(marked))
    hidden = jax.nn.gelu(convolve_valid(inputs, conv_first) + bias_first, approximate=False)
    hidden = jnp.where(alive[1:-1, 1:-1], hidden, 0.0).astype(jnp.bfloat16)
    second = jax.nn.gelu(convolve_valid(hidden, conv_second) + bias_second, approximate=False)
    second = jnp.where(alive[HALO:-HALO, HALO:-HALO], second, 0.0).astype(jnp.bfloat16)
    flattened = second.reshape(height * breadth, channels)
    key_rows = jnp.dot(flattened, key_weight, preferred_element_type=jnp.float32).astype(
        jnp.bfloat16
    )
    scale = 1.0 / math.sqrt(latent_queries.shape[1])
    scores = (
        lax.dot_general(
            key_rows, queries, (((1,), (1,)), ((), ())), preferred_element_type=jnp.float32
        )
        * scale
    )
    scores = jnp.where(tissue.reshape(-1, 1) > 0, scores, -1e30)
    shift = jnp.max(scores, axis=0, keepdims=True)
    chosen = jnp.exp(scores - shift)
    total = jnp.sum(chosen, axis=0, keepdims=True)
    pooled = lax.dot_general(
        flattened,
        chosen.astype(jnp.bfloat16),
        (((0,), (0,)), ((), ())),
        preferred_element_type=jnp.float32,
    )

    own_row = lax.axis_index("row")
    size = pooled.shape[1] // rows

    def block_of(step):
        start = ((own_row + step) % rows) * size
        cut = lambda array: lax.dynamic_slice_in_dim(array, start, size, axis=1)
        return cut(pooled), cut(shift), cut(total)

    arrived = [shifted(packed(*block_of(k)), "row", k) for k in range(1, rows)]
    partial = merged([block_of(0)] + [unpacked(block, channels) for block in arrived])
    bit = lax.axis_size("col") // 2
    while bit > 0:
        other = flipped(packed(*partial), "col", bit)
        partial = merged([partial, unpacked(other, channels)])
        bit //= 2
    normalized = (partial[0] / partial[2]).astype(jnp.bfloat16)
    return normalized


def gelu(value):
    return 0.5 * value * (1.0 + lax.erf(value * math.sqrt(0.5)))


def mark_kernel(features, tissue, queries, out, queries_out, features_held, tissue_held, done):
    copies = [
        pltpu.make_async_copy(tissue, tissue_held, done.at[0]),
        pltpu.make_async_copy(features, features_held, done.at[1]),
        pltpu.make_async_copy(queries, queries_out, done.at[2]),
    ]
    for copy in copies:
        copy.start()
    height, breadth, channels = features.shape
    copies[0].wait()
    line = lax.broadcasted_iota(jnp.int32, (breadth, breadth), 0)
    place = lax.broadcasted_iota(jnp.int32, (breadth, breadth), 1)
    flags = tissue_held[...].astype(jnp.float32)
    spread = [
        jnp.where(line == place, jnp.broadcast_to(flags[k : k + 1], line.shape), 0.0)
        for k in range(height)
    ]
    keep = jnp.dot(
        jnp.concatenate(spread, axis=0).astype(jnp.bfloat16),
        jnp.ones((breadth, channels), jnp.bfloat16),
        preferred_element_type=jnp.float32,
    )
    copies[1].wait()
    for k in range(height):
        out[k] = jnp.where(
            keep[k * breadth : (k + 1) * breadth] > 0.0, features_held[k].astype(jnp.float32), FAR
        ).astype(jnp.bfloat16)
    copies[2].wait()


def halve_kernel(own, other, out):
    half = own.shape[0] // 2
    core = lax.rem(lax.axis_index("col"), 2)
    start = pl.multiple_of(core * half, half)
    out[pl.ds(start, half), :] = own[pl.ds(start, half), :]
    out[pl.ds(pl.multiple_of((1 - core) * half, half), half), :] = other[pl.ds(start, half), :]


def conv_kernel(
    marked, top, bottom, paired, crossed, first, bias_first, second,
    mid, second_held, cells, taps, done,
):
    later = pltpu.make_async_copy(second, second_held, done)
    later.start()
    height, breadth, channels = marked.shape
    slot = (cells.shape[0] - 2 * EDGE - LEAD) // (height + 2 * HALO)
    flat = cells.shape[0] - 2 * EDGE
    row, col = lax.axis_index("row"), lax.axis_index("col")
    first_row, last_row = row == 0, row == lax.axis_size("row") - 1
    first_col, last_col = col == 0, col == lax.axis_size("col") - 1
    even = lax.rem(col, 2) == 0

    def put(line, place, values, outside):
        start = EDGE + LEAD + line * slot + place
        values = values.astype(jnp.float32)
        if outside is not None:
            values = jnp.where(outside, FAR, values)
        cells[start : start + values.shape[0], :] = values

    cells[...] = jnp.full(cells.shape, FAR, jnp.float32)
    for line in range(height):
        put(line + HALO, 0, marked[line], None)
    for line in range(HALO):
        put(line, 0, top[line], first_row)
        put(height + HALO + line, 0, bottom[line], last_row)
    for line in range(height + 2 * HALO):
        beyond_left, beyond_right = first_col, last_col
        if line < HALO:
            beyond_left, beyond_right = first_col | first_row, last_col | first_row
        if line >= height + HALO:
            beyond_left, beyond_right = first_col | last_row, last_col | last_row
        one, two = paired[line].astype(jnp.float32), crossed[line].astype(jnp.float32)
        put(line, -HALO, jnp.where(even, two, one), beyond_left)
        put(line, breadth, jnp.where(even, one, two), beyond_right)

    for shift in range(3):
        values = cells[EDGE - 1 + shift : EDGE - 1 + shift + flat, :]
        taps[:, shift * channels : (shift + 1) * channels] = jnp.where(
            values < FAR, values, 0.0
        ).astype(jnp.bfloat16)

    count = flat - 2 * slot
    summed = jnp.dot(taps[0:count, :], first[0], preferred_element_type=jnp.float32)
    for line in range(1, 3):
        summed = summed + jnp.dot(
            taps[line * slot : line * slot + count, :], first[line],
            preferred_element_type=jnp.float32,
        )
    alive = cells[EDGE + slot : EDGE + slot + count, :] < FAR
    edge = jnp.zeros((EDGE, channels), jnp.float32)
    mid[0:EDGE, :] = edge
    mid[EDGE + count : 2 * EDGE + count, :] = edge
    mid[EDGE : EDGE + count, :] = jnp.where(alive, gelu(summed + bias_first[...]), 0.0)
    later.wait()


def second_conv_kernel(marked, mid, second, bias_second, out, sent, taps):
    height, breadth, channels = marked.shape
    count = mid.shape[0] - 2 * EDGE
    slot = (count - LEAD) // (height + 2)
    for shift in range(3):
        taps[0:count, shift * channels : (shift + 1) * channels] = mid[
            EDGE - 1 + shift : EDGE - 1 + shift + count, :
        ].astype(jnp.bfloat16)
    inner = height * slot
    summed = jnp.dot(taps[LEAD : LEAD + inner, :], second[0], preferred_element_type=jnp.float32)
    for line in range(1, 3):
        summed = summed + jnp.dot(
            taps[LEAD + line * slot : LEAD + line * slot + inner, :], second[line],
            preferred_element_type=jnp.float32,
        )
    summed = summed.reshape(height, slot, channels)[:, :breadth].reshape(height * breadth, channels)
    alive = marked[...].reshape(height * breadth, channels) < FAR
    value = gelu(summed + bias_second[...])
    out[...] = jnp.where(alive, value, 0.0).astype(jnp.bfloat16)
    sent[...] = jnp.where(alive, value, FAR).astype(jnp.bfloat16)


def key_kernel(cells, weight, keys):
    keys[...] = jnp.dot(cells[...], weight[...], preferred_element_type=jnp.float32).astype(
        jnp.bfloat16
    )


def write_parts(block, values, top, total):
    channels = values.shape[0]
    parts = []
    for source, count in ((top, 3), (total, 2)):
        rest = source
        for _ in range(count):
            part = rest.astype(jnp.bfloat16).astype(jnp.float32)
            parts.append(part)
            rest = rest - part
    parts.append(jnp.zeros((block.shape[0] - channels - 5, values.shape[1]), jnp.float32))
    block[0:channels, :] = values.astype(jnp.bfloat16)
    block[channels:, :] = jnp.concatenate(parts, axis=0).astype(jnp.bfloat16)


def read_parts(block):
    channels = block.shape[0] - 16
    tail = block[channels:, :].astype(jnp.float32)
    row = lambda k: tail[k : k + 1]
    return (
        block[0:channels, :].astype(jnp.float32),
        row(0) + row(1) + row(2),
        row(3) + row(4),
    )


def read_whole(block):
    channels = block.shape[0] - 8
    tail = block[channels:, :]
    return block[0:channels, :], tail[0:1], tail[1:2]


def write_whole(block, values, top, total):
    channels = values.shape[0]
    block[0:channels, :] = values
    block[channels:, :] = jnp.concatenate(
        [top, total, jnp.zeros((6, values.shape[1]), jnp.float32)], axis=0
    )


PLACES = (0, 2, 1, 3)


def hold_queries(held, parts):
    half = held.shape[0] // 8
    row = lax.axis_index("row")
    blocks = [(part, 2 * k * half) for part in parts for k in range(part.shape[0] // (2 * half))]
    for (part, start), place in zip(blocks, PLACES):
        for parity in range(2):
            source = start + parity * half
            target = pl.multiple_of(parity * 4 * half + (row ^ place) * half, half)
            held[pl.ds(target, half), :] = part[source : source + half, :]


def masked_scores(queries, marked, keys):
    scale = 1.0 / math.sqrt(queries.shape[1])
    raw = lax.dot_general(
        keys[...], queries[...], (((1,), (1,)), ((), ())), preferred_element_type=jnp.float32
    )
    return jnp.where(marked[:, : raw.shape[1]] < FAR, raw * scale, -1e30)


def score_blocks(scores, sides):
    top = jnp.maximum(*[jnp.max(part, axis=0, keepdims=True) for part in scores])
    pooled = total = 0.0
    for part, cells in zip(scores, sides):
        chosen = jnp.exp(part - top)
        total = total + jnp.sum(chosen, axis=0, keepdims=True)
        pooled = pooled + lax.dot_general(
            cells[...], chosen.astype(jnp.bfloat16), (((0,), (0,)), ((), ())),
            preferred_element_type=jnp.float32,
        )
    channels, lanes = pooled.shape[0] // 2, pooled.shape[1]
    turn = lambda array: pltpu.roll(array, lanes // 2, 1)
    lower = lambda rows: lax.broadcasted_iota(jnp.int32, (rows, lanes), 1) < lanes // 2
    tall, flat = lower(channels), lower(1)
    turned, turned_top, turned_total = turn(pooled), turn(top), turn(total)
    return (
        (
            jnp.where(tall, pooled[:channels], turned[channels:]),
            jnp.where(flat, top, turned_top),
            jnp.where(flat, total, turned_total),
        ),
        (
            jnp.where(tall, turned[:channels], pooled[channels:]),
            jnp.where(flat, turned_top, top),
            jnp.where(flat, turned_total, total),
        ),
    )


def own_kernel(own, own_sent, weight, *refs):
    *queries, keys, scores, held = refs
    key_kernel(own, weight, keys)
    hold_queries(held, queries)
    scores[...] = masked_scores(held, own_sent, keys)


def near_kernel(own, own_scores, other_sent, weight, held, out, other, keys):
    values = other_sent[...].astype(jnp.float32)
    other[...] = jnp.where(values < FAR, values, 0.0).astype(jnp.bfloat16)
    key_kernel(other, weight, keys)
    scores = (own_scores[...], masked_scores(held, other_sent, keys))
    for parity, block in enumerate(score_blocks(scores, (own, other))):
        write_whole(out.at[parity], *block)


def far_kernel(
    near, own, own_sent, own_keys, other, other_sent, other_keys, *refs
):
    *queries, kept, send_1, send_2, send_3, held, blocks = refs
    row, across = lax.axis_index("row"), lax.axis_index("col") // 2
    for parity in range(2):
        blocks[2 * across + parity] = near[parity]
    hold_queries(held, queries)
    scores = (
        masked_scores(held, own_sent, own_keys), masked_scores(held, other_sent, other_keys)
    )
    for parity, block in enumerate(score_blocks(scores, (own, other))):
        write_whole(blocks.at[2 * (1 - across) + parity], *block)
    kept[...] = blocks[row]
    for step, send in ((1, send_1), (2, send_2), (3, send_3)):
        write_parts(send, *read_whole(blocks.at[row ^ step]))


def merge_kernel(own, *refs):
    *arrived, whole, packed_out = refs
    values, top, total = merged([read_whole(own)] + [read_parts(block) for block in arrived])
    write_whole(whole, values, top, total)
    write_parts(packed_out, values, top, total)


def normalize_kernel(own, arrived, out):
    values, _, total = merged([read_whole(own), read_parts(arrived)])
    out[...] = (values / total).astype(jnp.bfloat16)


def attend_kernel(normalized, value_weight, attended):
    lanes = normalized.shape[1] // 2
    values = normalized[...].astype(jnp.float32)
    tall = jnp.concatenate([values, pltpu.roll(values, lanes, 1)], axis=0).astype(jnp.bfloat16)
    attended[...] = lax.dot_general(
        tall, value_weight[...], (((0,), (0,)), ((), ())), preferred_element_type=jnp.float32
    )[:lanes].astype(jnp.bfloat16)


def finish_kernel(mine, arrived, value_weight, out_weight, out, other, attended):
    attend_kernel(arrived, value_weight, other)
    core = lax.rem(lax.axis_index("col"), 2)
    piece = mine.shape[0] // 4
    for place in range(4):
        source = slice(place * piece, (place + 1) * piece)
        first = pl.multiple_of((2 * place + core) * piece, piece)
        last = pl.multiple_of((2 * place + 1 - core) * piece, piece)
        attended[pl.ds(first, piece), :] = mine[source]
        attended[pl.ds(last, piece), :] = other[source]
    out[...] = lax.dot_general(
        out_weight[...], attended[...], (((1,), (1,)), ((), ())),
        preferred_element_type=jnp.float32,
    ).astype(out.dtype)


MIB = 1 << 20


def call(kernel, outs, args, scratch=(), limit=4, flops=0, far=()):
    held = pl.BlockSpec(memory_space=pltpu.VMEM)
    outside = pl.BlockSpec(memory_space=pltpu.HBM)
    return pl.pallas_call(
        kernel,
        out_shape=[pltpu.VMEM(shape, dtype) for shape, dtype in outs],
        in_specs=[outside if k in far else held for k in range(len(args))],
        out_specs=[held] * len(outs),
        scratch_shapes=[
            pltpu.VMEM(*kind) if isinstance(kind, tuple) else kind for kind in scratch
        ],
        compiler_params=pltpu.CompilerParams(vmem_limit_bytes=limit * MIB),
        cost_estimate=pl.CostEstimate(flops=flops, bytes_accessed=0, transcendentals=0),
    )(
        *[
            pltpu.with_memory_space_constraint(arg, pltpu.HBM if k in far else pltpu.VMEM)
            for k, arg in enumerate(args)
        ]
    )


def kernel_path(
    features, tissue, conv_first, bias_first, conv_second, bias_second, key_weight,
    value_weight, latent_queries, out_weight,
):
    height, breadth, channels = features.shape
    col, cols = lax.axis_index("col"), lax.axis_size("col")
    size, width = latent_queries.shape
    cells = height * breadth
    slot = -(-(breadth + 2 * HALO) // 16) * 16
    flat = LEAD + (height + 2 * HALO) * slot
    wide, half = jnp.float32, jnp.bfloat16
    block = 4 * size
    whole_block, sent_block = (channels // 2 + 8, block), (channels // 2 + 16, block)
    score_flops = 4 * cells * block * (width + channels)

    beside = flipped(latent_queries, "col", 1)
    marked, queries = call(
        mark_kernel, [(features.shape, half), ((size, width), half)],
        [features, tissue, latent_queries],
        [(features.shape, half), (tissue.shape, jnp.int32), pltpu.SemaphoreType.DMA((3,))],
        far=(0, 1, 2), flops=1 << 20,
    )
    (queries,) = call(halve_kernel, [((size, width), half)], [queries, beside])
    far_queries = flipped(queries, "col", 2)
    two = flipped(queries, "row", 2)
    one = flipped(queries, "row", 1)
    top = shifted(marked[height - HALO :], "row", 1)
    bottom = shifted(marked[:HALO], "row", -1)
    edge = lambda cut: jnp.concatenate([top[:, cut], marked[:, cut], bottom[:, cut]], axis=0)
    even = lax.rem(col, 2) == 0
    ends = edge(slice(breadth - HALO, breadth)), edge(slice(0, HALO))
    paired = flipped(jnp.where(even, *ends), "col", 1)
    rounds = [(k, (k + 1 if k % 2 else k - 1) % cols) for k in range(cols)]
    crossed = lax.ppermute(jnp.where(even, *ends[::-1]), "col", rounds)

    pair = jnp.concatenate([two, one], axis=0)
    far_pair = flipped(pair, "col", 2)
    three = flipped(two, "row", 1)
    far_three = flipped(three, "col", 2)

    count = flat - 2 * slot
    mid, weight = call(
        conv_kernel,
        [((count + 2 * EDGE, channels), wide), ((3, 3 * channels, channels), half)],
        [
            marked, top, bottom, paired, crossed,
            conv_first.reshape(3, 3 * channels, channels), bias_first.reshape(1, channels),
            conv_second.reshape(3, 3 * channels, channels),
        ],
        [
            ((flat + 2 * EDGE, channels), wide),
            ((flat, 3 * channels), half),
            pltpu.SemaphoreType.DMA,
        ],
        limit=12, far=(7,), flops=21 * cells * channels * channels,
    )
    own, own_sent = call(
        second_conv_kernel, [((cells, channels), half)] * 2,
        [marked, mid, weight, bias_second.reshape(1, channels)],
        [((count, 3 * channels), half)],
        limit=10, flops=18 * cells * channels * channels,
    )
    other_sent = flipped(own_sent, "col", 1)
    own_keys, own_scores, held_queries = call(
        own_kernel,
        [((cells, width), half), ((cells, block), wide), ((block, width), half)],
        [own, own_sent, key_weight, queries, pair, three],
        limit=6, flops=2 * cells * width * (channels + block),
    )
    near, other, other_keys = call(
        near_kernel,
        [((2,) + whole_block, wide), ((cells, channels), half), ((cells, width), half)],
        [own, own_scores, other_sent, key_weight, held_queries],
        limit=8, flops=score_flops,
    )
    kept, *sends = call(
        far_kernel, [(whole_block, wide)] + [(sent_block, half)] * 3,
        [
            near, own, own_sent, own_keys, other, other_sent, other_keys,
            far_queries, far_pair, far_three,
        ],
        [((block, width), half), ((4,) + whole_block, wide)],
        limit=8, flops=score_flops,
    )
    arrived = [flipped(part, "row", k + 1) for k, part in enumerate(sends)]
    kept, sent = call(merge_kernel, [(whole_block, wide), (sent_block, half)], [kept, *arrived])
    arrived = flipped(sent, "col", 2)
    (normalized,) = call(normalize_kernel, [((channels // 2, block), half)], [kept, arrived])
    arrived = flipped(normalized, "col", 1)
    (attended,) = call(
        attend_kernel, [((2 * size, width), half)], [normalized, value_weight],
        flops=8 * size * channels * width,
    )
    held = pl.BlockSpec(memory_space=pltpu.VMEM)
    keep = lambda array: pltpu.with_memory_space_constraint(array, pltpu.VMEM)
    return pl.pallas_call(
        finish_kernel,
        out_shape=jax.ShapeDtypeStruct((out_weight.shape[1], block), half),
        in_specs=[held] * 4,
        out_specs=held,
        scratch_shapes=[pltpu.VMEM((2 * size, width), half), pltpu.VMEM((block, width), half)],
        compiler_params=pltpu.CompilerParams(vmem_limit_bytes=6 * MIB),
        name="finish",
    )(keep(attended), keep(arrived), keep(value_weight), keep(out_weight.T)).T


def shards(
    features, tissue, conv_first, bias_first, conv_second, bias_second, key_weight,
    value_weight, latent_queries, out_weight,
):
    rows, cols = lax.axis_size("row"), lax.axis_size("col")
    if rows == cols == 4 and rows * latent_queries.shape[0] == 128:
        return kernel_path(
            features, tissue, conv_first, bias_first, conv_second, bias_second, key_weight,
            value_weight, latent_queries, out_weight,
        )
    marked = jnp.where(tissue[:, :, None] > 0, features, jnp.asarray(FAR, features.dtype))
    marked = with_halo(with_halo(marked, "row", 0), "col", 1)
    normalized = plain_attend(
        features, tissue, marked, latent_queries,
        (conv_first, bias_first, conv_second, bias_second, key_weight),
    )
    attended = lax.dot_general(
        normalized, value_weight, (((0,), (0,)), ((), ())), preferred_element_type=jnp.float32
    ).astype(jnp.bfloat16)
    return jnp.dot(attended, out_weight, preferred_element_type=jnp.float32).astype(jnp.bfloat16)


def solution(mesh):
    placed = (
        P(("groups", "row"), "col", None),
        P(("groups", "row"), "col"),
        P(),
        P(),
        P(),
        P(),
        P(),
        P(),
        P(("col", "row"), None),
        P(None, "col"),
    )
    return jax.shard_map(
        shards, mesh=mesh, in_specs=placed, out_specs=P(("groups", "row"), "col"), check_vma=False
    )
```

```python
import math

import jax
import jax.numpy as jnp
from jax import lax
from jax.experimental import pallas as pl
from jax.experimental.pallas import tpu as pltpu
from jax.sharding import PartitionSpec as P


HALO = 2
FAR = float("inf")
EDGE = 8
LEAD = 16


def shifted(array, axis, step):
    count = lax.axis_size(axis)
    return lax.ppermute(array, axis, [(i, (i + step) % count) for i in range(count)])


def flipped(array, axis, bit):
    count = lax.axis_size(axis)
    return lax.ppermute(array, axis, [(i, i ^ bit) for i in range(count)])


def with_halo(cells, axis, dim):
    size = cells.shape[dim]
    index, last = lax.axis_index(axis), lax.axis_size(axis) - 1
    before = shifted(lax.slice_in_dim(cells, size - HALO, size, axis=dim), axis, 1)
    after = shifted(lax.slice_in_dim(cells, 0, HALO, axis=dim), axis, -1)
    far = jnp.asarray(FAR, cells.dtype)
    return jnp.concatenate(
        [jnp.where(index == 0, far, before), cells, jnp.where(index == last, far, after)], axis=dim
    )


def convolve_valid(padded, weight):
    height, breadth = padded.shape[0] - 2, padded.shape[1] - 2
    channels = padded.shape[2]
    summed = jnp.zeros((height * breadth, weight.shape[3]), jnp.float32)
    for offset_row in range(3):
        for offset_col in range(3):
            window = padded[offset_row : offset_row + height, offset_col : offset_col + breadth]
            summed = summed + jnp.dot(
                window.reshape(height * breadth, channels),
                weight[offset_row, offset_col],
                preferred_element_type=jnp.float32,
            )
    return summed.reshape(height, breadth, weight.shape[3])


def rotated(parts, offset, step):
    count = len(parts)
    size = parts[0].shape[0]
    ordered = [parts[(step * k) % count] for k in range(count)]
    twice = jnp.concatenate(ordered + ordered[:-1], axis=0)
    return lax.dynamic_slice_in_dim(twice, ((count - offset) % count) * size, count * size, axis=0)


def gathered_queries(latent_queries):
    rows, cols = lax.axis_size("row"), lax.axis_size("col")
    parts = [latent_queries] + [shifted(latent_queries, "row", k) for k in range(1, rows)]
    queries = rotated(parts, lax.axis_index("row"), -1)
    own = lax.axis_index("col")
    bit = cols // 2
    groups = [queries]
    order = [0]
    while bit > 0:
        groups = groups + list(flipped(jnp.concatenate(groups, axis=0), "col", bit).reshape(len(groups), -1, queries.shape[1]))
        order = order + [place ^ bit for place in order]
        bit //= 2
    stacked = jnp.stack(groups)
    place = jnp.asarray([order.index(k) for k in range(cols)], jnp.int32)
    return stacked[place[own ^ jnp.arange(cols)]].reshape(-1, queries.shape[1])


def in_parts(values, count):
    parts = []
    for _ in range(count):
        part = lax.reduce_precision(values, exponent_bits=8, mantissa_bits=7)
        parts.append(part.astype(jnp.bfloat16))
        values = values - part
    return parts


def packed(pooled, top, total):
    rest = jnp.zeros((11, pooled.shape[1]), jnp.bfloat16)
    return jnp.concatenate(
        [pooled.astype(jnp.bfloat16)] + in_parts(top, 3) + in_parts(total, 2) + [rest], axis=0
    )


def unpacked(block, channels):
    wide = block.astype(jnp.float32)
    row = lambda k: wide[channels + k : channels + k + 1]
    return wide[:channels], row(0) + row(1) + row(2), row(3) + row(4)


def merged(partials):
    top = partials[0][1]
    for _, other, _ in partials[1:]:
        top = jnp.maximum(top, other)
    pooled = total = 0.0
    for part, shift, count in partials:
        factor = jnp.exp(shift - top)
        pooled = pooled + part * factor
        total = total + count * factor
    return pooled, top, total


def plain_attend(features, tissue, marked, latent_queries, weights):
    conv_first, bias_first, conv_second, bias_second, key_weight = weights
    height, breadth, channels = features.shape
    rows = lax.axis_size("row")
    queries = gathered_queries(latent_queries)
    alive = marked < FAR
    inputs = jnp.where(alive, marked, jnp.zeros_like(marked))
    hidden = jax.nn.gelu(convolve_valid(inputs, conv_first) + bias_first, approximate=False)
    hidden = jnp.where(alive[1:-1, 1:-1], hidden, 0.0).astype(jnp.bfloat16)
    second = jax.nn.gelu(convolve_valid(hidden, conv_second) + bias_second, approximate=False)
    second = jnp.where(alive[HALO:-HALO, HALO:-HALO], second, 0.0).astype(jnp.bfloat16)
    flattened = second.reshape(height * breadth, channels)
    key_rows = jnp.dot(flattened, key_weight, preferred_element_type=jnp.float32).astype(
        jnp.bfloat16
    )
    scale = 1.0 / math.sqrt(latent_queries.shape[1])
    scores = (
        lax.dot_general(
            key_rows, queries, (((1,), (1,)), ((), ())), preferred_element_type=jnp.float32
        )
        * scale
    )
    scores = jnp.where(tissue.reshape(-1, 1) > 0, scores, -1e30)
    shift = jnp.max(scores, axis=0, keepdims=True)
    chosen = jnp.exp(scores - shift)
    total = jnp.sum(chosen, axis=0, keepdims=True)
    pooled = lax.dot_general(
        flattened,
        chosen.astype(jnp.bfloat16),
        (((0,), (0,)), ((), ())),
        preferred_element_type=jnp.float32,
    )

    own_row = lax.axis_index("row")
    size = pooled.shape[1] // rows

    def block_of(step):
        start = ((own_row + step) % rows) * size
        cut = lambda array: lax.dynamic_slice_in_dim(array, start, size, axis=1)
        return cut(pooled), cut(shift), cut(total)

    arrived = [shifted(packed(*block_of(k)), "row", k) for k in range(1, rows)]
    partial = merged([block_of(0)] + [unpacked(block, channels) for block in arrived])
    bit = lax.axis_size("col") // 2
    while bit > 0:
        other = flipped(packed(*partial), "col", bit)
        partial = merged([partial, unpacked(other, channels)])
        bit //= 2
    normalized = (partial[0] / partial[2]).astype(jnp.bfloat16)
    return normalized


def gelu(value):
    return 0.5 * value * (1.0 + lax.erf(value * math.sqrt(0.5)))


def mark_kernel(features, tissue, queries, out, queries_out, features_held, tissue_held, done):
    copies = [
        pltpu.make_async_copy(tissue, tissue_held, done.at[0]),
        pltpu.make_async_copy(features, features_held, done.at[1]),
        pltpu.make_async_copy(queries, queries_out, done.at[2]),
    ]
    for copy in copies:
        copy.start()
    height, breadth, channels = features.shape
    copies[0].wait()
    line = lax.broadcasted_iota(jnp.int32, (breadth, breadth), 0)
    place = lax.broadcasted_iota(jnp.int32, (breadth, breadth), 1)
    flags = tissue_held[...].astype(jnp.float32)
    spread = [
        jnp.where(line == place, jnp.broadcast_to(flags[k : k + 1], line.shape), 0.0)
        for k in range(height)
    ]
    keep = jnp.dot(
        jnp.concatenate(spread, axis=0).astype(jnp.bfloat16),
        jnp.ones((breadth, channels), jnp.bfloat16),
        preferred_element_type=jnp.float32,
    )
    copies[1].wait()
    for k in range(height):
        out[k] = jnp.where(
            keep[k * breadth : (k + 1) * breadth] > 0.0, features_held[k].astype(jnp.float32), FAR
        ).astype(jnp.bfloat16)
    copies[2].wait()


def halve_kernel(own, other, out):
    half = own.shape[0] // 2
    core = lax.rem(lax.axis_index("col"), 2)
    start = pl.multiple_of(core * half, half)
    out[pl.ds(start, half), :] = own[pl.ds(start, half), :]
    out[pl.ds(pl.multiple_of((1 - core) * half, half), half), :] = other[pl.ds(start, half), :]


def conv_kernel(
    marked, top, bottom, paired, crossed, first, bias_first, second,
    mid, second_held, cells, taps, done,
):
    later = pltpu.make_async_copy(second, second_held, done)
    later.start()
    height, breadth, channels = marked.shape
    slot = (cells.shape[0] - 2 * EDGE - LEAD) // (height + 2 * HALO)
    flat = cells.shape[0] - 2 * EDGE
    row, col = lax.axis_index("row"), lax.axis_index("col")
    first_row, last_row = row == 0, row == lax.axis_size("row") - 1
    first_col, last_col = col == 0, col == lax.axis_size("col") - 1
    even = lax.rem(col, 2) == 0

    def put(line, place, values, outside):
        start = EDGE + LEAD + line * slot + place
        values = values.astype(jnp.float32)
        if outside is not None:
            values = jnp.where(outside, FAR, values)
        cells[start : start + values.shape[0], :] = values

    cells[...] = jnp.full(cells.shape, FAR, jnp.float32)
    for line in range(height):
        put(line + HALO, 0, marked[line], None)
    for line in range(HALO):
        put(line, 0, top[line], first_row)
        put(height + HALO + line, 0, bottom[line], last_row)
    for line in range(height + 2 * HALO):
        beyond_left, beyond_right = first_col, last_col
        if line < HALO:
            beyond_left, beyond_right = first_col | first_row, last_col | first_row
        if line >= height + HALO:
            beyond_left, beyond_right = first_col | last_row, last_col | last_row
        one, two = paired[line].astype(jnp.float32), crossed[line].astype(jnp.float32)
        put(line, -HALO, jnp.where(even, two, one), beyond_left)
        put(line, breadth, jnp.where(even, one, two), beyond_right)

    for shift in range(3):
        values = cells[EDGE - 1 + shift : EDGE - 1 + shift + flat, :]
        taps[:, shift * channels : (shift + 1) * channels] = jnp.where(
            values < FAR, values, 0.0
        ).astype(jnp.bfloat16)

    count = flat - 2 * slot
    summed = jnp.dot(taps[0:count, :], first[0], preferred_element_type=jnp.float32)
    for line in range(1, 3):
        summed = summed + jnp.dot(
            taps[line * slot : line * slot + count, :], first[line],
            preferred_element_type=jnp.float32,
        )
    alive = cells[EDGE + slot : EDGE + slot + count, :] < FAR
    edge = jnp.zeros((EDGE, channels), jnp.float32)
    mid[0:EDGE, :] = edge
    mid[EDGE + count : 2 * EDGE + count, :] = edge
    mid[EDGE : EDGE + count, :] = jnp.where(alive, gelu(summed + bias_first[...]), 0.0)
    later.wait()


def second_conv_kernel(marked, mid, second, bias_second, out, sent, taps):
    height, breadth, channels = marked.shape
    count = mid.shape[0] - 2 * EDGE
    slot = (count - LEAD) // (height + 2)
    for shift in range(3):
        taps[0:count, shift * channels : (shift + 1) * channels] = mid[
            EDGE - 1 + shift : EDGE - 1 + shift + count, :
        ].astype(jnp.bfloat16)
    inner = height * slot
    summed = jnp.dot(taps[LEAD : LEAD + inner, :], second[0], preferred_element_type=jnp.float32)
    for line in range(1, 3):
        summed = summed + jnp.dot(
            taps[LEAD + line * slot : LEAD + line * slot + inner, :], second[line],
            preferred_element_type=jnp.float32,
        )
    summed = summed.reshape(height, slot, channels)[:, :breadth].reshape(height * breadth, channels)
    alive = marked[...].reshape(height * breadth, channels) < FAR
    value = gelu(summed + bias_second[...])
    out[...] = jnp.where(alive, value, 0.0).astype(jnp.bfloat16)
    sent[...] = jnp.where(alive, value, FAR).astype(jnp.bfloat16)


def key_kernel(cells, weight, keys):
    keys[...] = jnp.dot(cells[...], weight[...], preferred_element_type=jnp.float32).astype(
        jnp.bfloat16
    )


def write_parts(block, values, top, total):
    channels = values.shape[0]
    parts = []
    for source, count in ((top, 3), (total, 2)):
        rest = source
        for _ in range(count):
            part = rest.astype(jnp.bfloat16).astype(jnp.float32)
            parts.append(part)
            rest = rest - part
    parts.append(jnp.zeros((block.shape[0] - channels - 5, values.shape[1]), jnp.float32))
    block[0:channels, :] = values.astype(jnp.bfloat16)
    block[channels:, :] = jnp.concatenate(parts, axis=0).astype(jnp.bfloat16)


def read_parts(block):
    channels = block.shape[0] - 16
    tail = block[channels:, :].astype(jnp.float32)
    row = lambda k: tail[k : k + 1]
    return (
        block[0:channels, :].astype(jnp.float32),
        row(0) + row(1) + row(2),
        row(3) + row(4),
    )


def read_whole(block):
    channels = block.shape[0] - 8
    tail = block[channels:, :]
    return block[0:channels, :], tail[0:1], tail[1:2]


def write_whole(block, values, top, total):
    channels = values.shape[0]
    block[0:channels, :] = values
    block[channels:, :] = jnp.concatenate(
        [top, total, jnp.zeros((6, values.shape[1]), jnp.float32)], axis=0
    )


PLACES = (0, 2, 1, 3)


def hold_queries(held, near, far, use_near):
    half = held.shape[0] // 8
    row = lax.axis_index("row")
    blocks = [
        (one, other, 2 * k * half)
        for one, other in zip(near, far)
        for k in range(one.shape[0] // (2 * half))
    ]
    for (one, other, start), place in zip(blocks, PLACES):
        for parity in range(2):
            source = slice(start + parity * half, start + (parity + 1) * half)
            target = pl.multiple_of(parity * 4 * half + (row ^ place) * half, half)
            held[pl.ds(target, half), :] = jnp.where(use_near, one[source, :], other[source, :])


def masked_scores(queries, marked, keys):
    scale = 1.0 / math.sqrt(queries.shape[1])
    raw = lax.dot_general(
        keys[...], queries[...], (((1,), (1,)), ((), ())), preferred_element_type=jnp.float32
    )
    return jnp.where(marked[:, : raw.shape[1]] < FAR, raw * scale, -1e30)


def score_blocks(scores, sides):
    top = jnp.maximum(*[jnp.max(part, axis=0, keepdims=True) for part in scores])
    pooled = total = 0.0
    for part, cells in zip(scores, sides):
        chosen = jnp.exp(part - top)
        total = total + jnp.sum(chosen, axis=0, keepdims=True)
        pooled = pooled + lax.dot_general(
            cells[...], chosen.astype(jnp.bfloat16), (((0,), (0,)), ((), ())),
            preferred_element_type=jnp.float32,
        )
    channels, lanes = pooled.shape[0] // 2, pooled.shape[1]
    turn = lambda array: pltpu.roll(array, lanes // 2, 1)
    lower = lambda rows: lax.broadcasted_iota(jnp.int32, (rows, lanes), 1) < lanes // 2
    tall, flat = lower(channels), lower(1)
    turned, turned_top, turned_total = turn(pooled), turn(top), turn(total)
    return (
        (
            jnp.where(tall, pooled[:channels], turned[channels:]),
            jnp.where(flat, top, turned_top),
            jnp.where(flat, total, turned_total),
        ),
        (
            jnp.where(tall, turned[:channels], pooled[channels:]),
            jnp.where(flat, turned_top, top),
            jnp.where(flat, turned_total, total),
        ),
    )


def first_score_kernel(own, own_sent, own_keys, other_sent, weight, *refs):
    *queries, send_2, send_3, other, keys, held, blocks = refs
    row, across = lax.axis_index("row"), lax.axis_index("col") // 2
    hold_queries(held, queries[:3], queries[3:], row // 2 != across)
    values = other_sent[...].astype(jnp.float32)
    other[...] = jnp.where(values < FAR, values, 0.0).astype(jnp.bfloat16)
    key_kernel(other, weight, keys)
    scores = masked_scores(held, own_sent, own_keys), masked_scores(held, other_sent, keys)
    for parity, block in enumerate(score_blocks(scores, (own, other))):
        write_whole(blocks.at[parity], *block)
    odd = lax.rem(row, 2)
    write_parts(send_2, *read_whole(blocks.at[odd]))
    write_parts(send_3, *read_whole(blocks.at[1 - odd]))


def last_score_kernel(own, own_sent, own_keys, other, other_sent, other_keys, *refs):
    *queries, kept, send_1, held, blocks = refs
    row, across = lax.axis_index("row"), lax.axis_index("col") // 2
    hold_queries(held, queries[:3], queries[3:], row // 2 == across)
    scores = masked_scores(held, own_sent, own_keys), masked_scores(held, other_sent, other_keys)
    for parity, block in enumerate(score_blocks(scores, (own, other))):
        write_whole(blocks.at[parity], *block)
    odd = lax.rem(row, 2)
    kept[...] = blocks[odd]
    write_parts(send_1, *read_whole(blocks.at[1 - odd]))


def merge_kernel(own, *refs):
    *arrived, whole, packed_out = refs
    values, top, total = merged([read_whole(own)] + [read_parts(block) for block in arrived])
    write_whole(whole, values, top, total)
    write_parts(packed_out, values, top, total)


def normalize_kernel(own, arrived, out):
    values, _, total = merged([read_whole(own), read_parts(arrived)])
    out[...] = (values / total).astype(jnp.bfloat16)


def attend_kernel(normalized, value_weight, attended):
    lanes = normalized.shape[1] // 2
    values = normalized[...].astype(jnp.float32)
    tall = jnp.concatenate([values, pltpu.roll(values, lanes, 1)], axis=0).astype(jnp.bfloat16)
    attended[...] = lax.dot_general(
        tall, value_weight[...], (((0,), (0,)), ((), ())), preferred_element_type=jnp.float32
    )[:lanes].astype(jnp.bfloat16)


def finish_kernel(mine, arrived, value_weight, out_weight, out, other, attended):
    attend_kernel(arrived, value_weight, other)
    core = lax.rem(lax.axis_index("col"), 2)
    piece = mine.shape[0] // 4
    for place in range(4):
        source = slice(place * piece, (place + 1) * piece)
        first = pl.multiple_of((2 * place + core) * piece, piece)
        last = pl.multiple_of((2 * place + 1 - core) * piece, piece)
        attended[pl.ds(first, piece), :] = mine[source]
        attended[pl.ds(last, piece), :] = other[source]
    out[...] = lax.dot_general(
        out_weight[...], attended[...], (((1,), (1,)), ((), ())),
        preferred_element_type=jnp.float32,
    ).astype(out.dtype)


MIB = 1 << 20


def call(kernel, outs, args, scratch=(), limit=4, flops=0, far=()):
    held = pl.BlockSpec(memory_space=pltpu.VMEM)
    outside = pl.BlockSpec(memory_space=pltpu.HBM)
    return pl.pallas_call(
        kernel,
        out_shape=[pltpu.VMEM(shape, dtype) for shape, dtype in outs],
        in_specs=[outside if k in far else held for k in range(len(args))],
        out_specs=[held] * len(outs),
        scratch_shapes=[pltpu.VMEM(*kind) if isinstance(kind, tuple) else kind for kind in scratch],
        compiler_params=pltpu.CompilerParams(vmem_limit_bytes=limit * MIB),
        cost_estimate=pl.CostEstimate(flops=flops, bytes_accessed=0, transcendentals=0),
    )(
        *[
            pltpu.with_memory_space_constraint(arg, pltpu.HBM if k in far else pltpu.VMEM)
            for k, arg in enumerate(args)
        ]
    )


def kernel_path(
    features, tissue, conv_first, bias_first, conv_second, bias_second, key_weight,
    value_weight, latent_queries, out_weight,
):
    height, breadth, channels = features.shape
    col, cols = lax.axis_index("col"), lax.axis_size("col")
    size, width = latent_queries.shape
    cells = height * breadth
    slot = -(-(breadth + 2 * HALO) // 16) * 16
    flat = LEAD + (height + 2 * HALO) * slot
    count = flat - 2 * slot
    wide, half = jnp.float32, jnp.bfloat16
    block = 4 * size
    whole_block, sent_block = (channels // 2 + 8, block), (channels // 2 + 16, block)
    score_flops = 4 * cells * block * (width + channels)

    beside = flipped(latent_queries, "col", 1)
    marked, queries = call(
        mark_kernel, [(features.shape, half), ((size, width), half)],
        [features, tissue, latent_queries],
        [(features.shape, half), (tissue.shape, jnp.int32), pltpu.SemaphoreType.DMA((3,))],
        far=(0, 1, 2), flops=1 << 20,
    )
    (queries,) = call(halve_kernel, [((size, width), half)], [queries, beside])
    two = flipped(queries, "row", 2)
    top = shifted(marked[height - HALO :], "row", 1)
    bottom = shifted(marked[:HALO], "row", -1)
    one = flipped(queries, "row", 1)
    three = flipped(queries, "row", 3)
    far_queries = flipped(queries, "col", 2)

    edge = lambda cut: jnp.concatenate([top[:, cut], marked[:, cut], bottom[:, cut]], axis=0)
    even = lax.rem(col, 2) == 0
    ends = edge(slice(breadth - HALO, breadth)), edge(slice(0, HALO))
    paired = flipped(jnp.where(even, *ends), "col", 1)
    rounds = [(k, (k + 1 if k % 2 else k - 1) % cols) for k in range(cols)]
    crossed = lax.ppermute(jnp.where(even, *ends[::-1]), "col", rounds)

    pair = jnp.concatenate([two, one], axis=0)
    far_pair = flipped(pair, "col", 2)
    far_three = flipped(three, "col", 2)

    mid, weight = call(
        conv_kernel,
        [((count + 2 * EDGE, channels), wide), ((3, 3 * channels, channels), half)],
        [
            marked, top, bottom, paired, crossed,
            conv_first.reshape(3, 3 * channels, channels), bias_first.reshape(1, channels),
            conv_second.reshape(3, 3 * channels, channels),
        ],
        [
            ((flat + 2 * EDGE, channels), wide),
            ((flat, 3 * channels), half),
            pltpu.SemaphoreType.DMA,
        ],
        limit=12, far=(7,), flops=21 * cells * channels * channels,
    )
    own, own_sent = call(
        second_conv_kernel, [((cells, channels), half)] * 2,
        [marked, mid, weight, bias_second.reshape(1, channels)],
        [((count, 3 * channels), half)],
        limit=10, flops=18 * cells * channels * channels,
    )
    other_sent = flipped(own_sent, "col", 1)
    (own_keys,) = call(
        key_kernel, [((cells, width), half)], [own, key_weight],
        limit=4, flops=2 * cells * width * channels,
    )
    all_queries = [queries, pair, three, far_queries, far_pair, far_three]
    score_scratch = [((block, width), half), ((2,) + whole_block, wide)]
    send_2, send_3, other, other_keys = call(
        first_score_kernel,
        [(sent_block, half)] * 2 + [((cells, channels), half), ((cells, width), half)],
        [own, own_sent, own_keys, other_sent, key_weight, *all_queries],
        score_scratch, limit=8, flops=score_flops + 2 * cells * channels * width,
    )
    arrived_2, arrived_3 = flipped(send_2, "row", 2), flipped(send_3, "row", 3)
    kept, send_1 = call(
        last_score_kernel, [(whole_block, wide), (sent_block, half)],
        [own, own_sent, own_keys, other, other_sent, other_keys, *all_queries],
        score_scratch, limit=8, flops=score_flops,
    )
    arrived_1 = flipped(send_1, "row", 1)
    kept, sent = call(
        merge_kernel, [(whole_block, wide), (sent_block, half)],
        [kept, arrived_1, arrived_2, arrived_3],
    )
    arrived = flipped(sent, "col", 2)
    (normalized,) = call(normalize_kernel, [((channels // 2, block), half)], [kept, arrived])
    arrived = flipped(normalized, "col", 1)
    (attended,) = call(
        attend_kernel, [((2 * size, width), half)], [normalized, value_weight],
        flops=8 * size * channels * width,
    )
    held = pl.BlockSpec(memory_space=pltpu.VMEM)
    keep = lambda array: pltpu.with_memory_space_constraint(array, pltpu.VMEM)
    return pl.pallas_call(
        finish_kernel,
        out_shape=jax.ShapeDtypeStruct((out_weight.shape[1], block), half),
        in_specs=[held] * 4,
        out_specs=held,
        scratch_shapes=[pltpu.VMEM((2 * size, width), half), pltpu.VMEM((block, width), half)],
        compiler_params=pltpu.CompilerParams(vmem_limit_bytes=6 * MIB),
        name="fn",
    )(keep(attended), keep(arrived), keep(value_weight), keep(out_weight.T)).T


def shards(
    features, tissue, conv_first, bias_first, conv_second, bias_second, key_weight,
    value_weight, latent_queries, out_weight,
):
    rows, cols = lax.axis_size("row"), lax.axis_size("col")
    if rows == cols == 4 and rows * latent_queries.shape[0] == 128:
        return kernel_path(
            features, tissue, conv_first, bias_first, conv_second, bias_second, key_weight,
            value_weight, latent_queries, out_weight,
        )
    marked = jnp.where(tissue[:, :, None] > 0, features, jnp.asarray(FAR, features.dtype))
    marked = with_halo(with_halo(marked, "row", 0), "col", 1)
    normalized = plain_attend(
        features, tissue, marked, latent_queries,
        (conv_first, bias_first, conv_second, bias_second, key_weight),
    )
    attended = lax.dot_general(
        normalized, value_weight, (((0,), (0,)), ((), ())), preferred_element_type=jnp.float32
    ).astype(jnp.bfloat16)
    return jnp.dot(attended, out_weight, preferred_element_type=jnp.float32).astype(jnp.bfloat16)


def solution(mesh):
    placed = (
        P(("groups", "row"), "col", None),
        P(("groups", "row"), "col"),
        P(),
        P(),
        P(),
        P(),
        P(),
        P(),
        P(("col", "row"), None),
        P(None, "col"),
    )
    return jax.shard_map(
        shards, mesh=mesh, in_specs=placed, out_specs=P(("groups", "row"), "col"), check_vma=False
    )
```

```python
import math

import jax
import jax.numpy as jnp
from jax import lax
from jax.experimental import pallas as pl
from jax.experimental.pallas import tpu as pltpu
from jax.sharding import PartitionSpec as P


HALO = 2
FAR = float("inf")
EDGE = 8
LEAD = 16


def shifted(array, axis, step):
    count = lax.axis_size(axis)
    return lax.ppermute(array, axis, [(i, (i + step) % count) for i in range(count)])


def flipped(array, axis, bit):
    count = lax.axis_size(axis)
    return lax.ppermute(array, axis, [(i, i ^ bit) for i in range(count)])


def with_halo(cells, axis, dim):
    size = cells.shape[dim]
    index, last = lax.axis_index(axis), lax.axis_size(axis) - 1
    before = shifted(lax.slice_in_dim(cells, size - HALO, size, axis=dim), axis, 1)
    after = shifted(lax.slice_in_dim(cells, 0, HALO, axis=dim), axis, -1)
    far = jnp.asarray(FAR, cells.dtype)
    return jnp.concatenate(
        [jnp.where(index == 0, far, before), cells, jnp.where(index == last, far, after)], axis=dim
    )


def convolve_valid(padded, weight):
    height, breadth = padded.shape[0] - 2, padded.shape[1] - 2
    channels = padded.shape[2]
    summed = jnp.zeros((height * breadth, weight.shape[3]), jnp.float32)
    for offset_row in range(3):
        for offset_col in range(3):
            window = padded[offset_row : offset_row + height, offset_col : offset_col + breadth]
            summed = summed + jnp.dot(
                window.reshape(height * breadth, channels),
                weight[offset_row, offset_col],
                preferred_element_type=jnp.float32,
            )
    return summed.reshape(height, breadth, weight.shape[3])


def rotated(parts, offset, step):
    count = len(parts)
    size = parts[0].shape[0]
    ordered = [parts[(step * k) % count] for k in range(count)]
    twice = jnp.concatenate(ordered + ordered[:-1], axis=0)
    return lax.dynamic_slice_in_dim(twice, ((count - offset) % count) * size, count * size, axis=0)


def gathered_queries(latent_queries):
    rows, cols = lax.axis_size("row"), lax.axis_size("col")
    parts = [latent_queries] + [shifted(latent_queries, "row", k) for k in range(1, rows)]
    queries = rotated(parts, lax.axis_index("row"), -1)
    own = lax.axis_index("col")
    bit = cols // 2
    groups = [queries]
    order = [0]
    while bit > 0:
        groups = groups + list(flipped(jnp.concatenate(groups, axis=0), "col", bit).reshape(len(groups), -1, queries.shape[1]))
        order = order + [place ^ bit for place in order]
        bit //= 2
    stacked = jnp.stack(groups)
    place = jnp.asarray([order.index(k) for k in range(cols)], jnp.int32)
    return stacked[place[own ^ jnp.arange(cols)]].reshape(-1, queries.shape[1])


def in_parts(values, count):
    parts = []
    for _ in range(count):
        part = lax.reduce_precision(values, exponent_bits=8, mantissa_bits=7)
        parts.append(part.astype(jnp.bfloat16))
        values = values - part
    return parts


def packed(pooled, top, total):
    rest = jnp.zeros((11, pooled.shape[1]), jnp.bfloat16)
    return jnp.concatenate(
        [pooled.astype(jnp.bfloat16)] + in_parts(top, 3) + in_parts(total, 2) + [rest], axis=0
    )


def unpacked(block, channels):
    wide = block.astype(jnp.float32)
    row = lambda k: wide[channels + k : channels + k + 1]
    return wide[:channels], row(0) + row(1) + row(2), row(3) + row(4)


def merged(partials):
    top = partials[0][1]
    for _, other, _ in partials[1:]:
        top = jnp.maximum(top, other)
    pooled = total = 0.0
    for part, shift, count in partials:
        factor = jnp.exp(shift - top)
        pooled = pooled + part * factor
        total = total + count * factor
    return pooled, top, total


def plain_attend(features, tissue, marked, latent_queries, weights):
    conv_first, bias_first, conv_second, bias_second, key_weight = weights
    height, breadth, channels = features.shape
    rows = lax.axis_size("row")
    queries = gathered_queries(latent_queries)
    alive = marked < FAR
    inputs = jnp.where(alive, marked, jnp.zeros_like(marked))
    hidden = jax.nn.gelu(convolve_valid(inputs, conv_first) + bias_first, approximate=False)
    hidden = jnp.where(alive[1:-1, 1:-1], hidden, 0.0).astype(jnp.bfloat16)
    second = jax.nn.gelu(convolve_valid(hidden, conv_second) + bias_second, approximate=False)
    second = jnp.where(alive[HALO:-HALO, HALO:-HALO], second, 0.0).astype(jnp.bfloat16)
    flattened = second.reshape(height * breadth, channels)
    key_rows = jnp.dot(flattened, key_weight, preferred_element_type=jnp.float32).astype(
        jnp.bfloat16
    )
    scale = 1.0 / math.sqrt(latent_queries.shape[1])
    scores = (
        lax.dot_general(
            key_rows, queries, (((1,), (1,)), ((), ())), preferred_element_type=jnp.float32
        )
        * scale
    )
    scores = jnp.where(tissue.reshape(-1, 1) > 0, scores, -1e30)
    shift = jnp.max(scores, axis=0, keepdims=True)
    chosen = jnp.exp(scores - shift)
    total = jnp.sum(chosen, axis=0, keepdims=True)
    pooled = lax.dot_general(
        flattened,
        chosen.astype(jnp.bfloat16),
        (((0,), (0,)), ((), ())),
        preferred_element_type=jnp.float32,
    )

    own_row = lax.axis_index("row")
    size = pooled.shape[1] // rows

    def block_of(step):
        start = ((own_row + step) % rows) * size
        cut = lambda array: lax.dynamic_slice_in_dim(array, start, size, axis=1)
        return cut(pooled), cut(shift), cut(total)

    arrived = [shifted(packed(*block_of(k)), "row", k) for k in range(1, rows)]
    partial = merged([block_of(0)] + [unpacked(block, channels) for block in arrived])
    bit = lax.axis_size("col") // 2
    while bit > 0:
        other = flipped(packed(*partial), "col", bit)
        partial = merged([partial, unpacked(other, channels)])
        bit //= 2
    normalized = (partial[0] / partial[2]).astype(jnp.bfloat16)
    return normalized


def gelu(value):
    return 0.5 * value * (1.0 + lax.erf(value * math.sqrt(0.5)))


def mark_kernel(features, tissue, queries, out, queries_out, features_held, tissue_held, done):
    copies = [
        pltpu.make_async_copy(tissue, tissue_held, done.at[0]),
        pltpu.make_async_copy(features, features_held, done.at[1]),
        pltpu.make_async_copy(queries, queries_out, done.at[2]),
    ]
    for copy in copies:
        copy.start()
    height, breadth, channels = features.shape
    copies[0].wait()
    line = lax.broadcasted_iota(jnp.int32, (breadth, breadth), 0)
    place = lax.broadcasted_iota(jnp.int32, (breadth, breadth), 1)
    flags = tissue_held[...].astype(jnp.float32)
    spread = [
        jnp.where(line == place, jnp.broadcast_to(flags[k : k + 1], line.shape), 0.0)
        for k in range(height)
    ]
    keep = jnp.dot(
        jnp.concatenate(spread, axis=0).astype(jnp.bfloat16),
        jnp.ones((breadth, channels), jnp.bfloat16),
        preferred_element_type=jnp.float32,
    )
    copies[1].wait()
    for k in range(height):
        out[k] = jnp.where(
            keep[k * breadth : (k + 1) * breadth] > 0.0, features_held[k].astype(jnp.float32), FAR
        ).astype(jnp.bfloat16)
    copies[2].wait()


def halve_kernel(own, other, out):
    half = own.shape[0] // 2
    core = lax.rem(lax.axis_index("col"), 2)
    start = pl.multiple_of(core * half, half)
    out[pl.ds(start, half), :] = own[pl.ds(start, half), :]
    out[pl.ds(pl.multiple_of((1 - core) * half, half), half), :] = other[pl.ds(start, half), :]


def conv_kernel(
    marked, top, bottom, paired, crossed, first, bias_first, second,
    mid, second_held, cells, taps, done,
):
    later = pltpu.make_async_copy(second, second_held, done)
    later.start()
    height, breadth, channels = marked.shape
    slot = (cells.shape[0] - 2 * EDGE - LEAD) // (height + 2 * HALO)
    flat = cells.shape[0] - 2 * EDGE
    row, col = lax.axis_index("row"), lax.axis_index("col")
    first_row, last_row = row == 0, row == lax.axis_size("row") - 1
    first_col, last_col = col == 0, col == lax.axis_size("col") - 1
    even = lax.rem(col, 2) == 0

    def put(line, place, values, outside):
        start = EDGE + LEAD + line * slot + place
        values = values.astype(jnp.float32)
        if outside is not None:
            values = jnp.where(outside, FAR, values)
        cells[start : start + values.shape[0], :] = values

    cells[...] = jnp.full(cells.shape, FAR, jnp.float32)
    for line in range(height):
        put(line + HALO, 0, marked[line], None)
    for line in range(HALO):
        put(line, 0, top[line], first_row)
        put(height + HALO + line, 0, bottom[line], last_row)
    for line in range(height + 2 * HALO):
        beyond_left, beyond_right = first_col, last_col
        if line < HALO:
            beyond_left, beyond_right = first_col | first_row, last_col | first_row
        if line >= height + HALO:
            beyond_left, beyond_right = first_col | last_row, last_col | last_row
        one, two = paired[line].astype(jnp.float32), crossed[line].astype(jnp.float32)
        put(line, -HALO, jnp.where(even, two, one), beyond_left)
        put(line, breadth, jnp.where(even, one, two), beyond_right)

    for shift in range(3):
        values = cells[EDGE - 1 + shift : EDGE - 1 + shift + flat, :]
        taps[:, shift * channels : (shift + 1) * channels] = jnp.where(
            values < FAR, values, 0.0
        ).astype(jnp.bfloat16)

    count = flat - 2 * slot
    summed = jnp.dot(taps[0:count, :], first[0], preferred_element_type=jnp.float32)
    for line in range(1, 3):
        summed = summed + jnp.dot(
            taps[line * slot : line * slot + count, :], first[line],
            preferred_element_type=jnp.float32,
        )
    alive = cells[EDGE + slot : EDGE + slot + count, :] < FAR
    edge = jnp.zeros((EDGE, channels), jnp.float32)
    mid[0:EDGE, :] = edge
    mid[EDGE + count : 2 * EDGE + count, :] = edge
    mid[EDGE : EDGE + count, :] = jnp.where(alive, gelu(summed + bias_first[...]), 0.0)
    later.wait()


def second_conv_kernel(marked, mid, second, bias_second, out, sent, taps):
    height, breadth, channels = marked.shape
    count = mid.shape[0] - 2 * EDGE
    slot = (count - LEAD) // (height + 2)
    for shift in range(3):
        taps[0:count, shift * channels : (shift + 1) * channels] = mid[
            EDGE - 1 + shift : EDGE - 1 + shift + count, :
        ].astype(jnp.bfloat16)
    inner = height * slot
    summed = jnp.dot(taps[LEAD : LEAD + inner, :], second[0], preferred_element_type=jnp.float32)
    for line in range(1, 3):
        summed = summed + jnp.dot(
            taps[LEAD + line * slot : LEAD + line * slot + inner, :], second[line],
            preferred_element_type=jnp.float32,
        )
    summed = summed.reshape(height, slot, channels)[:, :breadth].reshape(height * breadth, channels)
    alive = marked[...].reshape(height * breadth, channels) < FAR
    value = gelu(summed + bias_second[...])
    out[...] = jnp.where(alive, value, 0.0).astype(jnp.bfloat16)
    sent[...] = jnp.where(alive, value, FAR).astype(jnp.bfloat16)


def key_kernel(cells, weight, keys):
    keys[...] = jnp.dot(cells[...], weight[...], preferred_element_type=jnp.float32).astype(
        jnp.bfloat16
    )


def write_parts(block, values, top, total):
    channels = values.shape[0]
    parts = []
    for source, count in ((top, 3), (total, 2)):
        rest = source
        for _ in range(count):
            part = rest.astype(jnp.bfloat16).astype(jnp.float32)
            parts.append(part)
            rest = rest - part
    parts.append(jnp.zeros((block.shape[0] - channels - 5, values.shape[1]), jnp.float32))
    block[0:channels, :] = values.astype(jnp.bfloat16)
    block[channels:, :] = jnp.concatenate(parts, axis=0).astype(jnp.bfloat16)


def read_parts(block):
    channels = block.shape[0] - 16
    tail = block[channels:, :].astype(jnp.float32)
    row = lambda k: tail[k : k + 1]
    return (
        block[0:channels, :].astype(jnp.float32),
        row(0) + row(1) + row(2),
        row(3) + row(4),
    )


def read_whole(block):
    channels = block.shape[0] - 8
    tail = block[channels:, :]
    return block[0:channels, :], tail[0:1], tail[1:2]


def write_whole(block, values, top, total):
    channels = values.shape[0]
    block[0:channels, :] = values
    block[channels:, :] = jnp.concatenate(
        [top, total, jnp.zeros((6, values.shape[1]), jnp.float32)], axis=0
    )


PLACES = (0, 2, 1, 3)


def hold_queries(held, near, far, use_near):
    half = held.shape[0] // 8
    row = lax.axis_index("row")
    blocks = [
        (one, other, 2 * k * half)
        for one, other in zip(near, far)
        for k in range(one.shape[0] // (2 * half))
    ]
    for (one, other, start), place in zip(blocks, PLACES):
        for parity in range(2):
            source = slice(start + parity * half, start + (parity + 1) * half)
            target = pl.multiple_of(parity * 4 * half + (row ^ place) * half, half)
            held[pl.ds(target, half), :] = jnp.where(use_near, one[source, :], other[source, :])


def masked_scores(queries, marked, keys):
    scale = 1.0 / math.sqrt(queries.shape[1])
    raw = lax.dot_general(
        keys[...], queries[...], (((1,), (1,)), ((), ())), preferred_element_type=jnp.float32
    )
    return jnp.where(marked[:, : raw.shape[1]] < FAR, raw * scale, -1e30)


def score_blocks(scores, sides):
    top = jnp.maximum(*[jnp.max(part, axis=0, keepdims=True) for part in scores])
    pooled = total = 0.0
    for part, cells in zip(scores, sides):
        chosen = jnp.exp(part - top)
        total = total + jnp.sum(chosen, axis=0, keepdims=True)
        pooled = pooled + lax.dot_general(
            cells[...], chosen.astype(jnp.bfloat16), (((0,), (0,)), ((), ())),
            preferred_element_type=jnp.float32,
        )
    channels, lanes = pooled.shape[0] // 2, pooled.shape[1]
    turn = lambda array: pltpu.roll(array, lanes // 2, 1)
    lower = lambda rows: lax.broadcasted_iota(jnp.int32, (rows, lanes), 1) < lanes // 2
    tall, flat = lower(channels), lower(1)
    turned, turned_top, turned_total = turn(pooled), turn(top), turn(total)
    return (
        (
            jnp.where(tall, pooled[:channels], turned[channels:]),
            jnp.where(flat, top, turned_top),
            jnp.where(flat, total, turned_total),
        ),
        (
            jnp.where(tall, turned[:channels], pooled[channels:]),
            jnp.where(flat, turned_top, top),
            jnp.where(flat, turned_total, total),
        ),
    )


def other_kernel(other_sent, weight, other, keys):
    values = other_sent[...].astype(jnp.float32)
    other[...] = jnp.where(values < FAR, values, 0.0).astype(jnp.bfloat16)
    key_kernel(other, weight, keys)


def first_score_kernel(own, own_sent, own_keys, other, other_sent, other_keys, *refs):
    *queries, send_2, send_3, held, blocks = refs
    row, across = lax.axis_index("row"), lax.axis_index("col") // 2
    hold_queries(held, queries[:2], queries[2:], row // 2 != across)
    scores = masked_scores(held, own_sent, own_keys), masked_scores(held, other_sent, other_keys)
    for parity, block in enumerate(score_blocks(scores, (own, other))):
        write_whole(blocks.at[parity], *block)
    odd = lax.rem(row, 2)
    write_parts(send_2, *read_whole(blocks.at[odd]))
    write_parts(send_3, *read_whole(blocks.at[1 - odd]))


def last_score_kernel(own, own_sent, own_keys, other, other_sent, other_keys, *refs):
    *queries, kept, send_1, held, blocks = refs
    row, across = lax.axis_index("row"), lax.axis_index("col") // 2
    hold_queries(held, queries[:2], queries[2:], row // 2 == across)
    scores = masked_scores(held, own_sent, own_keys), masked_scores(held, other_sent, other_keys)
    for parity, block in enumerate(score_blocks(scores, (own, other))):
        write_whole(blocks.at[parity], *block)
    odd = lax.rem(row, 2)
    kept[...] = blocks[odd]
    write_parts(send_1, *read_whole(blocks.at[1 - odd]))


def merge_kernel(own, *refs):
    *arrived, whole, packed_out = refs
    values, top, total = merged([read_whole(own)] + [read_parts(block) for block in arrived])
    write_whole(whole, values, top, total)
    write_parts(packed_out, values, top, total)


def normalize_kernel(own, arrived, out):
    values, _, total = merged([read_whole(own), read_parts(arrived)])
    out[...] = (values / total).astype(jnp.bfloat16)


def attend_kernel(normalized, value_weight, attended):
    lanes = normalized.shape[1] // 2
    values = normalized[...].astype(jnp.float32)
    tall = jnp.concatenate([values, pltpu.roll(values, lanes, 1)], axis=0).astype(jnp.bfloat16)
    attended[...] = lax.dot_general(
        tall, value_weight[...], (((0,), (0,)), ((), ())), preferred_element_type=jnp.float32
    )[:lanes].astype(jnp.bfloat16)


def finish_kernel(mine, arrived, value_weight, out_weight, out, other, attended):
    attend_kernel(arrived, value_weight, other)
    core = lax.rem(lax.axis_index("col"), 2)
    piece = mine.shape[0] // 4
    for place in range(4):
        source = slice(place * piece, (place + 1) * piece)
        first = pl.multiple_of((2 * place + core) * piece, piece)
        last = pl.multiple_of((2 * place + 1 - core) * piece, piece)
        attended[pl.ds(first, piece), :] = mine[source]
        attended[pl.ds(last, piece), :] = other[source]
    out[...] = lax.dot_general(
        out_weight[...], attended[...], (((1,), (1,)), ((), ())),
        preferred_element_type=jnp.float32,
    ).astype(out.dtype)


MIB = 1 << 20


def call(kernel, outs, args, scratch=(), limit=4, flops=0, far=()):
    held = pl.BlockSpec(memory_space=pltpu.VMEM)
    outside = pl.BlockSpec(memory_space=pltpu.HBM)
    return pl.pallas_call(
        kernel,
        out_shape=[pltpu.VMEM(shape, dtype) for shape, dtype in outs],
        in_specs=[outside if k in far else held for k in range(len(args))],
        out_specs=[held] * len(outs),
        scratch_shapes=[pltpu.VMEM(*kind) if isinstance(kind, tuple) else kind for kind in scratch],
        compiler_params=pltpu.CompilerParams(vmem_limit_bytes=limit * MIB),
        cost_estimate=pl.CostEstimate(flops=flops, bytes_accessed=0, transcendentals=0),
    )(
        *[
            pltpu.with_memory_space_constraint(arg, pltpu.HBM if k in far else pltpu.VMEM)
            for k, arg in enumerate(args)
        ]
    )


def kernel_path(
    features, tissue, conv_first, bias_first, conv_second, bias_second, key_weight,
    value_weight, latent_queries, out_weight,
):
    height, breadth, channels = features.shape
    col, cols = lax.axis_index("col"), lax.axis_size("col")
    size, width = latent_queries.shape
    cells = height * breadth
    slot = -(-(breadth + 2 * HALO) // 16) * 16
    flat = LEAD + (height + 2 * HALO) * slot
    count = flat - 2 * slot
    wide, half = jnp.float32, jnp.bfloat16
    block = 4 * size
    whole_block, sent_block = (channels // 2 + 8, block), (channels // 2 + 16, block)
    score_flops = 4 * cells * block * (width + channels)

    beside = flipped(latent_queries, "col", 1)
    marked, queries = call(
        mark_kernel, [(features.shape, half), ((size, width), half)],
        [features, tissue, latent_queries],
        [(features.shape, half), (tissue.shape, jnp.int32), pltpu.SemaphoreType.DMA((3,))],
        far=(0, 1, 2), flops=1 << 20,
    )
    (queries,) = call(halve_kernel, [((size, width), half)], [queries, beside])
    two = flipped(queries, "row", 2)
    top = shifted(marked[height - HALO :], "row", 1)
    bottom = shifted(marked[:HALO], "row", -1)
    one = flipped(queries, "row", 1)
    three = flipped(queries, "row", 3)

    edge = lambda cut: jnp.concatenate([top[:, cut], marked[:, cut], bottom[:, cut]], axis=0)
    even = lax.rem(col, 2) == 0
    ends = edge(slice(breadth - HALO, breadth)), edge(slice(0, HALO))
    paired = flipped(jnp.where(even, *ends), "col", 1)
    rounds = [(k, (k + 1 if k % 2 else k - 1) % cols) for k in range(cols)]
    crossed = lax.ppermute(jnp.where(even, *ends[::-1]), "col", rounds)

    trio = jnp.concatenate([queries, two, one], axis=0)
    far_trio = flipped(trio, "col", 2)
    far_three = flipped(three, "col", 2)

    mid, weight = call(
        conv_kernel,
        [((count + 2 * EDGE, channels), wide), ((3, 3 * channels, channels), half)],
        [
            marked, top, bottom, paired, crossed,
            conv_first.reshape(3, 3 * channels, channels), bias_first.reshape(1, channels),
            conv_second.reshape(3, 3 * channels, channels),
        ],
        [
            ((flat + 2 * EDGE, channels), wide),
            ((flat, 3 * channels), half),
            pltpu.SemaphoreType.DMA,
        ],
        limit=12, far=(7,), flops=21 * cells * channels * channels,
    )
    own, own_sent = call(
        second_conv_kernel, [((cells, channels), half)] * 2,
        [marked, mid, weight, bias_second.reshape(1, channels)],
        [((count, 3 * channels), half)],
        limit=10, flops=18 * cells * channels * channels,
    )
    other_sent = flipped(own_sent, "col", 1)
    (own_keys,) = call(
        key_kernel, [((cells, width), half)], [own, key_weight],
        limit=4, flops=2 * cells * width * channels,
    )
    all_queries = [trio, three, far_trio, far_three]
    score_scratch = [((block, width), half), ((2,) + whole_block, wide)]
    other, other_keys = call(
        other_kernel, [((cells, channels), half), ((cells, width), half)],
        [other_sent, key_weight], limit=4, flops=2 * cells * channels * width,
    )
    send_2, send_3 = call(
        first_score_kernel, [(sent_block, half)] * 2,
        [own, own_sent, own_keys, other, other_sent, other_keys, *all_queries],
        score_scratch, limit=8, flops=score_flops,
    )
    arrived_2, arrived_3 = flipped(send_2, "row", 2), flipped(send_3, "row", 3)
    kept, send_1 = call(
        last_score_kernel, [(whole_block, wide), (sent_block, half)],
        [own, own_sent, own_keys, other, other_sent, other_keys, *all_queries],
        score_scratch, limit=8, flops=score_flops,
    )
    arrived_1 = flipped(send_1, "row", 1)
    kept, sent = call(
        merge_kernel, [(whole_block, wide), (sent_block, half)],
        [kept, arrived_1, arrived_2, arrived_3],
    )
    arrived = flipped(sent, "col", 2)
    (normalized,) = call(normalize_kernel, [((channels // 2, block), half)], [kept, arrived])
    arrived = flipped(normalized, "col", 1)
    (attended,) = call(
        attend_kernel, [((2 * size, width), half)], [normalized, value_weight],
        flops=8 * size * channels * width,
    )
    held = pl.BlockSpec(memory_space=pltpu.VMEM)
    keep = lambda array: pltpu.with_memory_space_constraint(array, pltpu.VMEM)
    return pl.pallas_call(
        finish_kernel,
        out_shape=jax.ShapeDtypeStruct((out_weight.shape[1], block), half),
        in_specs=[held] * 4,
        out_specs=held,
        scratch_shapes=[pltpu.VMEM((2 * size, width), half), pltpu.VMEM((block, width), half)],
        compiler_params=pltpu.CompilerParams(vmem_limit_bytes=6 * MIB),
        name="fn",
    )(keep(attended), keep(arrived), keep(value_weight), keep(out_weight.T)).T


def shards(
    features, tissue, conv_first, bias_first, conv_second, bias_second, key_weight,
    value_weight, latent_queries, out_weight,
):
    rows, cols = lax.axis_size("row"), lax.axis_size("col")
    if rows == cols == 4 and rows * latent_queries.shape[0] == 128:
        return kernel_path(
            features, tissue, conv_first, bias_first, conv_second, bias_second, key_weight,
            value_weight, latent_queries, out_weight,
        )
    marked = jnp.where(tissue[:, :, None] > 0, features, jnp.asarray(FAR, features.dtype))
    marked = with_halo(with_halo(marked, "row", 0), "col", 1)
    normalized = plain_attend(
        features, tissue, marked, latent_queries,
        (conv_first, bias_first, conv_second, bias_second, key_weight),
    )
    attended = lax.dot_general(
        normalized, value_weight, (((0,), (0,)), ((), ())), preferred_element_type=jnp.float32
    ).astype(jnp.bfloat16)
    return jnp.dot(attended, out_weight, preferred_element_type=jnp.float32).astype(jnp.bfloat16)


def solution(mesh):
    placed = (
        P(("groups", "row"), "col", None),
        P(("groups", "row"), "col"),
        P(),
        P(),
        P(),
        P(),
        P(),
        P(),
        P(("col", "row"), None),
        P(None, "col"),
    )
    return jax.shard_map(
        shards, mesh=mesh, in_specs=placed, out_specs=P(("groups", "row"), "col"), check_vma=False
    )
```

```python
import math

import jax
import jax.numpy as jnp
from jax import lax
from jax.experimental import pallas as pl
from jax.experimental.pallas import tpu as pltpu
from jax.sharding import PartitionSpec as P


HALO = 2
FAR = float("inf")
EDGE = 8
LEAD = 16


def shifted(array, axis, step):
    count = lax.axis_size(axis)
    return lax.ppermute(array, axis, [(i, (i + step) % count) for i in range(count)])


def flipped(array, axis, bit):
    count = lax.axis_size(axis)
    return lax.ppermute(array, axis, [(i, i ^ bit) for i in range(count)])


def with_halo(cells, axis, dim):
    size = cells.shape[dim]
    index, last = lax.axis_index(axis), lax.axis_size(axis) - 1
    before = shifted(lax.slice_in_dim(cells, size - HALO, size, axis=dim), axis, 1)
    after = shifted(lax.slice_in_dim(cells, 0, HALO, axis=dim), axis, -1)
    far = jnp.asarray(FAR, cells.dtype)
    return jnp.concatenate(
        [jnp.where(index == 0, far, before), cells, jnp.where(index == last, far, after)], axis=dim
    )


def convolve_valid(padded, weight):
    height, breadth = padded.shape[0] - 2, padded.shape[1] - 2
    channels = padded.shape[2]
    summed = jnp.zeros((height * breadth, weight.shape[3]), jnp.float32)
    for offset_row in range(3):
        for offset_col in range(3):
            window = padded[offset_row : offset_row + height, offset_col : offset_col + breadth]
            summed = summed + jnp.dot(
                window.reshape(height * breadth, channels),
                weight[offset_row, offset_col],
                preferred_element_type=jnp.float32,
            )
    return summed.reshape(height, breadth, weight.shape[3])


def rotated(parts, offset, step):
    count = len(parts)
    size = parts[0].shape[0]
    ordered = [parts[(step * k) % count] for k in range(count)]
    twice = jnp.concatenate(ordered + ordered[:-1], axis=0)
    return lax.dynamic_slice_in_dim(twice, ((count - offset) % count) * size, count * size, axis=0)


def gathered_queries(latent_queries):
    rows, cols = lax.axis_size("row"), lax.axis_size("col")
    parts = [latent_queries] + [shifted(latent_queries, "row", k) for k in range(1, rows)]
    queries = rotated(parts, lax.axis_index("row"), -1)
    own = lax.axis_index("col")
    bit = cols // 2
    groups = [queries]
    order = [0]
    while bit > 0:
        groups = groups + list(flipped(jnp.concatenate(groups, axis=0), "col", bit).reshape(len(groups), -1, queries.shape[1]))
        order = order + [place ^ bit for place in order]
        bit //= 2
    stacked = jnp.stack(groups)
    place = jnp.asarray([order.index(k) for k in range(cols)], jnp.int32)
    return stacked[place[own ^ jnp.arange(cols)]].reshape(-1, queries.shape[1])


def in_parts(values, count):
    parts = []
    for _ in range(count):
        part = lax.reduce_precision(values, exponent_bits=8, mantissa_bits=7)
        parts.append(part.astype(jnp.bfloat16))
        values = values - part
    return parts


def packed(pooled, top, total):
    rest = jnp.zeros((11, pooled.shape[1]), jnp.bfloat16)
    return jnp.concatenate(
        [pooled.astype(jnp.bfloat16)] + in_parts(top, 3) + in_parts(total, 2) + [rest], axis=0
    )


def unpacked(block, channels):
    wide = block.astype(jnp.float32)
    row = lambda k: wide[channels + k : channels + k + 1]
    return wide[:channels], row(0) + row(1) + row(2), row(3) + row(4)


def merged(partials):
    top = partials[0][1]
    for _, other, _ in partials[1:]:
        top = jnp.maximum(top, other)
    pooled = total = 0.0
    for part, shift, count in partials:
        factor = jnp.exp(shift - top)
        pooled = pooled + part * factor
        total = total + count * factor
    return pooled, top, total


def plain_attend(features, tissue, marked, latent_queries, weights):
    conv_first, bias_first, conv_second, bias_second, key_weight = weights
    height, breadth, channels = features.shape
    rows = lax.axis_size("row")
    queries = gathered_queries(latent_queries)
    alive = marked < FAR
    inputs = jnp.where(alive, marked, jnp.zeros_like(marked))
    hidden = jax.nn.gelu(convolve_valid(inputs, conv_first) + bias_first, approximate=False)
    hidden = jnp.where(alive[1:-1, 1:-1], hidden, 0.0).astype(jnp.bfloat16)
    second = jax.nn.gelu(convolve_valid(hidden, conv_second) + bias_second, approximate=False)
    second = jnp.where(alive[HALO:-HALO, HALO:-HALO], second, 0.0).astype(jnp.bfloat16)
    flattened = second.reshape(height * breadth, channels)
    key_rows = jnp.dot(flattened, key_weight, preferred_element_type=jnp.float32).astype(
        jnp.bfloat16
    )
    scale = 1.0 / math.sqrt(latent_queries.shape[1])
    scores = (
        lax.dot_general(
            key_rows, queries, (((1,), (1,)), ((), ())), preferred_element_type=jnp.float32
        )
        * scale
    )
    scores = jnp.where(tissue.reshape(-1, 1) > 0, scores, -1e30)
    shift = jnp.max(scores, axis=0, keepdims=True)
    chosen = jnp.exp(scores - shift)
    total = jnp.sum(chosen, axis=0, keepdims=True)
    pooled = lax.dot_general(
        flattened,
        chosen.astype(jnp.bfloat16),
        (((0,), (0,)), ((), ())),
        preferred_element_type=jnp.float32,
    )

    own_row = lax.axis_index("row")
    size = pooled.shape[1] // rows

    def block_of(step):
        start = ((own_row + step) % rows) * size
        cut = lambda array: lax.dynamic_slice_in_dim(array, start, size, axis=1)
        return cut(pooled), cut(shift), cut(total)

    arrived = [shifted(packed(*block_of(k)), "row", k) for k in range(1, rows)]
    partial = merged([block_of(0)] + [unpacked(block, channels) for block in arrived])
    bit = lax.axis_size("col") // 2
    while bit > 0:
        other = flipped(packed(*partial), "col", bit)
        partial = merged([partial, unpacked(other, channels)])
        bit //= 2
    normalized = (partial[0] / partial[2]).astype(jnp.bfloat16)
    return normalized


def gelu(value):
    return 0.5 * value * (1.0 + lax.erf(value * math.sqrt(0.5)))


def mark_kernel(features, tissue, queries, out, queries_out, features_held, tissue_held, done):
    copies = [
        pltpu.make_async_copy(tissue, tissue_held, done.at[0]),
        pltpu.make_async_copy(features, features_held, done.at[1]),
        pltpu.make_async_copy(queries, queries_out, done.at[2]),
    ]
    for copy in copies:
        copy.start()
    height, breadth, channels = features.shape
    copies[0].wait()
    line = lax.broadcasted_iota(jnp.int32, (breadth, breadth), 0)
    place = lax.broadcasted_iota(jnp.int32, (breadth, breadth), 1)
    flags = tissue_held[...].astype(jnp.float32)
    spread = [
        jnp.where(line == place, jnp.broadcast_to(flags[k : k + 1], line.shape), 0.0)
        for k in range(height)
    ]
    keep = jnp.dot(
        jnp.concatenate(spread, axis=0).astype(jnp.bfloat16),
        jnp.ones((breadth, channels), jnp.bfloat16),
        preferred_element_type=jnp.float32,
    )
    copies[1].wait()
    for k in range(height):
        out[k] = jnp.where(
            keep[k * breadth : (k + 1) * breadth] > 0.0, features_held[k].astype(jnp.float32), FAR
        ).astype(jnp.bfloat16)
    copies[2].wait()


def halve_kernel(own, other, out):
    half = own.shape[0] // 2
    core = lax.rem(lax.axis_index("col"), 2)
    start = pl.multiple_of(core * half, half)
    out[pl.ds(start, half), :] = own[pl.ds(start, half), :]
    out[pl.ds(pl.multiple_of((1 - core) * half, half), half), :] = other[pl.ds(start, half), :]


def conv_kernel(
    marked, top, bottom, paired, crossed, first, bias_first, second,
    mid, second_held, cells, taps, done,
):
    later = pltpu.make_async_copy(second, second_held, done)
    later.start()
    height, breadth, channels = marked.shape
    slot = (cells.shape[0] - 2 * EDGE - LEAD) // (height + 2 * HALO)
    flat = cells.shape[0] - 2 * EDGE
    row, col = lax.axis_index("row"), lax.axis_index("col")
    first_row, last_row = row == 0, row == lax.axis_size("row") - 1
    first_col, last_col = col == 0, col == lax.axis_size("col") - 1
    even = lax.rem(col, 2) == 0

    def put(line, place, values, outside):
        start = EDGE + LEAD + line * slot + place
        values = values.astype(jnp.float32)
        if outside is not None:
            values = jnp.where(outside, FAR, values)
        cells[start : start + values.shape[0], :] = values

    cells[...] = jnp.full(cells.shape, FAR, jnp.float32)
    for line in range(height):
        put(line + HALO, 0, marked[line], None)
    for line in range(HALO):
        put(line, 0, top[line], first_row)
        put(height + HALO + line, 0, bottom[line], last_row)
    for line in range(height + 2 * HALO):
        beyond_left, beyond_right = first_col, last_col
        if line < HALO:
            beyond_left, beyond_right = first_col | first_row, last_col | first_row
        if line >= height + HALO:
            beyond_left, beyond_right = first_col | last_row, last_col | last_row
        one, two = paired[line].astype(jnp.float32), crossed[line].astype(jnp.float32)
        put(line, -HALO, jnp.where(even, two, one), beyond_left)
        put(line, breadth, jnp.where(even, one, two), beyond_right)

    for shift in range(3):
        values = cells[EDGE - 1 + shift : EDGE - 1 + shift + flat, :]
        taps[:, shift * channels : (shift + 1) * channels] = jnp.where(
            values < FAR, values, 0.0
        ).astype(jnp.bfloat16)

    count = flat - 2 * slot
    summed = jnp.dot(taps[0:count, :], first[0], preferred_element_type=jnp.float32)
    for line in range(1, 3):
        summed = summed + jnp.dot(
            taps[line * slot : line * slot + count, :], first[line],
            preferred_element_type=jnp.float32,
        )
    alive = cells[EDGE + slot : EDGE + slot + count, :] < FAR
    edge = jnp.zeros((EDGE, channels), jnp.float32)
    mid[0:EDGE, :] = edge
    mid[EDGE + count : 2 * EDGE + count, :] = edge
    mid[EDGE : EDGE + count, :] = jnp.where(alive, gelu(summed + bias_first[...]), 0.0)
    later.wait()


def second_conv_kernel(marked, mid, second, bias_second, out, sent, taps):
    height, breadth, channels = marked.shape
    count = mid.shape[0] - 2 * EDGE
    slot = (count - LEAD) // (height + 2)
    for shift in range(3):
        taps[0:count, shift * channels : (shift + 1) * channels] = mid[
            EDGE - 1 + shift : EDGE - 1 + shift + count, :
        ].astype(jnp.bfloat16)
    inner = height * slot
    summed = jnp.dot(taps[LEAD : LEAD + inner, :], second[0], preferred_element_type=jnp.float32)
    for line in range(1, 3):
        summed = summed + jnp.dot(
            taps[LEAD + line * slot : LEAD + line * slot + inner, :], second[line],
            preferred_element_type=jnp.float32,
        )
    summed = summed.reshape(height, slot, channels)[:, :breadth].reshape(height * breadth, channels)
    alive = marked[...].reshape(height * breadth, channels) < FAR
    value = gelu(summed + bias_second[...])
    out[...] = jnp.where(alive, value, 0.0).astype(jnp.bfloat16)
    sent[...] = jnp.where(alive, value, FAR).astype(jnp.bfloat16)


def key_kernel(cells, weight, keys):
    keys[...] = jnp.dot(cells[...], weight[...], preferred_element_type=jnp.float32).astype(
        jnp.bfloat16
    )


def write_parts(block, values, top, total):
    channels = values.shape[0]
    parts = []
    for source, count in ((top, 3), (total, 2)):
        rest = source
        for _ in range(count):
            part = rest.astype(jnp.bfloat16).astype(jnp.float32)
            parts.append(part)
            rest = rest - part
    parts.append(jnp.zeros((block.shape[0] - channels - 5, values.shape[1]), jnp.float32))
    block[0:channels, :] = values.astype(jnp.bfloat16)
    block[channels:, :] = jnp.concatenate(parts, axis=0).astype(jnp.bfloat16)


def read_parts(block):
    channels = block.shape[0] - 16
    tail = block[channels:, :].astype(jnp.float32)
    row = lambda k: tail[k : k + 1]
    return (
        block[0:channels, :].astype(jnp.float32),
        row(0) + row(1) + row(2),
        row(3) + row(4),
    )


def read_whole(block):
    channels = block.shape[0] - 8
    tail = block[channels:, :]
    return block[0:channels, :], tail[0:1], tail[1:2]


def write_whole(block, values, top, total):
    channels = values.shape[0]
    block[0:channels, :] = values
    block[channels:, :] = jnp.concatenate(
        [top, total, jnp.zeros((6, values.shape[1]), jnp.float32)], axis=0
    )


PLACES = (0, 2, 1, 3)


def hold_queries(held, near, far, use_near):
    half = held.shape[0] // 8
    row = lax.axis_index("row")
    blocks = [
        (one, other, 2 * k * half)
        for one, other in zip(near, far)
        for k in range(one.shape[0] // (2 * half))
    ]
    for (one, other, start), place in zip(blocks, PLACES):
        for parity in range(2):
            source = slice(start + parity * half, start + (parity + 1) * half)
            target = pl.multiple_of(parity * 4 * half + (row ^ place) * half, half)
            held[pl.ds(target, half), :] = jnp.where(use_near, one[source, :], other[source, :])


def masked_scores(queries, marked, keys):
    scale = 1.0 / math.sqrt(queries.shape[1])
    raw = lax.dot_general(
        keys[...], queries[...], (((1,), (1,)), ((), ())), preferred_element_type=jnp.float32
    )
    return jnp.where(marked[:, : raw.shape[1]] < FAR, raw * scale, -1e30)


def score_blocks(scores, sides):
    top = jnp.maximum(*[jnp.max(part, axis=0, keepdims=True) for part in scores])
    pooled = total = 0.0
    for part, cells in zip(scores, sides):
        chosen = jnp.exp(part - top)
        total = total + jnp.sum(chosen, axis=0, keepdims=True)
        pooled = pooled + lax.dot_general(
            cells[...], chosen.astype(jnp.bfloat16), (((0,), (0,)), ((), ())),
            preferred_element_type=jnp.float32,
        )
    channels, lanes = pooled.shape[0] // 2, pooled.shape[1]
    turn = lambda array: pltpu.roll(array, lanes // 2, 1)
    lower = lambda rows: lax.broadcasted_iota(jnp.int32, (rows, lanes), 1) < lanes // 2
    tall, flat = lower(channels), lower(1)
    turned, turned_top, turned_total = turn(pooled), turn(top), turn(total)
    return (
        (
            jnp.where(tall, pooled[:channels], turned[channels:]),
            jnp.where(flat, top, turned_top),
            jnp.where(flat, total, turned_total),
        ),
        (
            jnp.where(tall, turned[:channels], pooled[channels:]),
            jnp.where(flat, turned_top, top),
            jnp.where(flat, turned_total, total),
        ),
    )


def other_kernel(other_sent, weight, other, keys):
    values = other_sent[...].astype(jnp.float32)
    other[...] = jnp.where(values < FAR, values, 0.0).astype(jnp.bfloat16)
    key_kernel(other, weight, keys)


def first_score_kernel(own, own_sent, own_keys, other, other_sent, other_keys, *refs):
    *queries, send_2, send_3, held, blocks = refs
    row, across = lax.axis_index("row"), lax.axis_index("col") // 2
    hold_queries(held, queries[:3], queries[3:], row // 2 != across)
    scores = masked_scores(held, own_sent, own_keys), masked_scores(held, other_sent, other_keys)
    for parity, block in enumerate(score_blocks(scores, (own, other))):
        write_whole(blocks.at[parity], *block)
    odd = lax.rem(row, 2)
    write_parts(send_2, *read_whole(blocks.at[odd]))
    write_parts(send_3, *read_whole(blocks.at[1 - odd]))


def last_score_kernel(own, own_sent, own_keys, other, other_sent, other_keys, *refs):
    *queries, kept, send_1, held, blocks = refs
    row, across = lax.axis_index("row"), lax.axis_index("col") // 2
    hold_queries(held, queries[:3], queries[3:], row // 2 == across)
    scores = masked_scores(held, own_sent, own_keys), masked_scores(held, other_sent, other_keys)
    for parity, block in enumerate(score_blocks(scores, (own, other))):
        write_whole(blocks.at[parity], *block)
    odd = lax.rem(row, 2)
    kept[...] = blocks[odd]
    write_parts(send_1, *read_whole(blocks.at[1 - odd]))


def merge_kernel(own, *refs):
    *arrived, whole, packed_out = refs
    values, top, total = merged([read_whole(own)] + [read_parts(block) for block in arrived])
    write_whole(whole, values, top, total)
    write_parts(packed_out, values, top, total)


def normalize_kernel(own, arrived, out):
    values, _, total = merged([read_whole(own), read_parts(arrived)])
    out[...] = (values / total).astype(jnp.bfloat16)


def attend_kernel(normalized, value_weight, attended):
    lanes = normalized.shape[1] // 2
    values = normalized[...].astype(jnp.float32)
    tall = jnp.concatenate([values, pltpu.roll(values, lanes, 1)], axis=0).astype(jnp.bfloat16)
    attended[...] = lax.dot_general(
        tall, value_weight[...], (((0,), (0,)), ((), ())), preferred_element_type=jnp.float32
    )[:lanes].astype(jnp.bfloat16)


def finish_kernel(mine, arrived, value_weight, out_weight, out, other, attended):
    attend_kernel(arrived, value_weight, other)
    core = lax.rem(lax.axis_index("col"), 2)
    piece = mine.shape[0] // 4
    for place in range(4):
        source = slice(place * piece, (place + 1) * piece)
        first = pl.multiple_of((2 * place + core) * piece, piece)
        last = pl.multiple_of((2 * place + 1 - core) * piece, piece)
        attended[pl.ds(first, piece), :] = mine[source]
        attended[pl.ds(last, piece), :] = other[source]
    out[...] = lax.dot_general(
        out_weight[...], attended[...], (((1,), (1,)), ((), ())),
        preferred_element_type=jnp.float32,
    ).astype(out.dtype)


MIB = 1 << 20


def call(kernel, outs, args, scratch=(), limit=4, flops=0, far=()):
    held = pl.BlockSpec(memory_space=pltpu.VMEM)
    outside = pl.BlockSpec(memory_space=pltpu.HBM)
    return pl.pallas_call(
        kernel,
        out_shape=[pltpu.VMEM(shape, dtype) for shape, dtype in outs],
        in_specs=[outside if k in far else held for k in range(len(args))],
        out_specs=[held] * len(outs),
        scratch_shapes=[pltpu.VMEM(*kind) if isinstance(kind, tuple) else kind for kind in scratch],
        compiler_params=pltpu.CompilerParams(vmem_limit_bytes=limit * MIB),
        cost_estimate=pl.CostEstimate(flops=flops, bytes_accessed=0, transcendentals=0),
    )(
        *[
            pltpu.with_memory_space_constraint(arg, pltpu.HBM if k in far else pltpu.VMEM)
            for k, arg in enumerate(args)
        ]
    )


def kernel_path(
    features, tissue, conv_first, bias_first, conv_second, bias_second, key_weight,
    value_weight, latent_queries, out_weight,
):
    height, breadth, channels = features.shape
    col, cols = lax.axis_index("col"), lax.axis_size("col")
    size, width = latent_queries.shape
    cells = height * breadth
    slot = -(-(breadth + 2 * HALO) // 16) * 16
    flat = LEAD + (height + 2 * HALO) * slot
    count = flat - 2 * slot
    wide, half = jnp.float32, jnp.bfloat16
    block = 4 * size
    whole_block, sent_block = (channels // 2 + 8, block), (channels // 2 + 16, block)
    score_flops = 4 * cells * block * (width + channels)

    beside = flipped(latent_queries, "col", 1)
    marked, queries = call(
        mark_kernel, [(features.shape, half), ((size, width), half)],
        [features, tissue, latent_queries],
        [(features.shape, half), (tissue.shape, jnp.int32), pltpu.SemaphoreType.DMA((3,))],
        far=(0, 1, 2), flops=1 << 20,
    )
    (queries,) = call(halve_kernel, [((size, width), half)], [queries, beside])
    two = flipped(queries, "row", 2)
    top = shifted(marked[height - HALO :], "row", 1)
    bottom = shifted(marked[:HALO], "row", -1)
    one = flipped(queries, "row", 1)
    three = flipped(queries, "row", 3)
    far_queries = flipped(queries, "col", 2)

    edge = lambda cut: jnp.concatenate([top[:, cut], marked[:, cut], bottom[:, cut]], axis=0)
    even = lax.rem(col, 2) == 0
    ends = edge(slice(breadth - HALO, breadth)), edge(slice(0, HALO))
    paired = flipped(jnp.where(even, *ends), "col", 1)
    rounds = [(k, (k + 1 if k % 2 else k - 1) % cols) for k in range(cols)]
    crossed = lax.ppermute(jnp.where(even, *ends[::-1]), "col", rounds)

    pair = jnp.concatenate([two, one], axis=0)
    far_pair = flipped(pair, "col", 2)
    far_three = flipped(three, "col", 2)

    mid, weight = call(
        conv_kernel,
        [((count + 2 * EDGE, channels), wide), ((3, 3 * channels, channels), half)],
        [
            marked, top, bottom, paired, crossed,
            conv_first.reshape(3, 3 * channels, channels), bias_first.reshape(1, channels),
            conv_second.reshape(3, 3 * channels, channels),
        ],
        [
            ((flat + 2 * EDGE, channels), wide),
            ((flat, 3 * channels), half),
            pltpu.SemaphoreType.DMA,
        ],
        limit=12, far=(7,), flops=21 * cells * channels * channels,
    )
    own, own_sent = call(
        second_conv_kernel, [((cells, channels), half)] * 2,
        [marked, mid, weight, bias_second.reshape(1, channels)],
        [((count, 3 * channels), half)],
        limit=10, flops=18 * cells * channels * channels,
    )
    other_sent = flipped(own_sent, "col", 1)
    (own_keys,) = call(
        key_kernel, [((cells, width), half)], [own, key_weight],
        limit=4, flops=2 * cells * width * channels,
    )
    all_queries = [queries, pair, three, far_queries, far_pair, far_three]
    score_scratch = [((block, width), half), ((2,) + whole_block, wide)]
    other, other_keys = call(
        other_kernel, [((cells, channels), half), ((cells, width), half)],
        [other_sent, key_weight], limit=4, flops=2 * cells * channels * width,
    )
    send_2, send_3 = call(
        first_score_kernel, [(sent_block, half)] * 2,
        [own, own_sent, own_keys, other, other_sent, other_keys, *all_queries],
        score_scratch, limit=8, flops=score_flops,
    )
    arrived_2, arrived_3 = flipped(send_2, "row", 2), flipped(send_3, "row", 3)
    kept, send_1 = call(
        last_score_kernel, [(whole_block, wide), (sent_block, half)],
        [own, own_sent, own_keys, other, other_sent, other_keys, *all_queries],
        score_scratch, limit=8, flops=score_flops,
    )
    arrived_1 = flipped(send_1, "row", 1)
    kept, sent = call(
        merge_kernel, [(whole_block, wide), (sent_block, half)],
        [kept, arrived_1, arrived_2, arrived_3],
    )
    arrived = flipped(sent, "col", 2)
    (normalized,) = call(normalize_kernel, [((channels // 2, block), half)], [kept, arrived])
    arrived = flipped(normalized, "col", 1)
    (attended,) = call(
        attend_kernel, [((2 * size, width), half)], [normalized, value_weight],
        flops=8 * size * channels * width,
    )
    held = pl.BlockSpec(memory_space=pltpu.VMEM)
    keep = lambda array: pltpu.with_memory_space_constraint(array, pltpu.VMEM)
    return pl.pallas_call(
        finish_kernel,
        out_shape=jax.ShapeDtypeStruct((out_weight.shape[1], block), half),
        in_specs=[held] * 4,
        out_specs=held,
        scratch_shapes=[pltpu.VMEM((2 * size, width), half), pltpu.VMEM((block, width), half)],
        compiler_params=pltpu.CompilerParams(vmem_limit_bytes=6 * MIB),
        name="fn",
    )(keep(attended), keep(arrived), keep(value_weight), keep(out_weight.T)).T


def shards(
    features, tissue, conv_first, bias_first, conv_second, bias_second, key_weight,
    value_weight, latent_queries, out_weight,
):
    rows, cols = lax.axis_size("row"), lax.axis_size("col")
    if rows == cols == 4 and rows * latent_queries.shape[0] == 128:
        return kernel_path(
            features, tissue, conv_first, bias_first, conv_second, bias_second, key_weight,
            value_weight, latent_queries, out_weight,
        )
    marked = jnp.where(tissue[:, :, None] > 0, features, jnp.asarray(FAR, features.dtype))
    marked = with_halo(with_halo(marked, "row", 0), "col", 1)
    normalized = plain_attend(
        features, tissue, marked, latent_queries,
        (conv_first, bias_first, conv_second, bias_second, key_weight),
    )
    attended = lax.dot_general(
        normalized, value_weight, (((0,), (0,)), ((), ())), preferred_element_type=jnp.float32
    ).astype(jnp.bfloat16)
    return jnp.dot(attended, out_weight, preferred_element_type=jnp.float32).astype(jnp.bfloat16)


def solution(mesh):
    placed = (
        P(("groups", "row"), "col", None),
        P(("groups", "row"), "col"),
        P(),
        P(),
        P(),
        P(),
        P(),
        P(),
        P(("col", "row"), None),
        P(None, "col"),
    )
    return jax.shard_map(
        shards, mesh=mesh, in_specs=placed, out_specs=P(("groups", "row"), "col"), check_vma=False
    )
```

```python
import math

import jax
import jax.numpy as jnp
from jax import lax
from jax.experimental import pallas as pl
from jax.experimental.pallas import tpu as pltpu
from jax.sharding import PartitionSpec as P


HALO = 2
FAR = float("inf")
EDGE = 8
LEAD = 16


def shifted(array, axis, step):
    count = lax.axis_size(axis)
    return lax.ppermute(array, axis, [(i, (i + step) % count) for i in range(count)])


def flipped(array, axis, bit):
    count = lax.axis_size(axis)
    return lax.ppermute(array, axis, [(i, i ^ bit) for i in range(count)])


def with_halo(cells, axis, dim):
    size = cells.shape[dim]
    index, last = lax.axis_index(axis), lax.axis_size(axis) - 1
    before = shifted(lax.slice_in_dim(cells, size - HALO, size, axis=dim), axis, 1)
    after = shifted(lax.slice_in_dim(cells, 0, HALO, axis=dim), axis, -1)
    far = jnp.asarray(FAR, cells.dtype)
    return jnp.concatenate(
        [jnp.where(index == 0, far, before), cells, jnp.where(index == last, far, after)], axis=dim
    )


def convolve_valid(padded, weight):
    height, breadth = padded.shape[0] - 2, padded.shape[1] - 2
    channels = padded.shape[2]
    summed = jnp.zeros((height * breadth, weight.shape[3]), jnp.float32)
    for offset_row in range(3):
        for offset_col in range(3):
            window = padded[offset_row : offset_row + height, offset_col : offset_col + breadth]
            summed = summed + jnp.dot(
                window.reshape(height * breadth, channels),
                weight[offset_row, offset_col],
                preferred_element_type=jnp.float32,
            )
    return summed.reshape(height, breadth, weight.shape[3])


def rotated(parts, offset, step):
    count = len(parts)
    size = parts[0].shape[0]
    ordered = [parts[(step * k) % count] for k in range(count)]
    twice = jnp.concatenate(ordered + ordered[:-1], axis=0)
    return lax.dynamic_slice_in_dim(twice, ((count - offset) % count) * size, count * size, axis=0)


def gathered_queries(latent_queries):
    rows, cols = lax.axis_size("row"), lax.axis_size("col")
    parts = [latent_queries] + [shifted(latent_queries, "row", k) for k in range(1, rows)]
    queries = rotated(parts, lax.axis_index("row"), -1)
    own = lax.axis_index("col")
    bit = cols // 2
    groups = [queries]
    order = [0]
    while bit > 0:
        groups = groups + list(flipped(jnp.concatenate(groups, axis=0), "col", bit).reshape(len(groups), -1, queries.shape[1]))
        order = order + [place ^ bit for place in order]
        bit //= 2
    stacked = jnp.stack(groups)
    place = jnp.asarray([order.index(k) for k in range(cols)], jnp.int32)
    return stacked[place[own ^ jnp.arange(cols)]].reshape(-1, queries.shape[1])


def in_parts(values, count):
    parts = []
    for _ in range(count):
        part = lax.reduce_precision(values, exponent_bits=8, mantissa_bits=7)
        parts.append(part.astype(jnp.bfloat16))
        values = values - part
    return parts


def packed(pooled, top, total):
    rest = jnp.zeros((11, pooled.shape[1]), jnp.bfloat16)
    return jnp.concatenate(
        [pooled.astype(jnp.bfloat16)] + in_parts(top, 3) + in_parts(total, 2) + [rest], axis=0
    )


def unpacked(block, channels):
    wide = block.astype(jnp.float32)
    row = lambda k: wide[channels + k : channels + k + 1]
    return wide[:channels], row(0) + row(1) + row(2), row(3) + row(4)


def merged(partials):
    top = partials[0][1]
    for _, other, _ in partials[1:]:
        top = jnp.maximum(top, other)
    pooled = total = 0.0
    for part, shift, count in partials:
        factor = jnp.exp(shift - top)
        pooled = pooled + part * factor
        total = total + count * factor
    return pooled, top, total


def plain_attend(features, tissue, marked, latent_queries, weights):
    conv_first, bias_first, conv_second, bias_second, key_weight = weights
    height, breadth, channels = features.shape
    rows = lax.axis_size("row")
    queries = gathered_queries(latent_queries)
    alive = marked < FAR
    inputs = jnp.where(alive, marked, jnp.zeros_like(marked))
    hidden = jax.nn.gelu(convolve_valid(inputs, conv_first) + bias_first, approximate=False)
    hidden = jnp.where(alive[1:-1, 1:-1], hidden, 0.0).astype(jnp.bfloat16)
    second = jax.nn.gelu(convolve_valid(hidden, conv_second) + bias_second, approximate=False)
    second = jnp.where(alive[HALO:-HALO, HALO:-HALO], second, 0.0).astype(jnp.bfloat16)
    flattened = second.reshape(height * breadth, channels)
    key_rows = jnp.dot(flattened, key_weight, preferred_element_type=jnp.float32).astype(
        jnp.bfloat16
    )
    scale = 1.0 / math.sqrt(latent_queries.shape[1])
    scores = (
        lax.dot_general(
            key_rows, queries, (((1,), (1,)), ((), ())), preferred_element_type=jnp.float32
        )
        * scale
    )
    scores = jnp.where(tissue.reshape(-1, 1) > 0, scores, -1e30)
    shift = jnp.max(scores, axis=0, keepdims=True)
    chosen = jnp.exp(scores - shift)
    total = jnp.sum(chosen, axis=0, keepdims=True)
    pooled = lax.dot_general(
        flattened,
        chosen.astype(jnp.bfloat16),
        (((0,), (0,)), ((), ())),
        preferred_element_type=jnp.float32,
    )

    own_row = lax.axis_index("row")
    size = pooled.shape[1] // rows

    def block_of(step):
        start = ((own_row + step) % rows) * size
        cut = lambda array: lax.dynamic_slice_in_dim(array, start, size, axis=1)
        return cut(pooled), cut(shift), cut(total)

    arrived = [shifted(packed(*block_of(k)), "row", k) for k in range(1, rows)]
    partial = merged([block_of(0)] + [unpacked(block, channels) for block in arrived])
    bit = lax.axis_size("col") // 2
    while bit > 0:
        other = flipped(packed(*partial), "col", bit)
        partial = merged([partial, unpacked(other, channels)])
        bit //= 2
    normalized = (partial[0] / partial[2]).astype(jnp.bfloat16)
    return normalized


def gelu(value):
    return 0.5 * value * (1.0 + lax.erf(value * math.sqrt(0.5)))


def mark_kernel(features, tissue, queries, out, queries_out, features_held, tissue_held, done):
    copies = [
        pltpu.make_async_copy(tissue, tissue_held, done.at[0]),
        pltpu.make_async_copy(features, features_held, done.at[1]),
        pltpu.make_async_copy(queries, queries_out, done.at[2]),
    ]
    for copy in copies:
        copy.start()
    height, breadth, channels = features.shape
    copies[0].wait()
    line = lax.broadcasted_iota(jnp.int32, (breadth, breadth), 0)
    place = lax.broadcasted_iota(jnp.int32, (breadth, breadth), 1)
    flags = tissue_held[...].astype(jnp.float32)
    spread = [
        jnp.where(line == place, jnp.broadcast_to(flags[k : k + 1], line.shape), 0.0)
        for k in range(height)
    ]
    keep = jnp.dot(
        jnp.concatenate(spread, axis=0).astype(jnp.bfloat16),
        jnp.ones((breadth, channels), jnp.bfloat16),
        preferred_element_type=jnp.float32,
    )
    copies[1].wait()
    for k in range(height):
        out[k] = jnp.where(
            keep[k * breadth : (k + 1) * breadth] > 0.0, features_held[k].astype(jnp.float32), FAR
        ).astype(jnp.bfloat16)
    copies[2].wait()


def halve_kernel(own, other, out):
    half = own.shape[0] // 2
    core = lax.rem(lax.axis_index("col"), 2)
    start = pl.multiple_of(core * half, half)
    out[pl.ds(start, half), :] = own[pl.ds(start, half), :]
    out[pl.ds(pl.multiple_of((1 - core) * half, half), half), :] = other[pl.ds(start, half), :]


def conv_kernel(
    marked, top, bottom, paired, crossed, first, bias_first, second,
    mid, second_held, cells, taps, done,
):
    later = pltpu.make_async_copy(second, second_held, done)
    later.start()
    height, breadth, channels = marked.shape
    slot = (cells.shape[0] - 2 * EDGE - LEAD) // (height + 2 * HALO)
    flat = cells.shape[0] - 2 * EDGE
    row, col = lax.axis_index("row"), lax.axis_index("col")
    first_row, last_row = row == 0, row == lax.axis_size("row") - 1
    first_col, last_col = col == 0, col == lax.axis_size("col") - 1
    even = lax.rem(col, 2) == 0

    def put(line, place, values, outside):
        start = EDGE + LEAD + line * slot + place
        values = values.astype(jnp.float32)
        if outside is not None:
            values = jnp.where(outside, FAR, values)
        cells[start : start + values.shape[0], :] = values

    cells[...] = jnp.full(cells.shape, FAR, jnp.float32)
    for line in range(height):
        put(line + HALO, 0, marked[line], None)
    for line in range(HALO):
        put(line, 0, top[line], first_row)
        put(height + HALO + line, 0, bottom[line], last_row)
    for line in range(height + 2 * HALO):
        beyond_left, beyond_right = first_col, last_col
        if line < HALO:
            beyond_left, beyond_right = first_col | first_row, last_col | first_row
        if line >= height + HALO:
            beyond_left, beyond_right = first_col | last_row, last_col | last_row
        one, two = paired[line].astype(jnp.float32), crossed[line].astype(jnp.float32)
        put(line, -HALO, jnp.where(even, two, one), beyond_left)
        put(line, breadth, jnp.where(even, one, two), beyond_right)

    for shift in range(3):
        values = cells[EDGE - 1 + shift : EDGE - 1 + shift + flat, :]
        taps[:, shift * channels : (shift + 1) * channels] = jnp.where(
            values < FAR, values, 0.0
        ).astype(jnp.bfloat16)

    count = flat - 2 * slot
    summed = jnp.dot(taps[0:count, :], first[0], preferred_element_type=jnp.float32)
    for line in range(1, 3):
        summed = summed + jnp.dot(
            taps[line * slot : line * slot + count, :], first[line],
            preferred_element_type=jnp.float32,
        )
    alive = cells[EDGE + slot : EDGE + slot + count, :] < FAR
    edge = jnp.zeros((EDGE, channels), jnp.float32)
    mid[0:EDGE, :] = edge
    mid[EDGE + count : 2 * EDGE + count, :] = edge
    mid[EDGE : EDGE + count, :] = jnp.where(alive, gelu(summed + bias_first[...]), 0.0)
    later.wait()


def second_conv_kernel(marked, mid, second, bias_second, out, sent, taps):
    height, breadth, channels = marked.shape
    count = mid.shape[0] - 2 * EDGE
    slot = (count - LEAD) // (height + 2)
    for shift in range(3):
        taps[0:count, shift * channels : (shift + 1) * channels] = mid[
            EDGE - 1 + shift : EDGE - 1 + shift + count, :
        ].astype(jnp.bfloat16)
    inner = height * slot
    summed = jnp.dot(taps[LEAD : LEAD + inner, :], second[0], preferred_element_type=jnp.float32)
    for line in range(1, 3):
        summed = summed + jnp.dot(
            taps[LEAD + line * slot : LEAD + line * slot + inner, :], second[line],
            preferred_element_type=jnp.float32,
        )
    summed = summed.reshape(height, slot, channels)[:, :breadth].reshape(height * breadth, channels)
    alive = marked[...].reshape(height * breadth, channels) < FAR
    value = gelu(summed + bias_second[...])
    out[...] = jnp.where(alive, value, 0.0).astype(jnp.bfloat16)
    sent[...] = jnp.where(alive, value, FAR).astype(jnp.bfloat16)


def key_kernel(cells, weight, keys):
    keys[...] = jnp.dot(cells[...], weight[...], preferred_element_type=jnp.float32).astype(
        jnp.bfloat16
    )


def write_parts(block, values, top, total):
    channels = values.shape[0]
    parts = []
    for source, count in ((top, 3), (total, 2)):
        rest = source
        for _ in range(count):
            part = rest.astype(jnp.bfloat16).astype(jnp.float32)
            parts.append(part)
            rest = rest - part
    parts.append(jnp.zeros((block.shape[0] - channels - 5, values.shape[1]), jnp.float32))
    block[0:channels, :] = values.astype(jnp.bfloat16)
    block[channels:, :] = jnp.concatenate(parts, axis=0).astype(jnp.bfloat16)


def read_parts(block):
    channels = block.shape[0] - 16
    tail = block[channels:, :].astype(jnp.float32)
    row = lambda k: tail[k : k + 1]
    return (
        block[0:channels, :].astype(jnp.float32),
        row(0) + row(1) + row(2),
        row(3) + row(4),
    )


def read_whole(block):
    channels = block.shape[0] - 8
    tail = block[channels:, :]
    return block[0:channels, :], tail[0:1], tail[1:2]


def write_whole(block, values, top, total):
    channels = values.shape[0]
    block[0:channels, :] = values
    block[channels:, :] = jnp.concatenate(
        [top, total, jnp.zeros((6, values.shape[1]), jnp.float32)], axis=0
    )


PLACES = (0, 2, 1, 3)


def hold_queries(held, near, far, use_near):
    half = held.shape[0] // 8
    row = lax.axis_index("row")
    blocks = [
        (one, other, 2 * k * half)
        for one, other in zip(near, far)
        for k in range(one.shape[0] // (2 * half))
    ]
    for (one, other, start), place in zip(blocks, PLACES):
        for parity in range(2):
            source = slice(start + parity * half, start + (parity + 1) * half)
            target = pl.multiple_of(parity * 4 * half + (row ^ place) * half, half)
            held[pl.ds(target, half), :] = jnp.where(use_near, one[source, :], other[source, :])


def masked_scores(queries, marked, keys):
    scale = 1.0 / math.sqrt(queries.shape[1])
    raw = lax.dot_general(
        keys[...], queries[...], (((1,), (1,)), ((), ())), preferred_element_type=jnp.float32
    )
    return jnp.where(marked[:, : raw.shape[1]] < FAR, raw * scale, -1e30)


def score_blocks(scores, sides):
    top = jnp.maximum(*[jnp.max(part, axis=0, keepdims=True) for part in scores])
    pooled = total = 0.0
    for part, cells in zip(scores, sides):
        chosen = jnp.exp(part - top)
        total = total + jnp.sum(chosen, axis=0, keepdims=True)
        pooled = pooled + lax.dot_general(
            cells[...], chosen.astype(jnp.bfloat16), (((0,), (0,)), ((), ())),
            preferred_element_type=jnp.float32,
        )
    channels, lanes = pooled.shape[0] // 2, pooled.shape[1]
    turn = lambda array: pltpu.roll(array, lanes // 2, 1)
    lower = lambda rows: lax.broadcasted_iota(jnp.int32, (rows, lanes), 1) < lanes // 2
    tall, flat = lower(channels), lower(1)
    turned, turned_top, turned_total = turn(pooled), turn(top), turn(total)
    return (
        (
            jnp.where(tall, pooled[:channels], turned[channels:]),
            jnp.where(flat, top, turned_top),
            jnp.where(flat, total, turned_total),
        ),
        (
            jnp.where(tall, turned[:channels], pooled[channels:]),
            jnp.where(flat, turned_top, top),
            jnp.where(flat, turned_total, total),
        ),
    )


def other_kernel(other_sent, weight, other, keys):
    values = other_sent[...].astype(jnp.float32)
    other[...] = jnp.where(values < FAR, values, 0.0).astype(jnp.bfloat16)
    key_kernel(other, weight, keys)


def first_score_kernel(own, own_sent, own_keys, other, other_sent, other_keys, *refs):
    *queries, send_2, send_3, held, blocks = refs
    row, across = lax.axis_index("row"), lax.axis_index("col") // 2
    hold_queries(held, queries[:3], queries[3:], row // 2 != across)
    scores = masked_scores(held, own_sent, own_keys), masked_scores(held, other_sent, other_keys)
    for parity, block in enumerate(score_blocks(scores, (own, other))):
        write_whole(blocks.at[parity], *block)
    odd = lax.rem(row, 2)
    write_parts(send_2, *read_whole(blocks.at[odd]))
    write_parts(send_3, *read_whole(blocks.at[1 - odd]))


def last_score_kernel(own, own_sent, own_keys, other, other_sent, other_keys, *refs):
    *queries, kept, send_1, held, blocks = refs
    row, across = lax.axis_index("row"), lax.axis_index("col") // 2
    hold_queries(held, queries[:3], queries[3:], row // 2 == across)
    scores = masked_scores(held, own_sent, own_keys), masked_scores(held, other_sent, other_keys)
    for parity, block in enumerate(score_blocks(scores, (own, other))):
        write_whole(blocks.at[parity], *block)
    odd = lax.rem(row, 2)
    kept[...] = blocks[odd]
    write_parts(send_1, *read_whole(blocks.at[1 - odd]))


def merge_kernel(own, *refs):
    *arrived, whole, packed_out = refs
    values, top, total = merged([read_whole(own)] + [read_parts(block) for block in arrived])
    write_whole(whole, values, top, total)
    write_parts(packed_out, values, top, total)


def normalize_kernel(own, arrived, out):
    values, _, total = merged([read_whole(own), read_parts(arrived)])
    out[...] = (values / total).astype(jnp.bfloat16)


def attend_kernel(normalized, value_weight, attended):
    lanes = normalized.shape[1] // 2
    values = normalized[...].astype(jnp.float32)
    tall = jnp.concatenate([values, pltpu.roll(values, lanes, 1)], axis=0).astype(jnp.bfloat16)
    attended[...] = lax.dot_general(
        tall, value_weight[...], (((0,), (0,)), ((), ())), preferred_element_type=jnp.float32
    )[:lanes].astype(jnp.bfloat16)


def finish_kernel(mine, arrived, value_weight, out_weight, out, other, attended):
    attend_kernel(arrived, value_weight, other)
    core = lax.rem(lax.axis_index("col"), 2)
    piece = mine.shape[0] // 4
    for place in range(4):
        source = slice(place * piece, (place + 1) * piece)
        first = pl.multiple_of((2 * place + core) * piece, piece)
        last = pl.multiple_of((2 * place + 1 - core) * piece, piece)
        attended[pl.ds(first, piece), :] = mine[source]
        attended[pl.ds(last, piece), :] = other[source]
    out[...] = lax.dot_general(
        out_weight[...], attended[...], (((1,), (1,)), ((), ())),
        preferred_element_type=jnp.float32,
    ).astype(out.dtype)


MIB = 1 << 20


def call(kernel, outs, args, scratch=(), limit=4, flops=0, far=()):
    held = pl.BlockSpec(memory_space=pltpu.VMEM)
    outside = pl.BlockSpec(memory_space=pltpu.HBM)
    return pl.pallas_call(
        kernel,
        out_shape=[pltpu.VMEM(shape, dtype) for shape, dtype in outs],
        in_specs=[outside if k in far else held for k in range(len(args))],
        out_specs=[held] * len(outs),
        scratch_shapes=[pltpu.VMEM(*kind) if isinstance(kind, tuple) else kind for kind in scratch],
        compiler_params=pltpu.CompilerParams(vmem_limit_bytes=limit * MIB),
        cost_estimate=pl.CostEstimate(flops=flops, bytes_accessed=0, transcendentals=0),
    )(
        *[
            pltpu.with_memory_space_constraint(arg, pltpu.HBM if k in far else pltpu.VMEM)
            for k, arg in enumerate(args)
        ]
    )


def kernel_path(
    features, tissue, conv_first, bias_first, conv_second, bias_second, key_weight,
    value_weight, latent_queries, out_weight,
):
    height, breadth, channels = features.shape
    col, cols = lax.axis_index("col"), lax.axis_size("col")
    size, width = latent_queries.shape
    cells = height * breadth
    slot = -(-(breadth + 2 * HALO) // 16) * 16
    flat = LEAD + (height + 2 * HALO) * slot
    count = flat - 2 * slot
    wide, half = jnp.float32, jnp.bfloat16
    block = 4 * size
    whole_block, sent_block = (channels // 2 + 8, block), (channels // 2 + 16, block)
    score_flops = 4 * cells * block * (width + channels)

    beside = flipped(latent_queries, "col", 1)
    marked, queries = call(
        mark_kernel, [(features.shape, half), ((size, width), half)],
        [features, tissue, latent_queries],
        [(features.shape, half), (tissue.shape, jnp.int32), pltpu.SemaphoreType.DMA((3,))],
        far=(0, 1, 2), flops=1 << 20,
    )
    (queries,) = call(halve_kernel, [((size, width), half)], [queries, beside])
    two = flipped(queries, "row", 2)
    top = shifted(marked[height - HALO :], "row", 1)
    bottom = shifted(marked[:HALO], "row", -1)
    one = flipped(queries, "row", 1)
    three = flipped(queries, "row", 3)
    far_queries = flipped(queries, "col", 2)

    sides = slice(breadth - HALO, breadth), slice(0, HALO)
    middles = [marked[:, cut] for cut in sides]
    even = lax.rem(col, 2) == 0
    ends = [
        jnp.concatenate([top[:, cut], middle, bottom[:, cut]], axis=0)
        for cut, middle in zip(sides, middles)
    ]
    paired = flipped(jnp.where(even, *ends), "col", 1)
    rounds = [(k, (k + 1 if k % 2 else k - 1) % cols) for k in range(cols)]
    crossed = lax.ppermute(jnp.where(even, *ends[::-1]), "col", rounds)

    pair = jnp.concatenate([two, one], axis=0)
    far_pair = flipped(pair, "col", 2)
    far_three = flipped(three, "col", 2)

    mid, weight = call(
        conv_kernel,
        [((count + 2 * EDGE, channels), wide), ((3, 3 * channels, channels), half)],
        [
            marked, top, bottom, paired, crossed,
            conv_first.reshape(3, 3 * channels, channels), bias_first.reshape(1, channels),
            conv_second.reshape(3, 3 * channels, channels),
        ],
        [
            ((flat + 2 * EDGE, channels), wide),
            ((flat, 3 * channels), half),
            pltpu.SemaphoreType.DMA,
        ],
        limit=12, far=(7,), flops=21 * cells * channels * channels,
    )
    own, own_sent = call(
        second_conv_kernel, [((cells, channels), half)] * 2,
        [marked, mid, weight, bias_second.reshape(1, channels)],
        [((count, 3 * channels), half)],
        limit=10, flops=18 * cells * channels * channels,
    )
    other_sent = flipped(own_sent, "col", 1)
    (own_keys,) = call(
        key_kernel, [((cells, width), half)], [own, key_weight],
        limit=4, flops=2 * cells * width * channels,
    )
    all_queries = [queries, pair, three, far_queries, far_pair, far_three]
    score_scratch = [((block, width), half), ((2,) + whole_block, wide)]
    other, other_keys = call(
        other_kernel, [((cells, channels), half), ((cells, width), half)],
        [other_sent, key_weight], limit=4, flops=2 * cells * channels * width,
    )
    send_2, send_3 = call(
        first_score_kernel, [(sent_block, half)] * 2,
        [own, own_sent, own_keys, other, other_sent, other_keys, *all_queries],
        score_scratch, limit=8, flops=score_flops,
    )
    arrived_2, arrived_3 = flipped(send_2, "row", 2), flipped(send_3, "row", 3)
    kept, send_1 = call(
        last_score_kernel, [(whole_block, wide), (sent_block, half)],
        [own, own_sent, own_keys, other, other_sent, other_keys, *all_queries],
        score_scratch, limit=8, flops=score_flops,
    )
    arrived_1 = flipped(send_1, "row", 1)
    kept, sent = call(
        merge_kernel, [(whole_block, wide), (sent_block, half)],
        [kept, arrived_1, arrived_2, arrived_3],
    )
    arrived = flipped(sent, "col", 2)
    (normalized,) = call(normalize_kernel, [((channels // 2, block), half)], [kept, arrived])
    arrived = flipped(normalized, "col", 1)
    (attended,) = call(
        attend_kernel, [((2 * size, width), half)], [normalized, value_weight],
        flops=8 * size * channels * width,
    )
    held = pl.BlockSpec(memory_space=pltpu.VMEM)
    keep = lambda array: pltpu.with_memory_space_constraint(array, pltpu.VMEM)
    return pl.pallas_call(
        finish_kernel,
        out_shape=jax.ShapeDtypeStruct((out_weight.shape[1], block), half),
        in_specs=[held] * 4,
        out_specs=held,
        scratch_shapes=[pltpu.VMEM((2 * size, width), half), pltpu.VMEM((block, width), half)],
        compiler_params=pltpu.CompilerParams(vmem_limit_bytes=6 * MIB),
        name="fn",
    )(keep(attended), keep(arrived), keep(value_weight), keep(out_weight.T)).T


def shards(
    features, tissue, conv_first, bias_first, conv_second, bias_second, key_weight,
    value_weight, latent_queries, out_weight,
):
    rows, cols = lax.axis_size("row"), lax.axis_size("col")
    if rows == cols == 4 and rows * latent_queries.shape[0] == 128:
        return kernel_path(
            features, tissue, conv_first, bias_first, conv_second, bias_second, key_weight,
            value_weight, latent_queries, out_weight,
        )
    marked = jnp.where(tissue[:, :, None] > 0, features, jnp.asarray(FAR, features.dtype))
    marked = with_halo(with_halo(marked, "row", 0), "col", 1)
    normalized = plain_attend(
        features, tissue, marked, latent_queries,
        (conv_first, bias_first, conv_second, bias_second, key_weight),
    )
    attended = lax.dot_general(
        normalized, value_weight, (((0,), (0,)), ((), ())), preferred_element_type=jnp.float32
    ).astype(jnp.bfloat16)
    return jnp.dot(attended, out_weight, preferred_element_type=jnp.float32).astype(jnp.bfloat16)


def solution(mesh):
    placed = (
        P(("groups", "row"), "col", None),
        P(("groups", "row"), "col"),
        P(),
        P(),
        P(),
        P(),
        P(),
        P(),
        P(("col", "row"), None),
        P(None, "col"),
    )
    return jax.shard_map(
        shards, mesh=mesh, in_specs=placed, out_specs=P(("groups", "row"), "col"), check_vma=False
    )
```

```python
import math

import jax
import jax.numpy as jnp
from jax import lax
from jax.experimental import pallas as pl
from jax.experimental.pallas import tpu as pltpu
from jax.sharding import PartitionSpec as P


HALO = 2
FAR = float("inf")
EDGE = 8
LEAD = 16


def shifted(array, axis, step):
    count = lax.axis_size(axis)
    return lax.ppermute(array, axis, [(i, (i + step) % count) for i in range(count)])


def flipped(array, axis, bit):
    count = lax.axis_size(axis)
    return lax.ppermute(array, axis, [(i, i ^ bit) for i in range(count)])


def with_halo(cells, axis, dim):
    size = cells.shape[dim]
    index, last = lax.axis_index(axis), lax.axis_size(axis) - 1
    before = shifted(lax.slice_in_dim(cells, size - HALO, size, axis=dim), axis, 1)
    after = shifted(lax.slice_in_dim(cells, 0, HALO, axis=dim), axis, -1)
    far = jnp.asarray(FAR, cells.dtype)
    return jnp.concatenate(
        [jnp.where(index == 0, far, before), cells, jnp.where(index == last, far, after)], axis=dim
    )


def convolve_valid(padded, weight):
    height, breadth = padded.shape[0] - 2, padded.shape[1] - 2
    channels = padded.shape[2]
    summed = jnp.zeros((height * breadth, weight.shape[3]), jnp.float32)
    for offset_row in range(3):
        for offset_col in range(3):
            window = padded[offset_row : offset_row + height, offset_col : offset_col + breadth]
            summed = summed + jnp.dot(
                window.reshape(height * breadth, channels),
                weight[offset_row, offset_col],
                preferred_element_type=jnp.float32,
            )
    return summed.reshape(height, breadth, weight.shape[3])


def rotated(parts, offset, step):
    count = len(parts)
    size = parts[0].shape[0]
    ordered = [parts[(step * k) % count] for k in range(count)]
    twice = jnp.concatenate(ordered + ordered[:-1], axis=0)
    return lax.dynamic_slice_in_dim(twice, ((count - offset) % count) * size, count * size, axis=0)


def gathered_queries(latent_queries):
    rows, cols = lax.axis_size("row"), lax.axis_size("col")
    parts = [latent_queries] + [shifted(latent_queries, "row", k) for k in range(1, rows)]
    queries = rotated(parts, lax.axis_index("row"), -1)
    own = lax.axis_index("col")
    bit = cols // 2
    groups = [queries]
    order = [0]
    while bit > 0:
        groups = groups + list(flipped(jnp.concatenate(groups, axis=0), "col", bit).reshape(len(groups), -1, queries.shape[1]))
        order = order + [place ^ bit for place in order]
        bit //= 2
    stacked = jnp.stack(groups)
    place = jnp.asarray([order.index(k) for k in range(cols)], jnp.int32)
    return stacked[place[own ^ jnp.arange(cols)]].reshape(-1, queries.shape[1])


def in_parts(values, count):
    parts = []
    for _ in range(count):
        part = lax.reduce_precision(values, exponent_bits=8, mantissa_bits=7)
        parts.append(part.astype(jnp.bfloat16))
        values = values - part
    return parts


def packed(pooled, top, total):
    rest = jnp.zeros((11, pooled.shape[1]), jnp.bfloat16)
    return jnp.concatenate(
        [pooled.astype(jnp.bfloat16)] + in_parts(top, 3) + in_parts(total, 2) + [rest], axis=0
    )


def unpacked(block, channels):
    wide = block.astype(jnp.float32)
    row = lambda k: wide[channels + k : channels + k + 1]
    return wide[:channels], row(0) + row(1) + row(2), row(3) + row(4)


def merged(partials):
    top = partials[0][1]
    for _, other, _ in partials[1:]:
        top = jnp.maximum(top, other)
    pooled = total = 0.0
    for part, shift, count in partials:
        factor = jnp.exp(shift - top)
        pooled = pooled + part * factor
        total = total + count * factor
    return pooled, top, total


def plain_attend(features, tissue, marked, latent_queries, weights):
    conv_first, bias_first, conv_second, bias_second, key_weight = weights
    height, breadth, channels = features.shape
    rows = lax.axis_size("row")
    queries = gathered_queries(latent_queries)
    alive = marked < FAR
    inputs = jnp.where(alive, marked, jnp.zeros_like(marked))
    hidden = jax.nn.gelu(convolve_valid(inputs, conv_first) + bias_first, approximate=False)
    hidden = jnp.where(alive[1:-1, 1:-1], hidden, 0.0).astype(jnp.bfloat16)
    second = jax.nn.gelu(convolve_valid(hidden, conv_second) + bias_second, approximate=False)
    second = jnp.where(alive[HALO:-HALO, HALO:-HALO], second, 0.0).astype(jnp.bfloat16)
    flattened = second.reshape(height * breadth, channels)
    key_rows = jnp.dot(flattened, key_weight, preferred_element_type=jnp.float32).astype(
        jnp.bfloat16
    )
    scale = 1.0 / math.sqrt(latent_queries.shape[1])
    scores = (
        lax.dot_general(
            key_rows, queries, (((1,), (1,)), ((), ())), preferred_element_type=jnp.float32
        )
        * scale
    )
    scores = jnp.where(tissue.reshape(-1, 1) > 0, scores, -1e30)
    shift = jnp.max(scores, axis=0, keepdims=True)
    chosen = jnp.exp(scores - shift)
    total = jnp.sum(chosen, axis=0, keepdims=True)
    pooled = lax.dot_general(
        flattened,
        chosen.astype(jnp.bfloat16),
        (((0,), (0,)), ((), ())),
        preferred_element_type=jnp.float32,
    )

    own_row = lax.axis_index("row")
    size = pooled.shape[1] // rows

    def block_of(step):
        start = ((own_row + step) % rows) * size
        cut = lambda array: lax.dynamic_slice_in_dim(array, start, size, axis=1)
        return cut(pooled), cut(shift), cut(total)

    arrived = [shifted(packed(*block_of(k)), "row", k) for k in range(1, rows)]
    partial = merged([block_of(0)] + [unpacked(block, channels) for block in arrived])
    bit = lax.axis_size("col") // 2
    while bit > 0:
        other = flipped(packed(*partial), "col", bit)
        partial = merged([partial, unpacked(other, channels)])
        bit //= 2
    normalized = (partial[0] / partial[2]).astype(jnp.bfloat16)
    return normalized


def gelu(value):
    return 0.5 * value * (1.0 + lax.erf(value * math.sqrt(0.5)))


def mark_kernel(features, tissue, queries, out, queries_out, features_held, tissue_held, done):
    copies = [
        pltpu.make_async_copy(tissue, tissue_held, done.at[0]),
        pltpu.make_async_copy(features, features_held, done.at[1]),
        pltpu.make_async_copy(queries, queries_out, done.at[2]),
    ]
    for copy in copies:
        copy.start()
    height, breadth, channels = features.shape
    copies[0].wait()
    line = lax.broadcasted_iota(jnp.int32, (breadth, breadth), 0)
    place = lax.broadcasted_iota(jnp.int32, (breadth, breadth), 1)
    flags = tissue_held[...].astype(jnp.float32)
    spread = [
        jnp.where(line == place, jnp.broadcast_to(flags[k : k + 1], line.shape), 0.0)
        for k in range(height)
    ]
    keep = jnp.dot(
        jnp.concatenate(spread, axis=0).astype(jnp.bfloat16),
        jnp.ones((breadth, channels), jnp.bfloat16),
        preferred_element_type=jnp.float32,
    )
    copies[1].wait()
    for k in range(height):
        out[k] = jnp.where(
            keep[k * breadth : (k + 1) * breadth] > 0.0, features_held[k].astype(jnp.float32), FAR
        ).astype(jnp.bfloat16)
    copies[2].wait()


def halve_kernel(own, other, out):
    half = own.shape[0] // 2
    core = lax.rem(lax.axis_index("col"), 2)
    start = pl.multiple_of(core * half, half)
    out[pl.ds(start, half), :] = own[pl.ds(start, half), :]
    out[pl.ds(pl.multiple_of((1 - core) * half, half), half), :] = other[pl.ds(start, half), :]


def conv_kernel(
    marked, top, bottom, paired, crossed, first, bias_first, second,
    mid, second_held, cells, taps, done,
):
    later = pltpu.make_async_copy(second, second_held, done)
    later.start()
    height, breadth, channels = marked.shape
    slot = (cells.shape[0] - 2 * EDGE - LEAD) // (height + 2 * HALO)
    flat = cells.shape[0] - 2 * EDGE
    row, col = lax.axis_index("row"), lax.axis_index("col")
    first_row, last_row = row == 0, row == lax.axis_size("row") - 1
    first_col, last_col = col == 0, col == lax.axis_size("col") - 1
    even = lax.rem(col, 2) == 0

    def put(line, place, values, outside):
        start = EDGE + LEAD + line * slot + place
        values = values.astype(jnp.float32)
        if outside is not None:
            values = jnp.where(outside, FAR, values)
        cells[start : start + values.shape[0], :] = values

    cells[...] = jnp.full(cells.shape, FAR, jnp.float32)
    for line in range(height):
        put(line + HALO, 0, marked[line], None)
    for line in range(HALO):
        put(line, 0, top[line], first_row)
        put(height + HALO + line, 0, bottom[line], last_row)
    for line in range(height + 2 * HALO):
        beyond_left, beyond_right = first_col, last_col
        if line < HALO:
            beyond_left, beyond_right = first_col | first_row, last_col | first_row
        if line >= height + HALO:
            beyond_left, beyond_right = first_col | last_row, last_col | last_row
        one, two = paired[line].astype(jnp.float32), crossed[line].astype(jnp.float32)
        put(line, -HALO, jnp.where(even, two, one), beyond_left)
        put(line, breadth, jnp.where(even, one, two), beyond_right)

    for shift in range(3):
        values = cells[EDGE - 1 + shift : EDGE - 1 + shift + flat, :]
        taps[:, shift * channels : (shift + 1) * channels] = jnp.where(
            values < FAR, values, 0.0
        ).astype(jnp.bfloat16)

    count = flat - 2 * slot
    summed = jnp.dot(taps[0:count, :], first[0], preferred_element_type=jnp.float32)
    for line in range(1, 3):
        summed = summed + jnp.dot(
            taps[line * slot : line * slot + count, :], first[line],
            preferred_element_type=jnp.float32,
        )
    alive = cells[EDGE + slot : EDGE + slot + count, :] < FAR
    edge = jnp.zeros((EDGE, channels), jnp.float32)
    mid[0:EDGE, :] = edge
    mid[EDGE + count : 2 * EDGE + count, :] = edge
    mid[EDGE : EDGE + count, :] = jnp.where(alive, gelu(summed + bias_first[...]), 0.0)
    later.wait()


def second_conv_kernel(marked, mid, second, bias_second, out, sent, taps):
    height, breadth, channels = marked.shape
    count = mid.shape[0] - 2 * EDGE
    slot = (count - LEAD) // (height + 2)
    for shift in range(3):
        taps[0:count, shift * channels : (shift + 1) * channels] = mid[
            EDGE - 1 + shift : EDGE - 1 + shift + count, :
        ].astype(jnp.bfloat16)
    inner = height * slot
    summed = jnp.dot(taps[LEAD : LEAD + inner, :], second[0], preferred_element_type=jnp.float32)
    for line in range(1, 3):
        summed = summed + jnp.dot(
            taps[LEAD + line * slot : LEAD + line * slot + inner, :], second[line],
            preferred_element_type=jnp.float32,
        )
    summed = summed.reshape(height, slot, channels)[:, :breadth].reshape(height * breadth, channels)
    alive = marked[...].reshape(height * breadth, channels) < FAR
    value = gelu(summed + bias_second[...])
    out[...] = jnp.where(alive, value, 0.0).astype(jnp.bfloat16)
    sent[...] = jnp.where(alive, value, FAR).astype(jnp.bfloat16)


def key_kernel(cells, weight, keys):
    keys[...] = jnp.dot(cells[...], weight[...], preferred_element_type=jnp.float32).astype(
        jnp.bfloat16
    )


def write_parts(block, values, top, total):
    channels = values.shape[0]
    parts = []
    for source, count in ((top, 3), (total, 2)):
        rest = source
        for _ in range(count):
            part = rest.astype(jnp.bfloat16).astype(jnp.float32)
            parts.append(part)
            rest = rest - part
    parts.append(jnp.zeros((block.shape[0] - channels - 5, values.shape[1]), jnp.float32))
    block[0:channels, :] = values.astype(jnp.bfloat16)
    block[channels:, :] = jnp.concatenate(parts, axis=0).astype(jnp.bfloat16)


def read_parts(block):
    channels = block.shape[0] - 16
    tail = block[channels:, :].astype(jnp.float32)
    row = lambda k: tail[k : k + 1]
    return (
        block[0:channels, :].astype(jnp.float32),
        row(0) + row(1) + row(2),
        row(3) + row(4),
    )


def read_whole(block):
    channels = block.shape[0] - 8
    tail = block[channels:, :]
    return block[0:channels, :], tail[0:1], tail[1:2]


def write_whole(block, values, top, total):
    channels = values.shape[0]
    block[0:channels, :] = values
    block[channels:, :] = jnp.concatenate(
        [top, total, jnp.zeros((6, values.shape[1]), jnp.float32)], axis=0
    )


PLACES = (0, 2, 1, 3)


def hold_queries(held, near, far, use_near):
    half = held.shape[0] // 8
    row = lax.axis_index("row")
    blocks = [
        (one, other, 2 * k * half)
        for one, other in zip(near, far)
        for k in range(one.shape[0] // (2 * half))
    ]
    for (one, other, start), place in zip(blocks, PLACES):
        for parity in range(2):
            source = slice(start + parity * half, start + (parity + 1) * half)
            target = pl.multiple_of(parity * 4 * half + (row ^ place) * half, half)
            held[pl.ds(target, half), :] = jnp.where(use_near, one[source, :], other[source, :])


def masked_scores(queries, marked, keys):
    scale = 1.0 / math.sqrt(queries.shape[1])
    raw = lax.dot_general(
        keys[...], queries[...], (((1,), (1,)), ((), ())), preferred_element_type=jnp.float32
    )
    return jnp.where(marked[:, : raw.shape[1]] < FAR, raw * scale, -1e30)


def score_blocks(scores, sides):
    top = jnp.maximum(*[jnp.max(part, axis=0, keepdims=True) for part in scores])
    pooled = total = 0.0
    for part, cells in zip(scores, sides):
        chosen = jnp.exp(part - top)
        total = total + jnp.sum(chosen, axis=0, keepdims=True)
        pooled = pooled + lax.dot_general(
            cells[...], chosen.astype(jnp.bfloat16), (((0,), (0,)), ((), ())),
            preferred_element_type=jnp.float32,
        )
    channels, lanes = pooled.shape[0] // 2, pooled.shape[1]
    turn = lambda array: pltpu.roll(array, lanes // 2, 1)
    lower = lambda rows: lax.broadcasted_iota(jnp.int32, (rows, lanes), 1) < lanes // 2
    tall, flat = lower(channels), lower(1)
    turned, turned_top, turned_total = turn(pooled), turn(top), turn(total)
    return (
        (
            jnp.where(tall, pooled[:channels], turned[channels:]),
            jnp.where(flat, top, turned_top),
            jnp.where(flat, total, turned_total),
        ),
        (
            jnp.where(tall, turned[:channels], pooled[channels:]),
            jnp.where(flat, turned_top, top),
            jnp.where(flat, turned_total, total),
        ),
    )


def other_kernel(other_sent, weight, other, keys):
    values = other_sent[...].astype(jnp.float32)
    other[...] = jnp.where(values < FAR, values, 0.0).astype(jnp.bfloat16)
    key_kernel(other, weight, keys)


def first_score_kernel(own, own_sent, own_keys, other, other_sent, other_keys, *refs):
    *queries, send_2, send_3, held, blocks = refs
    row, across = lax.axis_index("row"), lax.axis_index("col") // 2
    hold_queries(held, queries[:3], queries[3:], row // 2 != across)
    scores = masked_scores(held, own_sent, own_keys), masked_scores(held, other_sent, other_keys)
    for parity, block in enumerate(score_blocks(scores, (own, other))):
        write_whole(blocks.at[parity], *block)
    odd = lax.rem(row, 2)
    write_parts(send_2, *read_whole(blocks.at[odd]))
    write_parts(send_3, *read_whole(blocks.at[1 - odd]))


def last_score_kernel(own, own_sent, own_keys, other, other_sent, other_keys, *refs):
    *queries, kept, send_1, held, blocks = refs
    row, across = lax.axis_index("row"), lax.axis_index("col") // 2
    hold_queries(held, queries[:3], queries[3:], row // 2 == across)
    scores = masked_scores(held, own_sent, own_keys), masked_scores(held, other_sent, other_keys)
    for parity, block in enumerate(score_blocks(scores, (own, other))):
        write_whole(blocks.at[parity], *block)
    odd = lax.rem(row, 2)
    kept[...] = blocks[odd]
    write_parts(send_1, *read_whole(blocks.at[1 - odd]))


def merge_kernel(own, *refs):
    *arrived, whole, packed_out = refs
    values, top, total = merged([read_whole(own)] + [read_parts(block) for block in arrived])
    write_whole(whole, values, top, total)
    write_parts(packed_out, values, top, total)


def normalize_kernel(own, arrived, out):
    values, _, total = merged([read_whole(own), read_parts(arrived)])
    out[...] = (values / total).astype(jnp.bfloat16)


def attend_kernel(normalized, value_weight, attended):
    lanes = normalized.shape[1] // 2
    values = normalized[...].astype(jnp.float32)
    tall = jnp.concatenate([values, pltpu.roll(values, lanes, 1)], axis=0).astype(jnp.bfloat16)
    attended[...] = lax.dot_general(
        tall, value_weight[...], (((0,), (0,)), ((), ())), preferred_element_type=jnp.float32
    )[:lanes].astype(jnp.bfloat16)


def finish_kernel(mine, arrived, value_weight, out_weight, out, other, attended):
    attend_kernel(arrived, value_weight, other)
    core = lax.rem(lax.axis_index("col"), 2)
    piece = mine.shape[0] // 4
    for place in range(4):
        source = slice(place * piece, (place + 1) * piece)
        first = pl.multiple_of((2 * place + core) * piece, piece)
        last = pl.multiple_of((2 * place + 1 - core) * piece, piece)
        attended[pl.ds(first, piece), :] = mine[source]
        attended[pl.ds(last, piece), :] = other[source]
    out[...] = lax.dot_general(
        out_weight[...], attended[...], (((1,), (1,)), ((), ())),
        preferred_element_type=jnp.float32,
    ).astype(out.dtype)


MIB = 1 << 20


def call(kernel, outs, args, scratch=(), limit=4, flops=0, far=()):
    held = pl.BlockSpec(memory_space=pltpu.VMEM)
    outside = pl.BlockSpec(memory_space=pltpu.HBM)
    return pl.pallas_call(
        kernel,
        out_shape=[pltpu.VMEM(shape, dtype) for shape, dtype in outs],
        in_specs=[outside if k in far else held for k in range(len(args))],
        out_specs=[held] * len(outs),
        scratch_shapes=[pltpu.VMEM(*kind) if isinstance(kind, tuple) else kind for kind in scratch],
        compiler_params=pltpu.CompilerParams(vmem_limit_bytes=limit * MIB),
        cost_estimate=pl.CostEstimate(flops=flops, bytes_accessed=0, transcendentals=0),
    )(
        *[
            pltpu.with_memory_space_constraint(arg, pltpu.HBM if k in far else pltpu.VMEM)
            for k, arg in enumerate(args)
        ]
    )


def kernel_path(
    features, tissue, conv_first, bias_first, conv_second, bias_second, key_weight,
    value_weight, latent_queries, out_weight,
):
    height, breadth, channels = features.shape
    col, cols = lax.axis_index("col"), lax.axis_size("col")
    size, width = latent_queries.shape
    cells = height * breadth
    slot = -(-(breadth + 2 * HALO) // 16) * 16
    flat = LEAD + (height + 2 * HALO) * slot
    count = flat - 2 * slot
    wide, half = jnp.float32, jnp.bfloat16
    block = 4 * size
    whole_block, sent_block = (channels // 2 + 8, block), (channels // 2 + 16, block)
    score_flops = 4 * cells * block * (width + channels)

    beside = flipped(latent_queries, "col", 1)
    marked, queries = call(
        mark_kernel, [(features.shape, half), ((size, width), half)],
        [features, tissue, latent_queries],
        [(features.shape, half), (tissue.shape, jnp.int32), pltpu.SemaphoreType.DMA((3,))],
        far=(0, 1, 2), flops=1 << 20,
    )
    (queries,) = call(halve_kernel, [((size, width), half)], [queries, beside])
    two = flipped(queries, "row", 2)
    top = shifted(marked[height - HALO :], "row", 1)
    bottom = shifted(marked[:HALO], "row", -1)
    one = flipped(queries, "row", 1)
    three = flipped(queries, "row", 3)
    far_queries = flipped(queries, "col", 2)

    sides = slice(breadth - HALO, breadth), slice(0, HALO)
    middles = [marked[:, cut] for cut in sides]
    even = lax.rem(col, 2) == 0
    ends = [
        jnp.concatenate([top[:, cut], middle, bottom[:, cut]], axis=0)
        for cut, middle in zip(sides, middles)
    ]
    paired = flipped(jnp.where(even, *ends), "col", 1)
    rounds = [(k, (k + 1 if k % 2 else k - 1) % cols) for k in range(cols)]
    crossed = lax.ppermute(jnp.where(even, *ends[::-1]), "col", rounds)

    rest = jnp.concatenate([one, three], axis=0)
    far_two = flipped(two, "col", 2)
    far_rest = flipped(rest, "col", 2)

    mid, weight = call(
        conv_kernel,
        [((count + 2 * EDGE, channels), wide), ((3, 3 * channels, channels), half)],
        [
            marked, top, bottom, paired, crossed,
            conv_first.reshape(3, 3 * channels, channels), bias_first.reshape(1, channels),
            conv_second.reshape(3, 3 * channels, channels),
        ],
        [
            ((flat + 2 * EDGE, channels), wide),
            ((flat, 3 * channels), half),
            pltpu.SemaphoreType.DMA,
        ],
        limit=12, far=(7,), flops=21 * cells * channels * channels,
    )
    own, own_sent = call(
        second_conv_kernel, [((cells, channels), half)] * 2,
        [marked, mid, weight, bias_second.reshape(1, channels)],
        [((count, 3 * channels), half)],
        limit=10, flops=18 * cells * channels * channels,
    )
    other_sent = flipped(own_sent, "col", 1)
    (own_keys,) = call(
        key_kernel, [((cells, width), half)], [own, key_weight],
        limit=4, flops=2 * cells * width * channels,
    )
    all_queries = [queries, two, rest, far_queries, far_two, far_rest]
    score_scratch = [((block, width), half), ((2,) + whole_block, wide)]
    other, other_keys = call(
        other_kernel, [((cells, channels), half), ((cells, width), half)],
        [other_sent, key_weight], limit=4, flops=2 * cells * channels * width,
    )
    send_2, send_3 = call(
        first_score_kernel, [(sent_block, half)] * 2,
        [own, own_sent, own_keys, other, other_sent, other_keys, *all_queries],
        score_scratch, limit=8, flops=score_flops,
    )
    arrived_2, arrived_3 = flipped(send_2, "row", 2), flipped(send_3, "row", 3)
    kept, send_1 = call(
        last_score_kernel, [(whole_block, wide), (sent_block, half)],
        [own, own_sent, own_keys, other, other_sent, other_keys, *all_queries],
        score_scratch, limit=8, flops=score_flops,
    )
    arrived_1 = flipped(send_1, "row", 1)
    kept, sent = call(
        merge_kernel, [(whole_block, wide), (sent_block, half)],
        [kept, arrived_1, arrived_2, arrived_3],
    )
    arrived = flipped(sent, "col", 2)
    (normalized,) = call(normalize_kernel, [((channels // 2, block), half)], [kept, arrived])
    arrived = flipped(normalized, "col", 1)
    (attended,) = call(
        attend_kernel, [((2 * size, width), half)], [normalized, value_weight],
        flops=8 * size * channels * width,
    )
    held = pl.BlockSpec(memory_space=pltpu.VMEM)
    keep = lambda array: pltpu.with_memory_space_constraint(array, pltpu.VMEM)
    return pl.pallas_call(
        finish_kernel,
        out_shape=jax.ShapeDtypeStruct((out_weight.shape[1], block), half),
        in_specs=[held] * 4,
        out_specs=held,
        scratch_shapes=[pltpu.VMEM((2 * size, width), half), pltpu.VMEM((block, width), half)],
        compiler_params=pltpu.CompilerParams(vmem_limit_bytes=6 * MIB),
        name="fn",
    )(keep(attended), keep(arrived), keep(value_weight), keep(out_weight.T)).T


def shards(
    features, tissue, conv_first, bias_first, conv_second, bias_second, key_weight,
    value_weight, latent_queries, out_weight,
):
    rows, cols = lax.axis_size("row"), lax.axis_size("col")
    if rows == cols == 4 and rows * latent_queries.shape[0] == 128:
        return kernel_path(
            features, tissue, conv_first, bias_first, conv_second, bias_second, key_weight,
            value_weight, latent_queries, out_weight,
        )
    marked = jnp.where(tissue[:, :, None] > 0, features, jnp.asarray(FAR, features.dtype))
    marked = with_halo(with_halo(marked, "row", 0), "col", 1)
    normalized = plain_attend(
        features, tissue, marked, latent_queries,
        (conv_first, bias_first, conv_second, bias_second, key_weight),
    )
    attended = lax.dot_general(
        normalized, value_weight, (((0,), (0,)), ((), ())), preferred_element_type=jnp.float32
    ).astype(jnp.bfloat16)
    return jnp.dot(attended, out_weight, preferred_element_type=jnp.float32).astype(jnp.bfloat16)


def solution(mesh):
    placed = (
        P(("groups", "row"), "col", None),
        P(("groups", "row"), "col"),
        P(),
        P(),
        P(),
        P(),
        P(),
        P(),
        P(("col", "row"), None),
        P(None, "col"),
    )
    return jax.shard_map(
        shards, mesh=mesh, in_specs=placed, out_specs=P(("groups", "row"), "col"), check_vma=False
    )
```

```python
import math

import jax
import jax.numpy as jnp
from jax import lax
from jax.experimental import pallas as pl
from jax.experimental.pallas import tpu as pltpu
from jax.sharding import PartitionSpec as P


HALO = 2
FAR = float("inf")
EDGE = 8
LEAD = 16


def shifted(array, axis, step):
    count = lax.axis_size(axis)
    return lax.ppermute(array, axis, [(i, (i + step) % count) for i in range(count)])


def flipped(array, axis, bit):
    count = lax.axis_size(axis)
    return lax.ppermute(array, axis, [(i, i ^ bit) for i in range(count)])


def with_halo(cells, axis, dim):
    size = cells.shape[dim]
    index, last = lax.axis_index(axis), lax.axis_size(axis) - 1
    before = shifted(lax.slice_in_dim(cells, size - HALO, size, axis=dim), axis, 1)
    after = shifted(lax.slice_in_dim(cells, 0, HALO, axis=dim), axis, -1)
    far = jnp.asarray(FAR, cells.dtype)
    return jnp.concatenate(
        [jnp.where(index == 0, far, before), cells, jnp.where(index == last, far, after)], axis=dim
    )


def convolve_valid(padded, weight):
    height, breadth = padded.shape[0] - 2, padded.shape[1] - 2
    channels = padded.shape[2]
    summed = jnp.zeros((height * breadth, weight.shape[3]), jnp.float32)
    for offset_row in range(3):
        for offset_col in range(3):
            window = padded[offset_row : offset_row + height, offset_col : offset_col + breadth]
            summed = summed + jnp.dot(
                window.reshape(height * breadth, channels),
                weight[offset_row, offset_col],
                preferred_element_type=jnp.float32,
            )
    return summed.reshape(height, breadth, weight.shape[3])


def rotated(parts, offset, step):
    count = len(parts)
    size = parts[0].shape[0]
    ordered = [parts[(step * k) % count] for k in range(count)]
    twice = jnp.concatenate(ordered + ordered[:-1], axis=0)
    return lax.dynamic_slice_in_dim(twice, ((count - offset) % count) * size, count * size, axis=0)


def gathered_queries(latent_queries):
    rows, cols = lax.axis_size("row"), lax.axis_size("col")
    parts = [latent_queries] + [shifted(latent_queries, "row", k) for k in range(1, rows)]
    queries = rotated(parts, lax.axis_index("row"), -1)
    own = lax.axis_index("col")
    bit = cols // 2
    groups = [queries]
    order = [0]
    while bit > 0:
        groups = groups + list(flipped(jnp.concatenate(groups, axis=0), "col", bit).reshape(len(groups), -1, queries.shape[1]))
        order = order + [place ^ bit for place in order]
        bit //= 2
    stacked = jnp.stack(groups)
    place = jnp.asarray([order.index(k) for k in range(cols)], jnp.int32)
    return stacked[place[own ^ jnp.arange(cols)]].reshape(-1, queries.shape[1])


def in_parts(values, count):
    parts = []
    for _ in range(count):
        part = lax.reduce_precision(values, exponent_bits=8, mantissa_bits=7)
        parts.append(part.astype(jnp.bfloat16))
        values = values - part
    return parts


def packed(pooled, top, total):
    rest = jnp.zeros((11, pooled.shape[1]), jnp.bfloat16)
    return jnp.concatenate(
        [pooled.astype(jnp.bfloat16)] + in_parts(top, 3) + in_parts(total, 2) + [rest], axis=0
    )


def unpacked(block, channels):
    wide = block.astype(jnp.float32)
    row = lambda k: wide[channels + k : channels + k + 1]
    return wide[:channels], row(0) + row(1) + row(2), row(3) + row(4)


def merged(partials):
    top = partials[0][1]
    for _, other, _ in partials[1:]:
        top = jnp.maximum(top, other)
    pooled = total = 0.0
    for part, shift, count in partials:
        factor = jnp.exp(shift - top)
        pooled = pooled + part * factor
        total = total + count * factor
    return pooled, top, total


def plain_attend(features, tissue, marked, latent_queries, weights):
    conv_first, bias_first, conv_second, bias_second, key_weight = weights
    height, breadth, channels = features.shape
    rows = lax.axis_size("row")
    queries = gathered_queries(latent_queries)
    alive = marked < FAR
    inputs = jnp.where(alive, marked, jnp.zeros_like(marked))
    hidden = jax.nn.gelu(convolve_valid(inputs, conv_first) + bias_first, approximate=False)
    hidden = jnp.where(alive[1:-1, 1:-1], hidden, 0.0).astype(jnp.bfloat16)
    second = jax.nn.gelu(convolve_valid(hidden, conv_second) + bias_second, approximate=False)
    second = jnp.where(alive[HALO:-HALO, HALO:-HALO], second, 0.0).astype(jnp.bfloat16)
    flattened = second.reshape(height * breadth, channels)
    key_rows = jnp.dot(flattened, key_weight, preferred_element_type=jnp.float32).astype(
        jnp.bfloat16
    )
    scale = 1.0 / math.sqrt(latent_queries.shape[1])
    scores = (
        lax.dot_general(
            key_rows, queries, (((1,), (1,)), ((), ())), preferred_element_type=jnp.float32
        )
        * scale
    )
    scores = jnp.where(tissue.reshape(-1, 1) > 0, scores, -1e30)
    shift = jnp.max(scores, axis=0, keepdims=True)
    chosen = jnp.exp(scores - shift)
    total = jnp.sum(chosen, axis=0, keepdims=True)
    pooled = lax.dot_general(
        flattened,
        chosen.astype(jnp.bfloat16),
        (((0,), (0,)), ((), ())),
        preferred_element_type=jnp.float32,
    )

    own_row = lax.axis_index("row")
    size = pooled.shape[1] // rows

    def block_of(step):
        start = ((own_row + step) % rows) * size
        cut = lambda array: lax.dynamic_slice_in_dim(array, start, size, axis=1)
        return cut(pooled), cut(shift), cut(total)

    arrived = [shifted(packed(*block_of(k)), "row", k) for k in range(1, rows)]
    partial = merged([block_of(0)] + [unpacked(block, channels) for block in arrived])
    bit = lax.axis_size("col") // 2
    while bit > 0:
        other = flipped(packed(*partial), "col", bit)
        partial = merged([partial, unpacked(other, channels)])
        bit //= 2
    normalized = (partial[0] / partial[2]).astype(jnp.bfloat16)
    return normalized


def gelu(value):
    return 0.5 * value * (1.0 + lax.erf(value * math.sqrt(0.5)))


def mark_kernel(
    features, tissue, queries, weight, bias,
    out, queries_out, weight_out, bias_out, features_held, tissue_held, done,
):
    copies = [
        pltpu.make_async_copy(tissue, tissue_held, done.at[0]),
        pltpu.make_async_copy(features, features_held, done.at[1]),
        pltpu.make_async_copy(queries, queries_out, done.at[2]),
        pltpu.make_async_copy(bias, bias_out, done.at[3]),
        pltpu.make_async_copy(weight, weight_out, done.at[4]),
    ]
    for copy in copies:
        copy.start()
    height, breadth, channels = features.shape
    copies[0].wait()
    line = lax.broadcasted_iota(jnp.int32, (breadth, breadth), 0)
    place = lax.broadcasted_iota(jnp.int32, (breadth, breadth), 1)
    flags = tissue_held[...].astype(jnp.float32)
    spread = [
        jnp.where(line == place, jnp.broadcast_to(flags[k : k + 1], line.shape), 0.0)
        for k in range(height)
    ]
    keep = jnp.dot(
        jnp.concatenate(spread, axis=0).astype(jnp.bfloat16),
        jnp.ones((breadth, channels), jnp.bfloat16),
        preferred_element_type=jnp.float32,
    )
    copies[1].wait()
    for k in range(height):
        out[k] = jnp.where(
            keep[k * breadth : (k + 1) * breadth] > 0.0, features_held[k].astype(jnp.float32), FAR
        ).astype(jnp.bfloat16)
    for copy in copies[2:]:
        copy.wait()


def halve_kernel(own, other, out):
    half = own.shape[0] // 2
    core = lax.rem(lax.axis_index("col"), 2)
    start = pl.multiple_of(core * half, half)
    out[pl.ds(start, half), :] = own[pl.ds(start, half), :]
    out[pl.ds(pl.multiple_of((1 - core) * half, half), half), :] = other[pl.ds(start, half), :]


def conv_kernel(
    marked, top, bottom, paired, crossed, first, bias_first, second,
    mid, second_held, cells, taps, done,
):
    later = pltpu.make_async_copy(second, second_held, done)
    later.start()
    height, breadth, channels = marked.shape
    slot = (cells.shape[0] - 2 * EDGE - LEAD) // (height + 2 * HALO)
    flat = cells.shape[0] - 2 * EDGE
    row, col = lax.axis_index("row"), lax.axis_index("col")
    first_row, last_row = row == 0, row == lax.axis_size("row") - 1
    first_col, last_col = col == 0, col == lax.axis_size("col") - 1
    even = lax.rem(col, 2) == 0

    def put(line, place, values, outside):
        start = EDGE + LEAD + line * slot + place
        values = values.astype(jnp.float32)
        if outside is not None:
            values = jnp.where(outside, FAR, values)
        cells[start : start + values.shape[0], :] = values

    cells[...] = jnp.full(cells.shape, FAR, jnp.float32)
    for line in range(height):
        put(line + HALO, 0, marked[line], None)
    for line in range(HALO):
        put(line, 0, top[line], first_row)
        put(height + HALO + line, 0, bottom[line], last_row)
    for line in range(height + 2 * HALO):
        beyond_left, beyond_right = first_col, last_col
        if line < HALO:
            beyond_left, beyond_right = first_col | first_row, last_col | first_row
        if line >= height + HALO:
            beyond_left, beyond_right = first_col | last_row, last_col | last_row
        one, two = paired[line].astype(jnp.float32), crossed[line].astype(jnp.float32)
        put(line, -HALO, jnp.where(even, two, one), beyond_left)
        put(line, breadth, jnp.where(even, one, two), beyond_right)

    for shift in range(3):
        values = cells[EDGE - 1 + shift : EDGE - 1 + shift + flat, :]
        taps[:, shift * channels : (shift + 1) * channels] = jnp.where(
            values < FAR, values, 0.0
        ).astype(jnp.bfloat16)

    count = flat - 2 * slot
    summed = jnp.dot(taps[0:count, :], first[0], preferred_element_type=jnp.float32)
    for line in range(1, 3):
        summed = summed + jnp.dot(
            taps[line * slot : line * slot + count, :], first[line],
            preferred_element_type=jnp.float32,
        )
    alive = cells[EDGE + slot : EDGE + slot + count, :] < FAR
    edge = jnp.zeros((EDGE, channels), jnp.float32)
    mid[0:EDGE, :] = edge
    mid[EDGE + count : 2 * EDGE + count, :] = edge
    mid[EDGE : EDGE + count, :] = jnp.where(alive, gelu(summed + bias_first[...]), 0.0)
    later.wait()


def second_conv_kernel(marked, mid, second, bias_second, out, sent, taps):
    height, breadth, channels = marked.shape
    count = mid.shape[0] - 2 * EDGE
    slot = (count - LEAD) // (height + 2)
    for shift in range(3):
        taps[0:count, shift * channels : (shift + 1) * channels] = mid[
            EDGE - 1 + shift : EDGE - 1 + shift + count, :
        ].astype(jnp.bfloat16)
    inner = height * slot
    summed = jnp.dot(taps[LEAD : LEAD + inner, :], second[0], preferred_element_type=jnp.float32)
    for line in range(1, 3):
        summed = summed + jnp.dot(
            taps[LEAD + line * slot : LEAD + line * slot + inner, :], second[line],
            preferred_element_type=jnp.float32,
        )
    summed = summed.reshape(height, slot, channels)[:, :breadth].reshape(height * breadth, channels)
    alive = marked[...].reshape(height * breadth, channels) < FAR
    value = gelu(summed + bias_second[...])
    out[...] = jnp.where(alive, value, 0.0).astype(jnp.bfloat16)
    sent[...] = jnp.where(alive, value, FAR).astype(jnp.bfloat16)


def key_kernel(cells, weight, keys):
    keys[...] = jnp.dot(cells[...], weight[...], preferred_element_type=jnp.float32).astype(
        jnp.bfloat16
    )


def write_parts(block, values, top, total):
    channels = values.shape[0]
    parts = []
    for source, count in ((top, 3), (total, 2)):
        rest = source
        for _ in range(count):
            part = rest.astype(jnp.bfloat16).astype(jnp.float32)
            parts.append(part)
            rest = rest - part
    parts.append(jnp.zeros((block.shape[0] - channels - 5, values.shape[1]), jnp.float32))
    block[0:channels, :] = values.astype(jnp.bfloat16)
    block[channels:, :] = jnp.concatenate(parts, axis=0).astype(jnp.bfloat16)


def read_parts(block):
    channels = block.shape[0] - 16
    tail = block[channels:, :].astype(jnp.float32)
    row = lambda k: tail[k : k + 1]
    return (
        block[0:channels, :].astype(jnp.float32),
        row(0) + row(1) + row(2),
        row(3) + row(4),
    )


def read_whole(block):
    channels = block.shape[0] - 8
    tail = block[channels:, :]
    return block[0:channels, :], tail[0:1], tail[1:2]


def write_whole(block, values, top, total):
    channels = values.shape[0]
    block[0:channels, :] = values
    block[channels:, :] = jnp.concatenate(
        [top, total, jnp.zeros((6, values.shape[1]), jnp.float32)], axis=0
    )


PLACES = (0, 2, 1, 3)


def hold_queries(held, near, far, use_near):
    half = held.shape[0] // 8
    row = lax.axis_index("row")
    blocks = [
        (one, other, 2 * k * half)
        for one, other in zip(near, far)
        for k in range(one.shape[0] // (2 * half))
    ]
    for (one, other, start), place in zip(blocks, PLACES):
        for parity in range(2):
            source = slice(start + parity * half, start + (parity + 1) * half)
            target = pl.multiple_of(parity * 4 * half + (row ^ place) * half, half)
            held[pl.ds(target, half), :] = jnp.where(use_near, one[source, :], other[source, :])


def masked_scores(queries, marked, keys):
    scale = 1.0 / math.sqrt(queries.shape[1])
    raw = lax.dot_general(
        keys[...], queries[...], (((1,), (1,)), ((), ())), preferred_element_type=jnp.float32
    )
    return jnp.where(marked[:, : raw.shape[1]] < FAR, raw * scale, -1e30)


def score_blocks(scores, sides):
    top = jnp.maximum(*[jnp.max(part, axis=0, keepdims=True) for part in scores])
    pooled = total = 0.0
    for part, cells in zip(scores, sides):
        chosen = jnp.exp(part - top)
        total = total + jnp.sum(chosen, axis=0, keepdims=True)
        pooled = pooled + lax.dot_general(
            cells[...], chosen.astype(jnp.bfloat16), (((0,), (0,)), ((), ())),
            preferred_element_type=jnp.float32,
        )
    channels, lanes = pooled.shape[0] // 2, pooled.shape[1]
    turn = lambda array: pltpu.roll(array, lanes // 2, 1)
    lower = lambda rows: lax.broadcasted_iota(jnp.int32, (rows, lanes), 1) < lanes // 2
    tall, flat = lower(channels), lower(1)
    turned, turned_top, turned_total = turn(pooled), turn(top), turn(total)
    return (
        (
            jnp.where(tall, pooled[:channels], turned[channels:]),
            jnp.where(flat, top, turned_top),
            jnp.where(flat, total, turned_total),
        ),
        (
            jnp.where(tall, turned[:channels], pooled[channels:]),
            jnp.where(flat, turned_top, top),
            jnp.where(flat, turned_total, total),
        ),
    )


def other_kernel(other_sent, weight, other, keys):
    values = other_sent[...].astype(jnp.float32)
    other[...] = jnp.where(values < FAR, values, 0.0).astype(jnp.bfloat16)
    key_kernel(other, weight, keys)


def first_score_kernel(own, own_sent, own_keys, other, other_sent, other_keys, *refs):
    *queries, send_2, send_3, held, blocks = refs
    row, across = lax.axis_index("row"), lax.axis_index("col") // 2
    hold_queries(held, queries[:3], queries[3:], row // 2 != across)
    scores = masked_scores(held, own_sent, own_keys), masked_scores(held, other_sent, other_keys)
    for parity, block in enumerate(score_blocks(scores, (own, other))):
        write_whole(blocks.at[parity], *block)
    odd = lax.rem(row, 2)
    write_parts(send_2, *read_whole(blocks.at[odd]))
    write_parts(send_3, *read_whole(blocks.at[1 - odd]))


def last_score_kernel(own, own_sent, own_keys, other, other_sent, other_keys, *refs):
    *queries, kept, send_1, held, blocks = refs
    row, across = lax.axis_index("row"), lax.axis_index("col") // 2
    hold_queries(held, queries[:3], queries[3:], row // 2 == across)
    scores = masked_scores(held, own_sent, own_keys), masked_scores(held, other_sent, other_keys)
    for parity, block in enumerate(score_blocks(scores, (own, other))):
        write_whole(blocks.at[parity], *block)
    odd = lax.rem(row, 2)
    kept[...] = blocks[odd]
    write_parts(send_1, *read_whole(blocks.at[1 - odd]))


def merge_kernel(own, *refs):
    *arrived, whole, packed_out = refs
    values, top, total = merged([read_whole(own)] + [read_parts(block) for block in arrived])
    write_whole(whole, values, top, total)
    write_parts(packed_out, values, top, total)


def normalize_kernel(own, arrived, out):
    values, _, total = merged([read_whole(own), read_parts(arrived)])
    out[...] = (values / total).astype(jnp.bfloat16)


def attend_kernel(normalized, value_weight, attended):
    lanes = normalized.shape[1] // 2
    values = normalized[...].astype(jnp.float32)
    tall = jnp.concatenate([values, pltpu.roll(values, lanes, 1)], axis=0).astype(jnp.bfloat16)
    attended[...] = lax.dot_general(
        tall, value_weight[...], (((0,), (0,)), ((), ())), preferred_element_type=jnp.float32
    )[:lanes].astype(jnp.bfloat16)


def finish_kernel(mine, arrived, value_weight, out_weight, out, other, attended):
    attend_kernel(arrived, value_weight, other)
    core = lax.rem(lax.axis_index("col"), 2)
    piece = mine.shape[0] // 4
    for place in range(4):
        source = slice(place * piece, (place + 1) * piece)
        first = pl.multiple_of((2 * place + core) * piece, piece)
        last = pl.multiple_of((2 * place + 1 - core) * piece, piece)
        attended[pl.ds(first, piece), :] = mine[source]
        attended[pl.ds(last, piece), :] = other[source]
    out[...] = lax.dot_general(
        out_weight[...], attended[...], (((1,), (1,)), ((), ())),
        preferred_element_type=jnp.float32,
    ).astype(out.dtype)


MIB = 1 << 20


def call(kernel, outs, args, scratch=(), limit=4, flops=0, far=()):
    held = pl.BlockSpec(memory_space=pltpu.VMEM)
    outside = pl.BlockSpec(memory_space=pltpu.HBM)
    return pl.pallas_call(
        kernel,
        out_shape=[pltpu.VMEM(shape, dtype) for shape, dtype in outs],
        in_specs=[outside if k in far else held for k in range(len(args))],
        out_specs=[held] * len(outs),
        scratch_shapes=[pltpu.VMEM(*kind) if isinstance(kind, tuple) else kind for kind in scratch],
        compiler_params=pltpu.CompilerParams(vmem_limit_bytes=limit * MIB),
        cost_estimate=pl.CostEstimate(flops=flops, bytes_accessed=0, transcendentals=0),
    )(
        *[
            pltpu.with_memory_space_constraint(arg, pltpu.HBM if k in far else pltpu.VMEM)
            for k, arg in enumerate(args)
        ]
    )


def kernel_path(
    features, tissue, conv_first, bias_first, conv_second, bias_second, key_weight,
    value_weight, latent_queries, out_weight,
):
    height, breadth, channels = features.shape
    col, cols = lax.axis_index("col"), lax.axis_size("col")
    size, width = latent_queries.shape
    cells = height * breadth
    slot = -(-(breadth + 2 * HALO) // 16) * 16
    flat = LEAD + (height + 2 * HALO) * slot
    count = flat - 2 * slot
    wide, half = jnp.float32, jnp.bfloat16
    block = 4 * size
    whole_block, sent_block = (channels // 2 + 8, block), (channels // 2 + 16, block)
    score_flops = 4 * cells * block * (width + channels)

    beside = flipped(latent_queries, "col", 1)
    weight_shape = (3, 3 * channels, channels)
    marked, queries, first_weight, first_bias = call(
        mark_kernel,
        [(features.shape, half), ((size, width), half), (weight_shape, half), ((1, channels), wide)],
        [
            features, tissue, latent_queries,
            conv_first.reshape(weight_shape), bias_first.reshape(1, channels),
        ],
        [(features.shape, half), (tissue.shape, jnp.int32), pltpu.SemaphoreType.DMA((5,))],
        limit=6, far=(0, 1, 2, 3, 4), flops=1 << 20,
    )
    (queries,) = call(halve_kernel, [((size, width), half)], [queries, beside])
    two = flipped(queries, "row", 2)
    top = shifted(marked[height - HALO :], "row", 1)
    bottom = shifted(marked[:HALO], "row", -1)
    one = flipped(queries, "row", 1)
    three = flipped(queries, "row", 3)
    far_queries = flipped(queries, "col", 2)

    sides = slice(breadth - HALO, breadth), slice(0, HALO)
    middles = [marked[:, cut] for cut in sides]
    even = lax.rem(col, 2) == 0
    ends = [
        jnp.concatenate([top[:, cut], middle, bottom[:, cut]], axis=0)
        for cut, middle in zip(sides, middles)
    ]
    paired = flipped(jnp.where(even, *ends), "col", 1)
    rounds = [(k, (k + 1 if k % 2 else k - 1) % cols) for k in range(cols)]
    crossed = lax.ppermute(jnp.where(even, *ends[::-1]), "col", rounds)

    rest = jnp.concatenate([one, three], axis=0)
    far_two = flipped(two, "col", 2)
    far_rest = flipped(rest, "col", 2)

    mid, weight = call(
        conv_kernel,
        [((count + 2 * EDGE, channels), wide), ((3, 3 * channels, channels), half)],
        [
            marked, top, bottom, paired, crossed,
            first_weight, first_bias,
            conv_second.reshape(3, 3 * channels, channels),
        ],
        [
            ((flat + 2 * EDGE, channels), wide),
            ((flat, 3 * channels), half),
            pltpu.SemaphoreType.DMA,
        ],
        limit=12, far=(7,), flops=21 * cells * channels * channels,
    )
    own, own_sent = call(
        second_conv_kernel, [((cells, channels), half)] * 2,
        [marked, mid, weight, bias_second.reshape(1, channels)],
        [((count, 3 * channels), half)],
        limit=10, flops=18 * cells * channels * channels,
    )
    other_sent = flipped(own_sent, "col", 1)
    (own_keys,) = call(
        key_kernel, [((cells, width), half)], [own, key_weight],
        limit=4, flops=2 * cells * width * channels,
    )
    all_queries = [queries, two, rest, far_queries, far_two, far_rest]
    score_scratch = [((block, width), half), ((2,) + whole_block, wide)]
    other, other_keys = call(
        other_kernel, [((cells, channels), half), ((cells, width), half)],
        [other_sent, key_weight], limit=4, flops=2 * cells * channels * width,
    )
    send_2, send_3 = call(
        first_score_kernel, [(sent_block, half)] * 2,
        [own, own_sent, own_keys, other, other_sent, other_keys, *all_queries],
        score_scratch, limit=8, flops=score_flops,
    )
    arrived_2, arrived_3 = flipped(send_2, "row", 2), flipped(send_3, "row", 3)
    kept, send_1 = call(
        last_score_kernel, [(whole_block, wide), (sent_block, half)],
        [own, own_sent, own_keys, other, other_sent, other_keys, *all_queries],
        score_scratch, limit=8, flops=score_flops,
    )
    arrived_1 = flipped(send_1, "row", 1)
    kept, sent = call(
        merge_kernel, [(whole_block, wide), (sent_block, half)],
        [kept, arrived_1, arrived_2, arrived_3],
    )
    arrived = flipped(sent, "col", 2)
    (normalized,) = call(normalize_kernel, [((channels // 2, block), half)], [kept, arrived])
    arrived = flipped(normalized, "col", 1)
    (attended,) = call(
        attend_kernel, [((2 * size, width), half)], [normalized, value_weight],
        flops=8 * size * channels * width,
    )
    held = pl.BlockSpec(memory_space=pltpu.VMEM)
    keep = lambda array: pltpu.with_memory_space_constraint(array, pltpu.VMEM)
    return pl.pallas_call(
        finish_kernel,
        out_shape=jax.ShapeDtypeStruct((out_weight.shape[1], block), half),
        in_specs=[held] * 4,
        out_specs=held,
        scratch_shapes=[pltpu.VMEM((2 * size, width), half), pltpu.VMEM((block, width), half)],
        compiler_params=pltpu.CompilerParams(vmem_limit_bytes=6 * MIB),
        name="fn",
    )(keep(attended), keep(arrived), keep(value_weight), keep(out_weight.T)).T


def shards(
    features, tissue, conv_first, bias_first, conv_second, bias_second, key_weight,
    value_weight, latent_queries, out_weight,
):
    rows, cols = lax.axis_size("row"), lax.axis_size("col")
    if rows == cols == 4 and rows * latent_queries.shape[0] == 128:
        return kernel_path(
            features, tissue, conv_first, bias_first, conv_second, bias_second, key_weight,
            value_weight, latent_queries, out_weight,
        )
    marked = jnp.where(tissue[:, :, None] > 0, features, jnp.asarray(FAR, features.dtype))
    marked = with_halo(with_halo(marked, "row", 0), "col", 1)
    normalized = plain_attend(
        features, tissue, marked, latent_queries,
        (conv_first, bias_first, conv_second, bias_second, key_weight),
    )
    attended = lax.dot_general(
        normalized, value_weight, (((0,), (0,)), ((), ())), preferred_element_type=jnp.float32
    ).astype(jnp.bfloat16)
    return jnp.dot(attended, out_weight, preferred_element_type=jnp.float32).astype(jnp.bfloat16)


def solution(mesh):
    placed = (
        P(("groups", "row"), "col", None),
        P(("groups", "row"), "col"),
        P(),
        P(),
        P(),
        P(),
        P(),
        P(),
        P(("col", "row"), None),
        P(None, "col"),
    )
    return jax.shard_map(
        shards, mesh=mesh, in_specs=placed, out_specs=P(("groups", "row"), "col"), check_vma=False
    )
```
